8 devices in a mesh: model: 2 (over z, y), data: 2 (over x), stage: 2 (over core).
Axes of the slice: x: 2, y: 2, z: 1, core: 2. Of those that a mesh axis runs over, the one named last changes fastest.
Arguments:
- w_up: float32 [2, 1280, 5120], P('stage', None, 'model')
- w_down: float32 [2, 5120, 1280], P('stage', 'model')
- m_up: float32 [2, 1280, 5120], P('stage', None, 'model')
- m_down: float32 [2, 5120, 1280], P('stage', 'model')
- v_up: float32 [2, 1280, 5120], P('stage', None, 'model')
- v_down: float32 [2, 5120, 1280], P('stage', 'model')
- g_up: float32 [2, 2, 1280, 5120], P('data', 'stage', None, 'model')
- g_down: float32 [2, 2, 5120, 1280], P('data', 'stage', 'model')
- acts_last: bfloat16 [2, 512, 1280], P('stage', 'data')
- grad_out: bfloat16 [512, 1280], P('data')
- x_next: bfloat16 [3, 512, 1280], P(None, 'data')
- learn_rate: float32 [1], replicated
- max_norm: float32 [1], replicated
Outputs:
- output 1: float32 [2, 1280, 5120], P('stage', None, 'model')
- output 2: float32 [2, 5120, 1280], P('stage', 'model')
- output 3: float32 [2, 1280, 5120], P('stage', None, 'model')
- output 4: float32 [2, 5120, 1280], P('stage', 'model')
- output 5: float32 [2, 1280, 5120], P('stage', None, 'model')
- output 6: float32 [2, 5120, 1280], P('stage', 'model')
- output 7: bfloat16 [3, 512, 1280], P(None, 'data')
All inputs are finite; a program needn't handle non-finite values.
Results may differ from the reference program's by a relative error of at most 0.00703998.
Values are sent between devices in bfloat16 or wider.
A program may use at most 1 GiB of HBM per device.

```python
import jax
import jax.numpy as jnp
from jax import lax

STAGES = 2
REPLICAS = 2
D_MODEL = 1280
FF_WIDTH = 5120
MICRO_ROWS = 256
NEXT_MICRO = 3
ADAM_STEP = 10
BETA_ONE = 0.9
BETA_TWO = 0.95
ADAM_EPS = 1e-8
WEIGHT_DECAY = 0.1
NORM_EPS = 1e-6
ALL_ROWS = REPLICAS * MICRO_ROWS


def gelu_vjp(pre_act, upstream):
    pull_back = jax.vjp(jax.nn.gelu, pre_act)[1]
    return pull_back(upstream)[0]


def stage_apply(acts_in, up_bf, down_bf):
    pre_act = jnp.dot(acts_in, up_bf, preferred_element_type=jnp.float32)
    hidden = jax.nn.gelu(pre_act).astype(jnp.bfloat16)
    branch = jnp.dot(hidden, down_bf, preferred_element_type=jnp.float32)
    return (acts_in.astype(jnp.float32) + branch).astype(jnp.bfloat16)


def averaged_grads(w_up, w_down, g_up, g_down, acts_last, grad_out):
    def back_step(upstream, layer_in):
        up_bf, down_bf, acts_in = layer_in
        pre_act = jnp.dot(acts_in, up_bf, preferred_element_type=jnp.float32)
        hidden = jax.nn.gelu(pre_act).astype(jnp.bfloat16)
        grad_down = jnp.dot(hidden.T, upstream, preferred_element_type=jnp.float32)
        grad_hid = jnp.dot(upstream, down_bf.T, preferred_element_type=jnp.float32)
        grad_pre = gelu_vjp(pre_act, grad_hid).astype(jnp.bfloat16)
        grad_up = jnp.dot(acts_in.T, grad_pre, preferred_element_type=jnp.float32)
        back_in = jnp.dot(grad_pre, up_bf.T, preferred_element_type=jnp.float32)
        grad_in = (upstream.astype(jnp.float32) + back_in).astype(jnp.bfloat16)
        return grad_in, (grad_up, grad_down)
    layer_all = (w_up.astype(jnp.bfloat16), w_down.astype(jnp.bfloat16), acts_last)
    grad_pair = lax.scan(back_step, grad_out, layer_all, reverse=True)[1]
    mean_up = (jnp.sum(g_up, axis=0) + grad_pair[0]) / REPLICAS
    mean_down = (jnp.sum(g_down, axis=0) + grad_pair[1]) / REPLICAS
    return mean_up, mean_down


def adamw_update(weight, moment_one, moment_two, grad_step, step_rate):
    mom_new = BETA_ONE * moment_one + (1.0 - BETA_ONE) * grad_step
    sec_new = BETA_TWO * moment_two + (1.0 - BETA_TWO) * grad_step * grad_step
    one_corr = 1.0 - BETA_ONE ** ADAM_STEP
    two_corr = 1.0 - BETA_TWO ** ADAM_STEP
    direction = (mom_new / one_corr) / (jnp.sqrt(sec_new / two_corr) + ADAM_EPS)
    weight_new = weight - step_rate * (direction + WEIGHT_DECAY * weight)
    return weight_new, mom_new, sec_new


def forward_all(up_bf, down_bf, x_next):
    def one_micro(acts_in):
        def fwd_step(acts_carry, layer_in):
            return stage_apply(acts_carry, layer_in[0], layer_in[1]), None
        return lax.scan(fwd_step, acts_in, (up_bf, down_bf))[0]
    return lax.map(one_micro, x_next)


def setup_inputs(seed: int = 0) -> dict:
    key_list = jax.random.split(jax.random.key(seed), 13)
    up_scale = D_MODEL ** -0.5
    down_scale = FF_WIDTH ** -0.5
    grad_scale = MICRO_ROWS ** 0.5
    w_up = jax.random.normal(key_list[0], (STAGES, D_MODEL, FF_WIDTH), jnp.float32) * up_scale
    w_down = jax.random.normal(key_list[1], (STAGES, FF_WIDTH, D_MODEL), jnp.float32) * down_scale
    g_up = jax.random.normal(key_list[2], (REPLICAS, STAGES, D_MODEL, FF_WIDTH), jnp.float32) * (0.3 * grad_scale)
    g_down = jax.random.normal(key_list[3], (REPLICAS, STAGES, FF_WIDTH, D_MODEL), jnp.float32) * (0.5 * grad_scale)
    acts_last = jax.random.normal(key_list[4], (STAGES, ALL_ROWS, D_MODEL), jnp.float32).astype(jnp.bfloat16)
    grad_out = jax.random.normal(key_list[5], (ALL_ROWS, D_MODEL), jnp.float32).astype(jnp.bfloat16)
    x_next = jax.random.normal(key_list[6], (NEXT_MICRO, ALL_ROWS, D_MODEL), jnp.float32).astype(jnp.bfloat16)
    learn_rate = jax.random.uniform(key_list[7], (1,), jnp.float32, 0.1, 0.25) * up_scale
    mean_up, mean_down = averaged_grads(w_up, w_down, g_up, g_down, acts_last, grad_out)
    grad_norm = jnp.sqrt(jnp.sum(mean_up * mean_up) + jnp.sum(mean_down * mean_down))
    clip_frac = jax.random.uniform(key_list[8], (1,), jnp.float32, 0.35, 0.65)
    max_norm = clip_frac * grad_norm
    up_rms = clip_frac[0] * jnp.sqrt(jnp.mean(mean_up * mean_up))
    down_rms = clip_frac[0] * jnp.sqrt(jnp.mean(mean_down * mean_down))
    m_up = jax.random.normal(key_list[9], w_up.shape, jnp.float32) * (0.1 * up_rms)
    m_down = jax.random.normal(key_list[10], w_down.shape, jnp.float32) * (0.1 * down_rms)
    v_up = (0.5 + jax.random.uniform(key_list[11], w_up.shape, jnp.float32)) * (0.02 * up_rms * up_rms)
    v_down = (0.5 + jax.random.uniform(key_list[12], w_down.shape, jnp.float32)) * (0.02 * down_rms * down_rms)
    return {'w_up': w_up, 'w_down': w_down, 'm_up': m_up, 'm_down': m_down, 'v_up': v_up, 'v_down': v_down, 'g_up': g_up, 'g_down': g_down, 'acts_last': acts_last, 'grad_out': grad_out, 'x_next': x_next, 'learn_rate': learn_rate, 'max_norm': max_norm}


def reference(w_up, w_down, m_up, m_down, v_up, v_down, g_up, g_down, acts_last, grad_out, x_next, learn_rate, max_norm):
    mean_up, mean_down = averaged_grads(w_up, w_down, g_up, g_down, acts_last, grad_out)
    norm_sq = jnp.sum(mean_up * mean_up) + jnp.sum(mean_down * mean_down)
    clip_scale = jnp.minimum(1.0, max_norm[0] / (jnp.sqrt(norm_sq) + NORM_EPS))
    up_new, up_mom, up_sec = adamw_update(w_up, m_up, v_up, clip_scale * mean_up, learn_rate[0])
    down_new, down_mom, down_sec = adamw_update(w_down, m_down, v_down, clip_scale * mean_down, learn_rate[0])
    y_next = forward_all(up_new.astype(jnp.bfloat16), down_new.astype(jnp.bfloat16), x_next)
    return (up_new, down_new, up_mom, down_mom, up_sec, down_sec, y_next)
```

```python
import functools

import jax
import jax.numpy as jnp
from jax import lax
from jax.experimental import pallas as pl
from jax.experimental.pallas import tpu as pltpu
from jax.sharding import PartitionSpec as P

ADAM_STEP = 10
BETA_ONE = 0.9
BETA_TWO = 0.95
ADAM_EPS = 1e-8
WEIGHT_DECAY = 0.1
NORM_EPS = 1e-6
ONE_CORR = 1.0 - BETA_ONE ** ADAM_STEP
TWO_CORR = 1.0 - BETA_TWO ** ADAM_STEP
GELU_A = 0.7978845608028654
GELU_B = 0.044715
NT = (((1,), (1,)), ((), ()))
TN = (((0,), (0,)), ((), ()))
MESH = pl.DeviceIdType.MESH
VMEM_MAX = 67_043_328
CHUNK = 256
F32 = jnp.float32
BF16 = jnp.bfloat16


def gelu_parts(z):
    t = jnp.tanh(GELU_A * (z + GELU_B * (z * z * z)))
    return t, z * (0.5 * (1.0 + t))


def gelu_slope(z, t):
    return 0.5 * (1.0 + t) + 0.5 * z * (1.0 - t * t) * (GELU_A * (1.0 + 3.0 * GELU_B * z * z))


def dot(a, b, dims=(((1,), (0,)), ((), ()))):
    return lax.dot_general(a, b, dims, preferred_element_type=F32)


def positions():
    return lax.axis_index("model"), lax.axis_index("data"), lax.axis_index("stage")


def entry_barrier(peers):
    barrier = pltpu.get_barrier_semaphore()
    for peer in peers:
        pl.semaphore_signal(barrier, inc=1, device_id=peer, device_id_type=MESH)
    pl.semaphore_wait(barrier, len(peers))


def remote(src, dst, send, recv, peer):
    return pltpu.make_async_remote_copy(src_ref=src, dst_ref=dst, send_sem=send, recv_sem=recv, device_id=peer, device_id_type=MESH)


def grad_kernel(n_chunk, width, w1, w2, g1, g2, acts, dy, max_norm, gb1, gb2, clip,
                gs1, gs2, gr1, gr2, w1b, w2b, gvec, gout, part, part_in, sq1, sq2, sq_out, sq_in,
                w_sem, g_sem, send1, send2, recv1, recv2, out1, out2, part_sem, gvec_sem, sq_send, sq_recv):
    m, d, s = positions()
    peer_x = (m, 1 - d, s)
    peer_y = (1 - m, d, s)
    peer_c = (m, d, 1 - s)
    peer_d = (1 - m, d, 1 - s)

    def loads(j):
        slot = lax.rem(j, 2)
        cols = pl.ds(pl.multiple_of(j * width, width), width)
        return (pltpu.make_async_copy(w1.at[:, cols], w1b.at[slot], w_sem.at[0, slot]),
                pltpu.make_async_copy(w2.at[cols, :], w2b.at[slot], w_sem.at[1, slot]),
                pltpu.make_async_copy(g2.at[cols, :], gs2.at[j], g_sem.at[0, slot]),
                pltpu.make_async_copy(g1.at[:, cols], gs1.at[j], g_sem.at[1, slot]))

    for first in (0, 1):
        for copy in loads(first):
            copy.start()
    entry_barrier((peer_x, peer_y, peer_c, peer_d))

    is_last = s == 1
    hand_over = remote(gout, gvec, gvec_sem.at[0], gvec_sem.at[1], peer_c)
    swap_part = remote(part, part_in, part_sem.at[0], part_sem.at[1], peer_y)

    @pl.when(is_last)
    def _():
        gvec[...] = dy[...]
        part[...] = jnp.zeros_like(part)

    @pl.when(jnp.logical_not(is_last))
    def _():
        hand_over.wait_recv()

    def send_two(j):
        return remote(gs2.at[j], gr2.at[j], send2.at[j], recv2.at[j], peer_x)

    def send_one(j):
        return remote(gs1.at[j], gr1.at[j], send1.at[j], recv1.at[j], peer_x)

    @pl.loop(0, n_chunk)
    def _(j):
        slot = lax.rem(j, 2)
        copies = loads(j)
        copies[0].wait()
        up = w1b[slot].astype(BF16)
        rows = acts[...]
        grad = gvec[...]
        z = dot(rows, up)
        t, act = gelu_parts(z)
        hid = act.astype(BF16)
        copies[2].wait()
        gs2[j] += dot(hid, grad, TN)
        send_two(j).start()
        copies[1].wait()
        grad_hid = dot(grad, w2b[slot].astype(BF16), NT)
        grad_pre = (gelu_slope(z, t) * grad_hid).astype(BF16)
        copies[3].wait()
        gs1[j] += dot(rows, grad_pre, TN)
        send_one(j).start()

        @pl.when(is_last)
        def _():
            part[...] += dot(grad_pre, up, NT)

        @pl.when(j + 2 < n_chunk)
        def _():
            for copy in loads(j + 2):
                copy.start()

    @pl.when(is_last)
    def _():
        swap_part.start()
        swap_part.wait()
        gout[...] = (gvec[...].astype(F32) + (part[...] + part_in[...])).astype(BF16)
        hand_over.start()

    sq1[...] = jnp.zeros_like(sq1)
    sq2[...] = jnp.zeros_like(sq2)

    def write_two(j):
        return pltpu.make_async_copy(gr2.at[j], gb2.at[j], out2.at[j])

    def write_one(j):
        return pltpu.make_async_copy(gr1.at[j], gb1.at[j], out1.at[j])

    @pl.loop(0, n_chunk)
    def _(j):
        send_two(j).wait_recv()
        mean = (gs2[j] + gr2[j]) * 0.5
        gr2[j] = mean
        sq2[...] += jnp.sum((mean * mean).reshape(-1, 8, mean.shape[1]), axis=0)
        write_two(j).start()
        send_one(j).wait_recv()
        mean = (gs1[j] + gr1[j]) * 0.5
        gr1[j] = mean
        sq1[...] += jnp.sum((mean * mean).reshape(-1, 8, mean.shape[1]), axis=0)
        write_one(j).start()

    sq_out[...] = jnp.full(sq_out.shape, jnp.sum(sq1[...]) + jnp.sum(sq2[...]), F32)
    mine = 2 * m + s
    others = ((peer_y, 2 * (1 - m) + s), (peer_c, 2 * m + 1 - s), (peer_d, 2 * (1 - m) + 1 - s))
    shares = [remote(sq_out, sq_in.at[mine], sq_send.at[k], sq_recv.at[mine], peer) for k, (peer, _) in enumerate(others)]
    for copy in shares:
        copy.start()
    sq_in[mine] = sq_out[...]
    for peer, index in others:
        remote(sq_out, sq_in.at[index], sq_send.at[0], sq_recv.at[index], peer).wait_recv()
    total = (sq_in[0] + sq_in[1]) + (sq_in[2] + sq_in[3])
    clip[...] = jnp.minimum(1.0, max_norm[0] / (jnp.sqrt(total) + NORM_EPS))

    for copy in shares:
        copy.wait_send()

    @pl.when(is_last)
    def _():
        hand_over.wait_send()

    @pl.loop(0, n_chunk)
    def _(j):
        send_two(j).wait_send()
        send_one(j).wait_send()
        write_two(j).wait()
        write_one(j).wait()


def update_kernel(clip, rate, w1, m1, v1, gb1, w2, m2, v2, gb2, x,
                  nw1, nw2, nm1, nm2, nv1, nv2, wb1, wb2, acc):
    s = lax.axis_index("stage")
    j = pl.program_id(0)
    scale = clip[0, 0]
    step_rate = rate[0]

    def adamw(w, mom, sec, mean):
        grad = scale * mean
        mom_new = BETA_ONE * mom + (1.0 - BETA_ONE) * grad
        sec_new = BETA_TWO * sec + (1.0 - BETA_TWO) * grad * grad
        direction = (mom_new / ONE_CORR) / (jnp.sqrt(sec_new / TWO_CORR) + ADAM_EPS)
        return w - step_rate * (direction + WEIGHT_DECAY * w), mom_new, sec_new

    a, b, c = adamw(w1[...], m1[...], v1[...], gb1[...])
    nw1[...] = a
    nm1[...] = b
    nv1[...] = c
    wb1[...] = a.astype(BF16)
    a, b, c = adamw(w2[...], m2[...], v2[...], gb2[...])
    nw2[...] = a
    nm2[...] = b
    nv2[...] = c
    wb2[...] = a.astype(BF16)

    @pl.when(j == 0)
    def _():
        acc[...] = jnp.zeros_like(acc)

    @pl.when(s == 0)
    def _():
        hid = gelu_parts(dot(x[...], wb1[...]))[1].astype(BF16)
        acc[...] += dot(hid, wb2[...])


def forward_kernel(n_chunk, n_micro, half, acc, x, wb1, wb2, y,
                   w1, w2, first_in, own_half, act, peer_half, part, part_in,
                   w_sem, a_send, a_recv, o_send, o_recv, p_send, p_recv, y_send, y_recv, f_send, f_recv):
    m, d, s = positions()
    peer_y = (1 - m, d, s)
    peer_c = (m, d, 1 - s)
    peer_d = (1 - m, d, 1 - s)
    entry_barrier((peer_y, peer_c, peer_d))
    mine = pl.ds(pl.multiple_of(m * half, half), half)
    theirs = pl.ds(pl.multiple_of((1 - m) * half, half), half)

    def send_first(k):
        return remote(acc.at[k, theirs, :], first_in.at[k], a_send.at[k], a_recv.at[k], peer_y)

    def give_core(k):
        return remote(own_half.at[k], act.at[k, mine, :], o_send.at[0, k], o_recv.at[0, k], peer_c)

    def give_diag(k):
        return remote(own_half.at[k], act.at[k, mine, :], o_send.at[1, k], o_recv.at[1, k], peer_d)

    def send_part(k):
        return remote(part.at[k, theirs, :], part_in.at[k], p_send.at[k], p_recv.at[k], peer_y)

    def swap_y(k):
        return remote(own_half.at[k], peer_half.at[k], y_send.at[0, k], y_recv.at[0, k], peer_y)

    def give_own(k):
        return remote(own_half.at[k], y.at[k, mine, :], y_send.at[1, k], y_recv.at[1, k], peer_c)

    def pass_on(k):
        return remote(peer_half.at[k], y.at[k, theirs, :], f_send.at[k], f_recv.at[k], peer_c)

    @pl.when(s == 0)
    def _():
        send_first(0).start()
        for k in range(n_micro):
            if k + 1 < n_micro:
                send_first(k + 1).start()
            send_first(k).wait_recv()
            out = x[k, mine, :].astype(F32) + (acc[k, mine, :] + first_in[k])
            own_half[k] = out.astype(BF16)
            give_core(k).start()
            give_diag(k).start()
        for k in range(n_micro):
            give_own(k).wait_recv()
            pass_on(k).wait_recv()
        for k in range(n_micro):
            send_first(k).wait_send()
            give_core(k).wait_send()
            give_diag(k).wait_send()

    @pl.when(s == 1)
    def _():
        cp1 = pltpu.make_async_copy(wb1, w1, w_sem.at[0])
        cp2 = pltpu.make_async_copy(wb2, w2, w_sem.at[1])
        cp1.start()
        cp2.start()
        cp1.wait()
        cp2.wait()

        def finish(k):
            send_part(k).wait_recv()
            out = act[k, mine, :].astype(F32) + (part[k, mine, :] + part_in[k])
            own_half[k] = out.astype(BF16)
            swap_y(k).start()
            give_own(k).start()
            y[k, mine, :] = own_half[k]

        for k in range(n_micro):
            give_core(k).wait_recv()
            give_diag(k).wait_recv()
            part[k] = jnp.zeros_like(part[k])

            @pl.loop(0, n_chunk)
            def _(j):
                hid = gelu_parts(dot(act[k], w1[j]))[1].astype(BF16)
                part[k] += dot(hid, w2[j])

            send_part(k).start()
            if k > 0:
                finish(k - 1)
        finish(n_micro - 1)
        for k in range(n_micro):
            swap_y(k).wait_recv()
            pass_on(k).start()
            y[k, theirs, :] = peer_half[k]
        for k in range(n_micro):
            send_part(k).wait_send()
            swap_y(k).wait_send()
            give_own(k).wait_send()
            pass_on(k).wait_send()


def solution(mesh):
    up_spec = P('stage', None, 'model')
    down_spec = P('stage', 'model', None)
    row_spec = P(None, 'data', None)
    in_specs = (up_spec, down_spec, up_spec, down_spec, up_spec, down_spec, P('data', 'stage', None, 'model'), P('data', 'stage', 'model', None), P('stage', 'data', None), P('data', None), row_spec, P(None), P(None))
    out_specs = (up_spec, down_spec, up_spec, down_spec, up_spec, down_spec, row_spec)

    def device_step(w_up, w_down, m_up, m_down, v_up, v_down, g_up, g_down, acts_last, grad_out, x_next, learn_rate, max_norm):
        d_model, ff = w_up.shape[1:]
        rows = grad_out.shape[0]
        n_micro = x_next.shape[0]
        width = CHUNK
        n_chunk = ff // width
        half = rows // 2
        hbm = pl.BlockSpec(memory_space=pl.ANY)
        vmem = pl.BlockSpec(memory_space=pltpu.VMEM)
        smem = pl.BlockSpec(memory_space=pltpu.SMEM)
        dma = pltpu.SemaphoreType.DMA

        mean_up, mean_down, clip = pl.pallas_call(
            functools.partial(grad_kernel, n_chunk, width),
            out_shape=(jax.ShapeDtypeStruct((n_chunk, d_model, width), F32),
                       jax.ShapeDtypeStruct((n_chunk, width, d_model), F32),
                       jax.ShapeDtypeStruct((8, 128), F32)),
            in_specs=[hbm, hbm, hbm, hbm, vmem, vmem, smem],
            out_specs=(hbm, hbm, vmem),
            scratch_shapes=[
                pltpu.VMEM((n_chunk, d_model, width), F32),
                pltpu.VMEM((n_chunk, width, d_model), F32),
                pltpu.VMEM((n_chunk, d_model, width), F32),
                pltpu.VMEM((n_chunk, width, d_model), F32),
                pltpu.VMEM((2, d_model, width), F32),
                pltpu.VMEM((2, width, d_model), F32),
                pltpu.VMEM((rows, d_model), BF16),
                pltpu.VMEM((rows, d_model), BF16),
                pltpu.VMEM((rows, d_model), F32),
                pltpu.VMEM((rows, d_model), F32),
                pltpu.VMEM((8, width), F32),
                pltpu.VMEM((8, d_model), F32),
                pltpu.VMEM((8, 128), F32),
                pltpu.VMEM((4, 8, 128), F32),
                dma((2, 2)), dma((2, 2)),
                dma((n_chunk,)), dma((n_chunk,)), dma((n_chunk,)), dma((n_chunk,)),
                dma((n_chunk,)), dma((n_chunk,)),
                dma((2,)), dma((2,)), dma((3,)), dma((4,)),
            ],
            compiler_params=pltpu.CompilerParams(collective_id=0, has_side_effects=True, vmem_limit_bytes=VMEM_MAX),
            name="grad_exchange",
        )(w_up[0], w_down[0], g_up[0, 0], g_down[0, 0], acts_last[0], grad_out, max_norm)

        x_all = x_next.reshape(n_micro * rows, d_model)
        up_block = pl.BlockSpec((None, d_model, width), lambda j: (0, 0, j))
        down_block = pl.BlockSpec((None, width, d_model), lambda j: (0, j, 0))
        up_chunk = pl.BlockSpec((None, d_model, width), lambda j: (j, 0, 0))
        down_chunk = pl.BlockSpec((None, width, d_model), lambda j: (j, 0, 0))
        whole = pl.BlockSpec((n_micro * rows, d_model), lambda j: (0, 0))
        up_out = jax.ShapeDtypeStruct(w_up.shape, F32)
        down_out = jax.ShapeDtypeStruct(w_down.shape, F32)
        nw1, nw2, nm1, nm2, nv1, nv2, wb1, wb2, acc = pl.pallas_call(
            update_kernel,
            grid=(n_chunk,),
            out_shape=(up_out, down_out, up_out, down_out, up_out, down_out,
                       jax.ShapeDtypeStruct((n_chunk, d_model, width), BF16),
                       jax.ShapeDtypeStruct((n_chunk, width, d_model), BF16),
                       jax.ShapeDtypeStruct((n_micro * rows, d_model), F32)),
            in_specs=[smem, smem, up_block, up_block, up_block, up_chunk,
                      down_block, down_block, down_block, down_chunk, whole],
            out_specs=(up_block, down_block, up_block, down_block, up_block, down_block, up_chunk, down_chunk, whole),
            compiler_params=pltpu.CompilerParams(vmem_limit_bytes=VMEM_MAX),
            name="update",
        )(clip, learn_rate, w_up, m_up, v_up, mean_up, w_down, m_down, v_down, mean_down, x_all)

        y_next = pl.pallas_call(
            functools.partial(forward_kernel, n_chunk, n_micro, half),
            out_shape=jax.ShapeDtypeStruct(x_next.shape, BF16),
            in_specs=[vmem, vmem, hbm, hbm],
            out_specs=vmem,
            scratch_shapes=[
                pltpu.VMEM((n_chunk, d_model, width), BF16),
                pltpu.VMEM((n_chunk, width, d_model), BF16),
                pltpu.VMEM((n_micro, half, d_model), F32),
                pltpu.VMEM((n_micro, half, d_model), BF16),
                pltpu.VMEM((n_micro, rows, d_model), BF16),
                pltpu.VMEM((n_micro, half, d_model), BF16),
                pltpu.VMEM((n_micro, rows, d_model), F32),
                pltpu.VMEM((n_micro, half, d_model), F32),
                dma((2,)), dma((n_micro,)), dma((n_micro,)), dma((2, n_micro)), dma((2, n_micro)),
                dma((n_micro,)), dma((n_micro,)), dma((2, n_micro)), dma((2, n_micro)), dma((n_micro,)), dma((n_micro,)),
            ],
            compiler_params=pltpu.CompilerParams(collective_id=1, has_side_effects=True, vmem_limit_bytes=VMEM_MAX),
            name="forward_exchange",
        )(acc.reshape(n_micro, rows, d_model), x_next, wb1, wb2)
        return nw1, nw2, nm1, nm2, nv1, nv2, y_next

    return jax.shard_map(device_step, mesh=mesh, in_specs=in_specs, out_specs=out_specs, check_vma=False)
```

```python
import functools

import jax
import jax.numpy as jnp
from jax import lax
from jax.experimental import pallas as pl
from jax.experimental.pallas import tpu as pltpu
from jax.sharding import PartitionSpec as P

ADAM_STEP = 10
BETA_ONE = 0.9
BETA_TWO = 0.95
ADAM_EPS = 1e-8
WEIGHT_DECAY = 0.1
NORM_EPS = 1e-6
ONE_CORR = 1.0 - BETA_ONE ** ADAM_STEP
TWO_CORR = 1.0 - BETA_TWO ** ADAM_STEP
GELU_A = 0.7978845608028654
GELU_B = 0.044715
NT = (((1,), (1,)), ((), ()))
TN = (((0,), (0,)), ((), ()))
MESH = pl.DeviceIdType.MESH
VMEM_MAX = 67_043_328
CHUNK = 256
COLS = 128
F32 = jnp.float32
BF16 = jnp.bfloat16


def gelu_parts(z):
    t = jnp.tanh(GELU_A * (z + GELU_B * (z * z * z)))
    return t, z * (0.5 * (1.0 + t))


def gelu_slope(z, t):
    return 0.5 * (1.0 + t) + 0.5 * z * (1.0 - t * t) * (GELU_A * (1.0 + 3.0 * GELU_B * z * z))


def dot(a, b, dims=(((1,), (0,)), ((), ()))):
    return lax.dot_general(a, b, dims, preferred_element_type=F32)


def positions():
    return lax.axis_index("model"), lax.axis_index("data"), lax.axis_index("stage")


def entry_barrier(peers):
    barrier = pltpu.get_barrier_semaphore()
    for peer in peers:
        pl.semaphore_signal(barrier, inc=1, device_id=peer, device_id_type=MESH)
    pl.semaphore_wait(barrier, len(peers))


def remote(src, dst, send, recv, peer):
    return pltpu.make_async_remote_copy(src_ref=src, dst_ref=dst, send_sem=send, recv_sem=recv, device_id=peer, device_id_type=MESH)


def grad_kernel(n_chunk, width, w1, w2, g1, g2, acts, dy, max_norm, gb1, gb2, clip,
                gs1, gs2, gr1, gr2, w1b, w2b, gvec, gout, part, part_in, sq1, sq2, sq_out, sq_in,
                w_sem, g_sem, send1, send2, recv1, recv2, out1, out2, part_sem, gvec_sem, sq_send, sq_recv):
    m, d, s = positions()
    peer_x = (m, 1 - d, s)
    peer_y = (1 - m, d, s)
    peer_c = (m, d, 1 - s)
    peer_d = (1 - m, d, 1 - s)

    def loads(j):
        slot = lax.rem(j, 2)
        cols = pl.ds(pl.multiple_of(j * width, width), width)
        return (pltpu.make_async_copy(w1.at[:, cols], w1b.at[slot], w_sem.at[0, slot]),
                pltpu.make_async_copy(w2.at[cols, :], w2b.at[slot], w_sem.at[1, slot]),
                pltpu.make_async_copy(g2.at[cols, :], gs2.at[j], g_sem.at[0, slot]),
                pltpu.make_async_copy(g1.at[:, cols], gs1.at[j], g_sem.at[1, slot]))

    for first in (0, 1):
        for copy in loads(first):
            copy.start()
    entry_barrier((peer_x, peer_y, peer_c, peer_d))

    is_last = s == 1
    hand_over = remote(gout, gvec, gvec_sem.at[0], gvec_sem.at[1], peer_c)
    swap_part = remote(part, part_in, part_sem.at[0], part_sem.at[1], peer_y)

    @pl.when(is_last)
    def _():
        gvec[...] = dy[...]
        part[...] = jnp.zeros_like(part)

    @pl.when(jnp.logical_not(is_last))
    def _():
        hand_over.wait_recv()

    def send_two(j):
        return remote(gs2.at[j], gr2.at[j], send2.at[j], recv2.at[j], peer_x)

    def send_one(j):
        return remote(gs1.at[j], gr1.at[j], send1.at[j], recv1.at[j], peer_x)

    @pl.loop(0, n_chunk)
    def _(j):
        slot = lax.rem(j, 2)
        copies = loads(j)
        copies[0].wait()
        up = w1b[slot].astype(BF16)
        rows = acts[...]
        grad = gvec[...]
        z = dot(rows, up)
        t, act = gelu_parts(z)
        hid = act.astype(BF16)
        copies[2].wait()
        gs2[j] += dot(hid, grad, TN)
        send_two(j).start()
        copies[1].wait()
        grad_hid = dot(grad, w2b[slot].astype(BF16), NT)
        grad_pre = (gelu_slope(z, t) * grad_hid).astype(BF16)
        copies[3].wait()
        gs1[j] += dot(rows, grad_pre, TN)
        send_one(j).start()

        @pl.when(is_last)
        def _():
            part[...] += dot(grad_pre, up, NT)

        @pl.when(j + 2 < n_chunk)
        def _():
            for copy in loads(j + 2):
                copy.start()

    @pl.when(is_last)
    def _():
        swap_part.start()
        swap_part.wait()
        gout[...] = (gvec[...].astype(F32) + (part[...] + part_in[...])).astype(BF16)
        hand_over.start()

    sq1[...] = jnp.zeros_like(sq1)
    sq2[...] = jnp.zeros_like(sq2)

    def write_two(j):
        return pltpu.make_async_copy(gr2.at[j], gb2.at[j], out2.at[j])

    def write_one(j):
        return pltpu.make_async_copy(gr1.at[j], gb1.at[j], out1.at[j])

    @pl.loop(0, n_chunk)
    def _(j):
        send_two(j).wait_recv()
        mean = (gs2[j] + gr2[j]) * 0.5
        gr2[j] = mean
        sq2[...] += jnp.sum((mean * mean).reshape(-1, 8, mean.shape[1]), axis=0)
        write_two(j).start()
        send_one(j).wait_recv()
        mean = (gs1[j] + gr1[j]) * 0.5
        gr1[j] = mean
        sq1[...] += jnp.sum((mean * mean).reshape(-1, 8, mean.shape[1]), axis=0)
        write_one(j).start()

    sq_out[...] = jnp.full(sq_out.shape, jnp.sum(sq1[...]) + jnp.sum(sq2[...]), F32)
    mine = 2 * m + s
    others = ((peer_y, 2 * (1 - m) + s), (peer_c, 2 * m + 1 - s), (peer_d, 2 * (1 - m) + 1 - s))
    shares = [remote(sq_out, sq_in.at[mine], sq_send.at[k], sq_recv.at[mine], peer) for k, (peer, _) in enumerate(others)]
    for copy in shares:
        copy.start()
    sq_in[mine] = sq_out[...]
    for peer, index in others:
        remote(sq_out, sq_in.at[index], sq_send.at[0], sq_recv.at[index], peer).wait_recv()
    total = (sq_in[0] + sq_in[1]) + (sq_in[2] + sq_in[3])
    clip[...] = jnp.minimum(1.0, max_norm[0] / (jnp.sqrt(total) + NORM_EPS))

    for copy in shares:
        copy.wait_send()

    @pl.when(is_last)
    def _():
        hand_over.wait_send()

    @pl.loop(0, n_chunk)
    def _(j):
        send_two(j).wait_send()
        send_one(j).wait_send()
        write_two(j).wait()
        write_one(j).wait()


def adamw(scale, step_rate, w, mom, sec, mean):
    grad = scale * mean
    mom_new = BETA_ONE * mom + (1.0 - BETA_ONE) * grad
    sec_new = BETA_TWO * sec + ((1.0 - BETA_TWO) * grad) * grad
    direction = (mom_new * (1.0 / ONE_CORR)) / (jnp.sqrt(sec_new * (1.0 / TWO_CORR)) + ADAM_EPS)
    return w - step_rate * (direction + WEIGHT_DECAY * w), mom_new, sec_new


def update_down(clip, rate, w2, m2, v2, gb2, hid, nw2, nm2, nv2, mine, theirs, prod):
    n_micro, half = mine.shape[0], mine.shape[1]
    new, mom, sec = adamw(clip[0, 0], rate[0], w2[...], m2[...], v2[...], gb2[...])
    nw2[...] = new
    nm2[...] = mom
    nv2[...] = sec

    @pl.when(lax.axis_index("stage") == 0)
    def _():
        m = lax.axis_index("model")
        prod[...] = dot(hid[...], nw2[...].astype(BF16)).reshape(prod.shape)
        for k in range(n_micro):
            mine[k] = prod[k, pl.ds(pl.multiple_of(m * half, half), half), :]
            theirs[k] = prod[k, pl.ds(pl.multiple_of((1 - m) * half, half), half), :]


def update_first(n_chunk, width, clip, rate, w1, m1, v1, gb1, w2, m2, v2, gb2, x,
                 nw1, nm1, nv1, nw2, nm2, nv2, hid, mine, theirs, prod):
    j = pl.program_id(0)

    @pl.when(j < n_chunk)
    def _():
        new, mom, sec = adamw(clip[0, 0], rate[0], w1[...], m1[...], v1[...], gb1[...])
        nw1[...] = new
        nm1[...] = mom
        nv1[...] = sec

        @pl.when(lax.axis_index("stage") == 0)
        def _():
            cols = pl.ds(pl.multiple_of(j * width, width), width)
            hid[:, cols] = gelu_parts(dot(x[...], nw1[...].astype(BF16)))[1].astype(BF16)

    @pl.when(j >= n_chunk)
    def _():
        update_down(clip, rate, w2, m2, v2, gb2, hid, nw2, nm2, nv2, mine, theirs, prod)


def update_second(clip, rate, w2, m2, v2, gb2, hid, _w, _m, _v, nw2, nm2, nv2, mine, theirs, prod):
    update_down(clip, rate, w2, m2, v2, gb2, hid, nw2, nm2, nv2, mine, theirs, prod)


def forward_kernel(n_chunk, n_micro, half, width, cut, mine_a, got_a, mine_b, theirs_b, x, nw1, nw2, y,
                   w1, w2, w1f, w2f, got_b, own_half, act, peer_half, part, part_in,
                   w_sem, a_send, a_recv, o_send, o_recv, p_send, p_recv, y_send, y_recv, f_send, f_recv):
    m, d, s = positions()
    peer_y = (1 - m, d, s)
    peer_c = (m, d, 1 - s)
    peer_d = (1 - m, d, 1 - s)

    def loads(j):
        slot = lax.rem(j, 2)
        cols = pl.ds(pl.multiple_of(j * width, width), width)
        return (pltpu.make_async_copy(nw1.at[0, :, cols], w1f.at[slot], w_sem.at[0, slot]),
                pltpu.make_async_copy(nw2.at[0, cols, :], w2f.at[slot], w_sem.at[1, slot]))

    @pl.when(s == 1)
    def _():
        for first in (0, 1):
            for copy in loads(first):
                copy.start()

    entry_barrier((peer_y, peer_c, peer_d))
    mine = pl.ds(pl.multiple_of(m * half, half), half)
    theirs = pl.ds(pl.multiple_of((1 - m) * half, half), half)

    def send_first(k):
        return remote(theirs_b.at[k], got_b.at[k], a_send.at[k], a_recv.at[k], peer_y)

    def give_core(k):
        return remote(own_half.at[k], act.at[k, mine, :], o_send.at[0, k], o_recv.at[0, k], peer_c)

    def give_diag(k):
        return remote(own_half.at[k], act.at[k, mine, :], o_send.at[1, k], o_recv.at[1, k], peer_d)

    def send_part(k):
        return remote(part.at[k, theirs, :], part_in.at[k], p_send.at[k], p_recv.at[k], peer_y)

    def swap_y(k):
        return remote(own_half.at[k], peer_half.at[k], y_send.at[0, k], y_recv.at[0, k], peer_y)

    def give_own(k):
        return remote(own_half.at[k], y.at[k, mine, :], y_send.at[1, k], y_recv.at[1, k], peer_c)

    def pass_on(k):
        return remote(peer_half.at[k], y.at[k, theirs, :], f_send.at[k], f_recv.at[k], peer_c)

    @pl.when(s == 0)
    def _():
        send_first(0).start()
        for k in range(n_micro):
            if k + 1 < n_micro:
                send_first(k + 1).start()
            rows = x[k, mine, :].astype(F32)
            own_half[k, :, :cut] = (rows[:, :cut] + (mine_a[k] + got_a[k])).astype(BF16)
            send_first(k).wait_recv()
            own_half[k, :, cut:] = (rows[:, cut:] + (mine_b[k] + got_b[k])).astype(BF16)
            give_diag(k).start()
            give_core(k).start()
        for k in range(n_micro):
            give_own(k).wait_recv()
            pass_on(k).wait_recv()
        for k in range(n_micro):
            send_first(k).wait_send()
            give_core(k).wait_send()
            give_diag(k).wait_send()

    @pl.when(s == 1)
    def _():
        @pl.loop(0, n_chunk)
        def _(j):
            slot = lax.rem(j, 2)
            copies = loads(j)
            copies[0].wait()
            w1[j] = w1f[slot].astype(BF16)
            copies[1].wait()
            w2[j] = w2f[slot].astype(BF16)

            @pl.when(j + 2 < n_chunk)
            def _():
                for copy in loads(j + 2):
                    copy.start()

        def finish(k):
            send_part(k).wait_recv()
            out = act[k, mine, :].astype(F32) + (part[k, mine, :] + part_in[k])
            own_half[k] = out.astype(BF16)
            swap_y(k).start()
            give_own(k).start()
            y[k, mine, :] = own_half[k]

        for k in range(n_micro):
            give_core(k).wait_recv()
            give_diag(k).wait_recv()
            part[k] = jnp.zeros_like(part[k])

            @pl.loop(0, n_chunk)
            def _(j):
                hid = gelu_parts(dot(act[k], w1[j]))[1].astype(BF16)
                part[k] += dot(hid, w2[j])

            send_part(k).start()
            if k > 0:
                finish(k - 1)
        finish(n_micro - 1)
        for k in range(n_micro):
            swap_y(k).wait_recv()
            pass_on(k).start()
            y[k, theirs, :] = peer_half[k]
        for k in range(n_micro):
            send_part(k).wait_send()
            swap_y(k).wait_send()
            give_own(k).wait_send()
            pass_on(k).wait_send()


def solution(mesh):
    up_spec = P('stage', None, 'model')
    down_spec = P('stage', 'model', None)
    row_spec = P(None, 'data', None)
    in_specs = (up_spec, down_spec, up_spec, down_spec, up_spec, down_spec, P('data', 'stage', None, 'model'), P('data', 'stage', 'model', None), P('stage', 'data', None), P('data', None), row_spec, P(None), P(None))
    out_specs = (up_spec, down_spec, up_spec, down_spec, up_spec, down_spec, row_spec)

    def device_step(w_up, w_down, m_up, m_down, v_up, v_down, g_up, g_down, acts_last, grad_out, x_next, learn_rate, max_norm):
        d_model, ff = w_up.shape[1:]
        rows = grad_out.shape[0]
        n_micro = x_next.shape[0]
        width = CHUNK
        n_chunk = ff // width
        half = rows // 2
        hbm = pl.BlockSpec(memory_space=pl.ANY)
        vmem = pl.BlockSpec(memory_space=pltpu.VMEM)
        smem = pl.BlockSpec(memory_space=pltpu.SMEM)
        dma = pltpu.SemaphoreType.DMA

        mean_up, mean_down, clip = pl.pallas_call(
            functools.partial(grad_kernel, n_chunk, width),
            out_shape=(jax.ShapeDtypeStruct((n_chunk, d_model, width), F32),
                       jax.ShapeDtypeStruct((n_chunk, width, d_model), F32),
                       jax.ShapeDtypeStruct((8, 128), F32)),
            in_specs=[hbm, hbm, hbm, hbm, vmem, vmem, smem],
            out_specs=(hbm, hbm, vmem),
            scratch_shapes=[
                pltpu.VMEM((n_chunk, d_model, width), F32),
                pltpu.VMEM((n_chunk, width, d_model), F32),
                pltpu.VMEM((n_chunk, d_model, width), F32),
                pltpu.VMEM((n_chunk, width, d_model), F32),
                pltpu.VMEM((2, d_model, width), F32),
                pltpu.VMEM((2, width, d_model), F32),
                pltpu.VMEM((rows, d_model), BF16),
                pltpu.VMEM((rows, d_model), BF16),
                pltpu.VMEM((rows, d_model), F32),
                pltpu.VMEM((rows, d_model), F32),
                pltpu.VMEM((8, width), F32),
                pltpu.VMEM((8, d_model), F32),
                pltpu.VMEM((8, 128), F32),
                pltpu.VMEM((4, 8, 128), F32),
                dma((2, 2)), dma((2, 2)),
                dma((n_chunk,)), dma((n_chunk,)), dma((n_chunk,)), dma((n_chunk,)),
                dma((n_chunk,)), dma((n_chunk,)),
                dma((2,)), dma((2,)), dma((3,)), dma((4,)),
            ],
            compiler_params=pltpu.CompilerParams(collective_id=0, has_side_effects=True, vmem_limit_bytes=VMEM_MAX),
            name="grad_exchange",
        )(w_up[0], w_down[0], g_up[0, 0], g_down[0, 0], acts_last[0], grad_out, max_norm)

        x_all = x_next.reshape(n_micro * rows, d_model)
        n_col = d_model // COLS
        n_first = n_col * 3 // 5
        cut = n_first * COLS
        mean_down = mean_down.reshape(1, ff, d_model)
        up_block = pl.BlockSpec((None, d_model, width), lambda j: (0, 0, jnp.minimum(j, n_chunk - 1)))
        up_chunk = pl.BlockSpec((None, d_model, width), lambda j: (jnp.minimum(j, n_chunk - 1), 0, 0))
        col_a = pl.BlockSpec((None, ff, COLS), lambda j: (0, 0, jnp.maximum(j - n_chunk, 0)))
        col_b = pl.BlockSpec((None, ff, COLS), lambda j: (0, 0, j + n_first))
        piece_a = pl.BlockSpec((n_micro, half, COLS), lambda j: (0, 0, jnp.maximum(j - n_chunk, 0)))
        piece_b = pl.BlockSpec((n_micro, half, COLS), lambda j: (0, 0, j))
        x_block = pl.BlockSpec((n_micro * rows, d_model), lambda j: (0, 0))
        hid_block = pl.BlockSpec((n_micro * rows, ff), lambda j: (0, 0))
        up_out = jax.ShapeDtypeStruct(w_up.shape, F32)
        down_out = jax.ShapeDtypeStruct(w_down.shape, F32)
        part_a = jax.ShapeDtypeStruct((n_micro, half, cut), F32)
        part_b = jax.ShapeDtypeStruct((n_micro, half, d_model - cut), F32)
        prod = [pltpu.VMEM((n_micro, rows, COLS), F32)]

        def cost(units):
            return pl.CostEstimate(flops=2 * n_micro * rows * units, bytes_accessed=28 * units, transcendentals=2 * units)

        nw1, nm1, nv1, nw2, nm2, nv2, hid, mine_a, theirs_a = pl.pallas_call(
            functools.partial(update_first, n_chunk, width),
            grid=(n_chunk + n_first,),
            out_shape=(up_out, up_out, up_out, down_out, down_out, down_out,
                       jax.ShapeDtypeStruct((n_micro * rows, ff), BF16), part_a, part_a),
            in_specs=[smem, smem, up_block, up_block, up_block, up_chunk, col_a, col_a, col_a, col_a, x_block],
            out_specs=(up_block, up_block, up_block, col_a, col_a, col_a, hid_block, piece_a, piece_a),
            scratch_shapes=prod,
            compiler_params=pltpu.CompilerParams(vmem_limit_bytes=VMEM_MAX),
            cost_estimate=cost(d_model * ff + cut * ff),
            name="update_first",
        )(clip, learn_rate, w_up, m_up, v_up, mean_up, w_down, m_down, v_down, mean_down, x_all)

        got_a = lax.ppermute(theirs_a, ('model', 'stage'), [(0, 2), (2, 0)])

        nw2, nm2, nv2, mine_b, theirs_b = pl.pallas_call(
            update_second,
            grid=(n_col - n_first,),
            out_shape=(down_out, down_out, down_out, part_b, part_b),
            in_specs=[smem, smem, col_b, col_b, col_b, col_b, hid_block, hbm, hbm, hbm],
            out_specs=(col_b, col_b, col_b, piece_b, piece_b),
            scratch_shapes=prod,
            input_output_aliases={7: 0, 8: 1, 9: 2},
            compiler_params=pltpu.CompilerParams(vmem_limit_bytes=VMEM_MAX),
            cost_estimate=cost((d_model - cut) * ff),
            name="update_second",
        )(clip, learn_rate, w_down, m_down, v_down, mean_down, hid, nw2, nm2, nv2)

        y_next = pl.pallas_call(
            functools.partial(forward_kernel, n_chunk, n_micro, half, width, cut),
            out_shape=jax.ShapeDtypeStruct(x_next.shape, BF16),
            in_specs=[vmem, vmem, vmem, vmem, vmem, hbm, hbm],
            out_specs=vmem,
            scratch_shapes=[
                pltpu.VMEM((n_chunk, d_model, width), BF16),
                pltpu.VMEM((n_chunk, width, d_model), BF16),
                pltpu.VMEM((2, d_model, width), F32),
                pltpu.VMEM((2, width, d_model), F32),
                pltpu.VMEM((n_micro, half, d_model - cut), F32),
                pltpu.VMEM((n_micro, half, d_model), BF16),
                pltpu.VMEM((n_micro, rows, d_model), BF16),
                pltpu.VMEM((n_micro, half, d_model), BF16),
                pltpu.VMEM((n_micro, rows, d_model), F32),
                pltpu.VMEM((n_micro, half, d_model), F32),
                dma((2, 2)), dma((n_micro,)), dma((n_micro,)), dma((2, n_micro)), dma((2, n_micro)),
                dma((n_micro,)), dma((n_micro,)), dma((2, n_micro)), dma((2, n_micro)), dma((n_micro,)), dma((n_micro,)),
            ],
            compiler_params=pltpu.CompilerParams(collective_id=1, has_side_effects=True, vmem_limit_bytes=VMEM_MAX),
            name="forward_exchange",
        )(mine_a, got_a, mine_b, theirs_b, x_next, nw1, nw2)
        return nw1, nw2, nm1, nm2, nv1, nv2, y_next

    return jax.shard_map(device_step, mesh=mesh, in_specs=in_specs, out_specs=out_specs, check_vma=False)
```

```python
import functools

import jax
import jax.numpy as jnp
from jax import lax
from jax.experimental import pallas as pl
from jax.experimental.pallas import tpu as pltpu
from jax.sharding import PartitionSpec as P

ADAM_STEP = 10
BETA_ONE = 0.9
BETA_TWO = 0.95
ADAM_EPS = 1e-8
WEIGHT_DECAY = 0.1
NORM_EPS = 1e-6
ONE_CORR = 1.0 - BETA_ONE ** ADAM_STEP
TWO_CORR = 1.0 - BETA_TWO ** ADAM_STEP
GELU_A = 0.7978845608028654
GELU_B = 0.044715
NT = (((1,), (1,)), ((), ()))
TN = (((0,), (0,)), ((), ()))
MESH = pl.DeviceIdType.MESH
VMEM_MAX = 67_043_328
CHUNK = 256
COLS = 128
SLOTS = 8
AHEAD = 5
SPARE = 1 << 20
F32 = jnp.float32
BF16 = jnp.bfloat16


def gelu_parts(z):
    t = jnp.tanh(GELU_A * (z + GELU_B * (z * z * z)))
    return t, z * (0.5 * (1.0 + t))


def gelu_slope(z, t):
    return 0.5 * (1.0 + t) + 0.5 * z * (1.0 - t * t) * (GELU_A * (1.0 + 3.0 * GELU_B * z * z))


def dot(a, b, dims=(((1,), (0,)), ((), ()))):
    return lax.dot_general(a, b, dims, preferred_element_type=F32)


def positions():
    return lax.axis_index("model"), lax.axis_index("data"), lax.axis_index("stage")


def entry_barrier(peers):
    barrier = pltpu.get_barrier_semaphore()
    for peer in peers:
        pl.semaphore_signal(barrier, inc=1, device_id=peer, device_id_type=MESH)
    pl.semaphore_wait(barrier, len(peers))


def remote(src, dst, send, recv, peer):
    return pltpu.make_async_remote_copy(src_ref=src, dst_ref=dst, send_sem=send, recv_sem=recv, device_id=peer, device_id_type=MESH)


def grad_kernel(n_chunk, width, w1, w2, g1, g2, acts, dy, max_norm, gr1, gr2, clip,
                gs1, gs2, w1b, w2b, gvec, gout, part, part_in, sq1, sq2, sq_out, sq_in,
                w_sem, g_sem, send1, send2, recv1, recv2, part_sem, gvec_sem, sq_send, sq_recv):
    m, d, s = positions()
    peer_x = (m, 1 - d, s)
    peer_y = (1 - m, d, s)
    peer_c = (m, d, 1 - s)
    peer_d = (1 - m, d, 1 - s)

    def loads(j):
        slot = lax.rem(j, 2)
        cols = pl.ds(pl.multiple_of(j * width, width), width)
        return (pltpu.make_async_copy(w1.at[:, cols], w1b.at[slot], w_sem.at[0, slot]),
                pltpu.make_async_copy(w2.at[cols, :], w2b.at[slot], w_sem.at[1, slot]),
                pltpu.make_async_copy(g2.at[cols, :], gs2.at[j], g_sem.at[0, slot]),
                pltpu.make_async_copy(g1.at[:, cols], gs1.at[j], g_sem.at[1, slot]))

    for first in (0, 1):
        for copy in loads(first):
            copy.start()
    entry_barrier((peer_x, peer_y, peer_c, peer_d))

    is_last = s == 1
    hand_over = remote(gout, gvec, gvec_sem.at[0], gvec_sem.at[1], peer_c)
    swap_part = remote(part, part_in, part_sem.at[0], part_sem.at[1], peer_y)

    @pl.when(is_last)
    def _():
        gvec[...] = dy[...]
        part[...] = jnp.zeros_like(part)

    @pl.when(jnp.logical_not(is_last))
    def _():
        hand_over.wait_recv()

    def send_two(j):
        return remote(gs2.at[j], gr2.at[j], send2.at[j], recv2.at[j], peer_x)

    def send_one(j):
        return remote(gs1.at[j], gr1.at[j], send1.at[j], recv1.at[j], peer_x)

    @pl.loop(0, n_chunk)
    def _(j):
        slot = lax.rem(j, 2)
        copies = loads(j)
        copies[0].wait()
        up = w1b[slot].astype(BF16)
        rows = acts[...]
        grad = gvec[...]
        z = dot(rows, up)
        t, act = gelu_parts(z)
        hid = act.astype(BF16)
        copies[2].wait()
        gs2[j] += dot(hid, grad, TN)
        send_two(j).start()
        copies[1].wait()
        grad_hid = dot(grad, w2b[slot].astype(BF16), NT)
        grad_pre = (gelu_slope(z, t) * grad_hid).astype(BF16)
        copies[3].wait()
        gs1[j] += dot(rows, grad_pre, TN)
        send_one(j).start()

        @pl.when(is_last)
        def _():
            part[...] += dot(grad_pre, up, NT)

        @pl.when(j + 2 < n_chunk)
        def _():
            for copy in loads(j + 2):
                copy.start()

    @pl.when(is_last)
    def _():
        swap_part.start()
        swap_part.wait()
        gout[...] = (gvec[...].astype(F32) + (part[...] + part_in[...])).astype(BF16)
        hand_over.start()

    sq1[...] = jnp.zeros_like(sq1)
    sq2[...] = jnp.zeros_like(sq2)

    @pl.loop(0, n_chunk)
    def _(j):
        send_two(j).wait_recv()
        mean = (gs2[j] + gr2[j]) * 0.5
        gr2[j] = mean
        sq2[...] += jnp.sum((mean * mean).reshape(-1, 8, mean.shape[1]), axis=0)
        send_one(j).wait_recv()
        mean = (gs1[j] + gr1[j]) * 0.5
        gr1[j] = mean
        sq1[...] += jnp.sum((mean * mean).reshape(-1, 8, mean.shape[1]), axis=0)

    sq_out[...] = jnp.full(sq_out.shape, jnp.sum(sq1[...]) + jnp.sum(sq2[...]), F32)
    mine = 2 * m + s
    others = ((peer_y, 2 * (1 - m) + s), (peer_c, 2 * m + 1 - s), (peer_d, 2 * (1 - m) + 1 - s))
    shares = [remote(sq_out, sq_in.at[mine], sq_send.at[k], sq_recv.at[mine], peer) for k, (peer, _) in enumerate(others)]
    for copy in shares:
        copy.start()
    sq_in[mine] = sq_out[...]
    for peer, index in others:
        remote(sq_out, sq_in.at[index], sq_send.at[0], sq_recv.at[index], peer).wait_recv()
    total = (sq_in[0] + sq_in[1]) + (sq_in[2] + sq_in[3])
    clip[...] = jnp.minimum(1.0, max_norm[0] / (jnp.sqrt(total) + NORM_EPS))

    for copy in shares:
        copy.wait_send()

    @pl.when(is_last)
    def _():
        hand_over.wait_send()

    @pl.loop(0, n_chunk)
    def _(j):
        send_two(j).wait_send()
        send_one(j).wait_send()


def adamw(scale, step_rate, w, mom, sec, mean):
    grad = scale * mean
    mom_new = BETA_ONE * mom + (1.0 - BETA_ONE) * grad
    sec_new = BETA_TWO * sec + ((1.0 - BETA_TWO) * grad) * grad
    direction = (mom_new * (1.0 / ONE_CORR)) / (jnp.sqrt(sec_new * (1.0 / TWO_CORR)) + ADAM_EPS)
    return w - step_rate * (direction + WEIGHT_DECAY * w), mom_new, sec_new


def update_kernel(first, last, n_up, width, clip, rate, w1, m1, v1, gb1, w2, m2, v2, gb2, x, hid_in,
                  nw1, nm1, nv1, nw2, nm2, nv2, hid, mine, theirs,
                  ring, x_buf, prod, in_sem, out_sem, x_sem):
    m, _, s = positions()
    n_slot = ring.shape[1]
    deep, wide = ring.shape[2:]
    n_micro, half = mine.shape[:2]
    first_col = (first - n_up) // 2 if first > n_up else 0
    scale = clip[0, 0]
    step_rate = rate[0]
    hid_now = hid if first < n_up else hid_in
    load_x = pltpu.make_async_copy(x, x_buf, x_sem)

    def place(i):
        col = pl.multiple_of(((i - n_up) // 2) * wide, wide)
        row = pl.multiple_of(lax.rem(i - n_up, 2) * deep, deep)
        return pl.ds(row, deep), pl.ds(col, wide)

    def start(i, fetch):
        slot = lax.rem(i, n_slot)
        sem = in_sem if fetch else out_sem

        def go(k, far):
            near = ring.at[k, slot]
            pair = (far, near) if fetch else (near, far)
            pltpu.make_async_copy(*pair, sem.at[k, slot]).start()

        if first < n_up:
            @pl.when(i < n_up)
            def _():
                cols = pl.ds(pl.multiple_of(i * wide, wide), wide)
                for k, ref in enumerate((w1, m1, v1) if fetch else (nw1, nm1, nv1)):
                    go(k, ref.at[0, :, cols])

        @pl.when(i >= n_up)
        def _():
            rows, cols = place(i)
            for k, ref in enumerate((w2, m2, v2) if fetch else (nw2, nm2, nv2)):
                go(k, ref.at[0, rows, cols])

    def finish(i, fetch):
        slot = lax.rem(i, n_slot)
        for k, ref in enumerate((w2, m2, v2) if fetch else (nw2, nm2, nv2)):
            far, near = ref.at[0, :deep, :wide], ring.at[k, slot]
            sem = (in_sem if fetch else out_sem).at[k, slot]
            (pltpu.make_async_copy(far, near, sem) if fetch else pltpu.make_async_copy(near, far, sem)).wait()

    for i in range(first, first + AHEAD):
        start(jnp.int32(i), True)
    if first < n_up:
        load_x.start()
        load_x.wait()

    def step(slot, mean):
        new, mom, sec = adamw(scale, step_rate, ring[0, slot], ring[1, slot], ring[2, slot], mean)
        ring[0, slot] = new
        ring[1, slot] = mom
        ring[2, slot] = sec

    def up_chunk(i, slot):
        part = pl.ds(pl.multiple_of(lax.rem(i, width // wide) * wide, wide), wide)
        step(slot, gb1[i // (width // wide), :, part])

        @pl.when(s == 0)
        def _():
            cols = pl.ds(pl.multiple_of(i * wide, wide), wide)
            rows = x_buf[...].reshape(-1, x_buf.shape[2])
            hid[:, cols] = gelu_parts(dot(rows, ring[0, slot].astype(BF16)))[1].astype(BF16)

    def down_chunk(i, slot):
        rows, cols = place(i)
        upper = lax.rem(i - n_up, 2)
        block = deep // gb2.shape[1]
        mean = gb2[pl.ds(upper * block, block), :, cols].reshape(deep, wide)
        step(slot, mean)

        @pl.when(s == 0)
        def _():
            new = dot(hid_now[:, rows], ring[0, slot].astype(BF16)).reshape(prod.shape)

            @pl.when(upper == 0)
            def _():
                prod[...] = new

            @pl.when(upper == 1)
            def _():
                prod[...] += new
                out = pl.ds(pl.multiple_of(((i - n_up) // 2 - first_col) * wide, wide), wide)
                for k in range(n_micro):
                    mine[k, :, out] = prod[k, pl.ds(pl.multiple_of(m * half, half), half), :]
                    theirs[k, :, out] = prod[k, pl.ds(pl.multiple_of((1 - m) * half, half), half), :]

    @pl.loop(first, last)
    def _(i):
        slot = lax.rem(i, n_slot)
        finish(i, True)
        if first < n_up:
            @pl.when(i < n_up)
            def _():
                up_chunk(i, slot)

        @pl.when(i >= n_up)
        def _():
            down_chunk(i, slot)

        start(i, False)

        @pl.when(i + AHEAD < last)
        def _():
            @pl.when(i + AHEAD - n_slot >= first)
            def _():
                finish(i + AHEAD - n_slot, False)
            start(i + AHEAD, True)

    for i in range(last - n_slot, last):
        finish(jnp.int32(i), False)


def update_first(n_up, width, last, clip, rate, w1, m1, v1, gb1, w2, m2, v2, gb2, x, *rest):
    update_kernel(0, last, n_up, width, clip, rate, w1, m1, v1, gb1, w2, m2, v2, gb2, x, None, *rest)


def update_second(n_up, width, first, last, clip, rate, w2, m2, v2, gb2, hid, _w, _m, _v, nw2, nm2, nv2, mine, theirs, *scratch):
    update_kernel(first, last, n_up, width, clip, rate, None, None, None, None, w2, m2, v2, gb2, None, hid,
                  None, None, None, nw2, nm2, nv2, None, mine, theirs, *scratch)


def forward_kernel(n_chunk, n_micro, half, width, cut, mine_a, got_a, mine_b, theirs_b, x, nw1, nw2, y,
                   w1, w2, w1f, w2f, got_b, own_half, act, peer_half, part, part_in,
                   w_sem, a_send, a_recv, o_send, o_recv, p_send, p_recv, y_send, y_recv, f_send, f_recv):
    m, d, s = positions()
    peer_y = (1 - m, d, s)
    peer_c = (m, d, 1 - s)
    peer_d = (1 - m, d, 1 - s)

    def loads(j):
        slot = lax.rem(j, 2)
        cols = pl.ds(pl.multiple_of(j * width, width), width)
        return (pltpu.make_async_copy(nw1.at[0, :, cols], w1f.at[slot], w_sem.at[0, slot]),
                pltpu.make_async_copy(nw2.at[0, cols, :], w2f.at[slot], w_sem.at[1, slot]))

    @pl.when(s == 1)
    def _():
        for first in (0, 1):
            for copy in loads(first):
                copy.start()

    entry_barrier((peer_y, peer_c, peer_d))
    mine = pl.ds(pl.multiple_of(m * half, half), half)
    theirs = pl.ds(pl.multiple_of((1 - m) * half, half), half)

    def send_first(k):
        return remote(theirs_b.at[k], got_b.at[k], a_send.at[k], a_recv.at[k], peer_y)

    def give_core(k):
        return remote(own_half.at[k], act.at[k, mine, :], o_send.at[0, k], o_recv.at[0, k], peer_c)

    def give_diag(k):
        return remote(own_half.at[k], act.at[k, mine, :], o_send.at[1, k], o_recv.at[1, k], peer_d)

    def send_part(k):
        return remote(part.at[k, theirs, :], part_in.at[k], p_send.at[k], p_recv.at[k], peer_y)

    def swap_y(k):
        return remote(own_half.at[k], peer_half.at[k], y_send.at[0, k], y_recv.at[0, k], peer_y)

    def give_own(k):
        return remote(own_half.at[k], y.at[k, mine, :], y_send.at[1, k], y_recv.at[1, k], peer_c)

    def pass_on(k):
        return remote(peer_half.at[k], y.at[k, theirs, :], f_send.at[k], f_recv.at[k], peer_c)

    @pl.when(s == 0)
    def _():
        send_first(0).start()
        for k in range(n_micro):
            if k + 1 < n_micro:
                send_first(k + 1).start()
            rows = x[k, mine, :].astype(F32)
            own_half[k, :, :cut] = (rows[:, :cut] + (mine_a[k] + got_a[k])).astype(BF16)
            send_first(k).wait_recv()
            own_half[k, :, cut:] = (rows[:, cut:] + (mine_b[k] + got_b[k])).astype(BF16)
            give_diag(k).start()
            give_core(k).start()
        for k in range(n_micro):
            give_own(k).wait_recv()
            pass_on(k).wait_recv()
        for k in range(n_micro):
            send_first(k).wait_send()
            give_core(k).wait_send()
            give_diag(k).wait_send()

    @pl.when(s == 1)
    def _():
        @pl.loop(0, n_chunk)
        def _(j):
            slot = lax.rem(j, 2)
            copies = loads(j)
            copies[0].wait()
            w1[j] = w1f[slot].astype(BF16)
            copies[1].wait()
            w2[j] = w2f[slot].astype(BF16)

            @pl.when(j + 2 < n_chunk)
            def _():
                for copy in loads(j + 2):
                    copy.start()

        def finish(k):
            send_part(k).wait_recv()
            out = act[k, mine, :].astype(F32) + (part[k, mine, :] + part_in[k])
            own_half[k] = out.astype(BF16)
            swap_y(k).start()
            give_own(k).start()
            y[k, mine, :] = own_half[k]

        for k in range(n_micro):
            give_core(k).wait_recv()
            give_diag(k).wait_recv()
            part[k] = jnp.zeros_like(part[k])

            @pl.loop(0, n_chunk)
            def _(j):
                hid = gelu_parts(dot(act[k], w1[j]))[1].astype(BF16)
                part[k] += dot(hid, w2[j])

            send_part(k).start()
            if k > 0:
                finish(k - 1)
        finish(n_micro - 1)
        for k in range(n_micro):
            swap_y(k).wait_recv()
            pass_on(k).start()
            y[k, theirs, :] = peer_half[k]
        for k in range(n_micro):
            send_part(k).wait_send()
            swap_y(k).wait_send()
            give_own(k).wait_send()
            pass_on(k).wait_send()


def solution(mesh):
    up_spec = P('stage', None, 'model')
    down_spec = P('stage', 'model', None)
    row_spec = P(None, 'data', None)
    in_specs = (up_spec, down_spec, up_spec, down_spec, up_spec, down_spec, P('data', 'stage', None, 'model'), P('data', 'stage', 'model', None), P('stage', 'data', None), P('data', None), row_spec, P(None), P(None))
    out_specs = (up_spec, down_spec, up_spec, down_spec, up_spec, down_spec, row_spec)

    def device_step(w_up, w_down, m_up, m_down, v_up, v_down, g_up, g_down, acts_last, grad_out, x_next, learn_rate, max_norm):
        d_model, ff = w_up.shape[1:]
        rows = grad_out.shape[0]
        n_micro = x_next.shape[0]
        width = CHUNK
        n_chunk = ff // width
        half = rows // 2
        hbm = pl.BlockSpec(memory_space=pl.ANY)
        vmem = pl.BlockSpec(memory_space=pltpu.VMEM)
        smem = pl.BlockSpec(memory_space=pltpu.SMEM)
        dma = pltpu.SemaphoreType.DMA

        resident = 4 * 2 * d_model * ff
        mean_up, mean_down, clip = pl.pallas_call(
            functools.partial(grad_kernel, n_chunk, width),
            out_shape=(pltpu.VMEM((n_chunk, d_model, width), F32),
                       pltpu.VMEM((n_chunk, width, d_model), F32),
                       jax.ShapeDtypeStruct((8, 128), F32)),
            in_specs=[hbm, hbm, hbm, hbm, vmem, vmem, smem],
            out_specs=(vmem, vmem, vmem),
            scratch_shapes=[
                pltpu.VMEM((n_chunk, d_model, width), F32),
                pltpu.VMEM((n_chunk, width, d_model), F32),
                pltpu.VMEM((2, d_model, width), F32),
                pltpu.VMEM((2, width, d_model), F32),
                pltpu.VMEM((rows, d_model), BF16),
                pltpu.VMEM((rows, d_model), BF16),
                pltpu.VMEM((rows, d_model), F32),
                pltpu.VMEM((rows, d_model), F32),
                pltpu.VMEM((8, width), F32),
                pltpu.VMEM((8, d_model), F32),
                pltpu.VMEM((8, 128), F32),
                pltpu.VMEM((4, 8, 128), F32),
                dma((2, 2)), dma((2, 2)),
                dma((n_chunk,)), dma((n_chunk,)), dma((n_chunk,)), dma((n_chunk,)),
                dma((2,)), dma((2,)), dma((3,)), dma((4,)),
            ],
            compiler_params=pltpu.CompilerParams(collective_id=0, has_side_effects=True, vmem_limit_bytes=VMEM_MAX - resident - SPARE),
            name="grad_exchange",
        )(w_up[0], w_down[0], g_up[0, 0], g_down[0, 0], acts_last[0], grad_out, max_norm)

        n_up = ff // COLS
        n_first = d_model // COLS // 2
        cut = n_first * COLS
        last = n_up + 2 * (d_model // COLS)
        middle = n_up + 2 * n_first
        up_out = jax.ShapeDtypeStruct(w_up.shape, F32)
        down_out = jax.ShapeDtypeStruct(w_down.shape, F32)
        part_a = jax.ShapeDtypeStruct((n_micro, half, cut), F32)
        part_b = jax.ShapeDtypeStruct((n_micro, half, d_model - cut), F32)

        def scratch(x_shape):
            return [pltpu.VMEM((3, SLOTS, d_model, COLS), F32),
                    pltpu.VMEM(x_shape, BF16),
                    pltpu.VMEM((n_micro, rows, COLS), F32),
                    dma((3, SLOTS)), dma((3, SLOTS)), dma(())]

        def cost(units):
            return pl.CostEstimate(flops=2 * n_micro * rows * units, bytes_accessed=24 * units, transcendentals=2 * units)

        def stay(array):
            return pltpu.with_memory_space_constraint(array, pltpu.VMEM)

        params = pltpu.CompilerParams(vmem_limit_bytes=VMEM_MAX - resident - 2 * SPARE)
        nw1, nm1, nv1, nw2, nm2, nv2, hid, mine_a, theirs_a = pl.pallas_call(
            functools.partial(update_first, n_up, width, middle),
            out_shape=(up_out, up_out, up_out, down_out, down_out, down_out,
                       jax.ShapeDtypeStruct((n_micro * rows, ff), BF16), part_a, part_a),
            in_specs=[smem, smem, hbm, hbm, hbm, vmem, hbm, hbm, hbm, vmem, hbm],
            out_specs=(hbm, hbm, hbm, hbm, hbm, hbm, vmem, vmem, vmem),
            scratch_shapes=scratch(x_next.shape),
            compiler_params=params,
            cost_estimate=cost(d_model * ff + cut * ff),
            name="update_first",
        )(clip, learn_rate, w_up, m_up, v_up, stay(mean_up), w_down, m_down, v_down, stay(mean_down), x_next)

        got_a = lax.ppermute(theirs_a, ('model', 'stage'), [(0, 2), (2, 0)])

        nw2, nm2, nv2, mine_b, theirs_b = pl.pallas_call(
            functools.partial(update_second, n_up, width, middle, last),
            out_shape=(down_out, down_out, down_out, part_b, part_b),
            in_specs=[smem, smem, hbm, hbm, hbm, vmem, vmem, hbm, hbm, hbm],
            out_specs=(hbm, hbm, hbm, vmem, vmem),
            scratch_shapes=scratch((1, 8, 128)),
            input_output_aliases={7: 0, 8: 1, 9: 2},
            compiler_params=params,
            cost_estimate=cost((d_model - cut) * ff),
            name="update_second",
        )(clip, learn_rate, w_down, m_down, v_down, stay(mean_down), hid, nw2, nm2, nv2)

        y_next = pl.pallas_call(
            functools.partial(forward_kernel, n_chunk, n_micro, half, width, cut),
            out_shape=jax.ShapeDtypeStruct(x_next.shape, BF16),
            in_specs=[vmem, vmem, vmem, vmem, vmem, hbm, hbm],
            out_specs=vmem,
            scratch_shapes=[
                pltpu.VMEM((n_chunk, d_model, width), BF16),
                pltpu.VMEM((n_chunk, width, d_model), BF16),
                pltpu.VMEM((2, d_model, width), F32),
                pltpu.VMEM((2, width, d_model), F32),
                pltpu.VMEM((n_micro, half, d_model - cut), F32),
                pltpu.VMEM((n_micro, half, d_model), BF16),
                pltpu.VMEM((n_micro, rows, d_model), BF16),
                pltpu.VMEM((n_micro, half, d_model), BF16),
                pltpu.VMEM((n_micro, rows, d_model), F32),
                pltpu.VMEM((n_micro, half, d_model), F32),
                dma((2, 2)), dma((n_micro,)), dma((n_micro,)), dma((2, n_micro)), dma((2, n_micro)),
                dma((n_micro,)), dma((n_micro,)), dma((2, n_micro)), dma((2, n_micro)), dma((n_micro,)), dma((n_micro,)),
            ],
            compiler_params=pltpu.CompilerParams(collective_id=1, has_side_effects=True, vmem_limit_bytes=VMEM_MAX),
            name="forward_exchange",
        )(mine_a, got_a, mine_b, theirs_b, x_next, nw1, nw2)
        return nw1, nw2, nm1, nm2, nv1, nv2, y_next

    return jax.shard_map(device_step, mesh=mesh, in_specs=in_specs, out_specs=out_specs, check_vma=False)
```

```python
import functools

import jax
import jax.numpy as jnp
from jax import lax
from jax.experimental import pallas as pl
from jax.experimental.pallas import tpu as pltpu
from jax.sharding import PartitionSpec as P

ADAM_STEP = 10
BETA_ONE = 0.9
BETA_TWO = 0.95
ADAM_EPS = 1e-8
WEIGHT_DECAY = 0.1
NORM_EPS = 1e-6
ONE_CORR = 1.0 - BETA_ONE ** ADAM_STEP
TWO_CORR = 1.0 - BETA_TWO ** ADAM_STEP
ROOT_EPS = ADAM_EPS * TWO_CORR ** 0.5
ROOT_GAIN = TWO_CORR ** 0.5 / ONE_CORR
TINY = 1.1754944e-38
HUGE = 3.4028235e38
GELU_A = 0.7978845608028654
GELU_B = 0.044715
NT = (((1,), (1,)), ((), ()))
TN = (((0,), (0,)), ((), ()))
MESH = pl.DeviceIdType.MESH
VMEM_MAX = 67_043_328
CHUNK = 128
SLOTS = 8
AHEAD = 5
SPARE = 1 << 20
F32 = jnp.float32
BF16 = jnp.bfloat16


def gelu_parts(z):
    t = jnp.tanh(GELU_A * (z + GELU_B * (z * z * z)))
    return t, z * (0.5 * (1.0 + t))


def gelu_slope(z, t):
    return 0.5 * (1.0 + t) + 0.5 * z * (1.0 - t * t) * (GELU_A * (1.0 + 3.0 * GELU_B * z * z))


def dot(a, b, dims=(((1,), (0,)), ((), ()))):
    return lax.dot_general(a, b, dims, preferred_element_type=F32)


def positions():
    return lax.axis_index("model"), lax.axis_index("data"), lax.axis_index("stage")


def entry_barrier(peers):
    barrier = pltpu.get_barrier_semaphore()
    for peer in peers:
        pl.semaphore_signal(barrier, inc=1, device_id=peer, device_id_type=MESH)
    pl.semaphore_wait(barrier, len(peers))


def remote(src, dst, send, recv, peer):
    return pltpu.make_async_remote_copy(src_ref=src, dst_ref=dst, send_sem=send, recv_sem=recv, device_id=peer, device_id_type=MESH)


def adamw(scale, rate, w, mom, sec, mean):
    grad = scale * mean
    mom_new = BETA_ONE * mom + (1.0 - BETA_ONE) * grad
    sec_new = BETA_TWO * sec + ((1.0 - BETA_TWO) * grad) * grad
    root = sec_new * lax.rsqrt(jnp.minimum(sec_new + TINY, HUGE))
    w_new = w * (1.0 - rate * WEIGHT_DECAY) - (rate * ROOT_GAIN) * (mom_new / (root + ROOT_EPS))
    return w_new, mom_new, sec_new


def grad_kernel(n_chunk, width, w1, w2, g1, g2, m1, v1, m2, v2, acts, dy, x, max_norm, rate,
                gr1, gr2, clip, act_half,
                gs1, gs2, w1b, w2b, gvec, part, got, x_buf, sq1, sq2, sq_out, sq_in,
                w_sem, g_sem, send1, send2, recv1, recv2, part_sem, gvec_sem, sq_send, sq_recv,
                row_sem, f_sem, rs_send, rs_recv):
    m, d, s = positions()
    peer_x = (m, 1 - d, s)
    peer_y = (1 - m, d, s)
    peer_c = (m, d, 1 - s)
    peer_d = (1 - m, d, 1 - s)
    d_model = w1.shape[0]
    is_last = s == 1
    is_first = s == 0

    def loads(j):
        slot = lax.rem(j, 2)
        cols = pl.ds(pl.multiple_of(j * width, width), width)
        return (pltpu.make_async_copy(w1.at[:, cols], w1b.at[slot], w_sem.at[0, slot]),
                pltpu.make_async_copy(w2.at[cols, :], w2b.at[slot], w_sem.at[1, slot]),
                pltpu.make_async_copy(g2.at[cols, :], gs2.at[j], g_sem.at[0, slot]),
                pltpu.make_async_copy(g1.at[:, cols], gs1.at[j], g_sem.at[1, slot]))

    load_dy = pltpu.make_async_copy(dy, gvec, row_sem)
    load_x = pltpu.make_async_copy(x, x_buf, row_sem)

    @pl.when(is_last)
    def _():
        load_dy.start()

    for first in (0, 1):
        for copy in loads(first):
            copy.start()

    @pl.when(is_first)
    def _():
        load_x.start()

    entry_barrier((peer_x, peer_y, peer_c, peer_d))

    hand_over = remote(x_buf.at[0], gvec, gvec_sem.at[0], gvec_sem.at[1], peer_c)
    swap_part = remote(part, got.at[:2], part_sem.at[0], part_sem.at[1], peer_y)

    @pl.when(is_last)
    def _():
        part[...] = jnp.zeros_like(part)
        load_dy.wait()

    @pl.when(is_first)
    def _():
        load_x.wait()
        hand_over.wait_recv()

    def send_two(j):
        return remote(gs2.at[j], gr2.at[j], send2.at[j], recv2.at[j], peer_x)

    def send_one(j):
        return remote(gs1.at[j], gr1.at[j], send1.at[j], recv1.at[j], peer_x)

    @pl.loop(0, n_chunk)
    def _(j):
        slot = lax.rem(j, 2)
        copies = loads(j)
        copies[0].wait()
        up = w1b[slot].astype(BF16)
        rows = acts[...]
        grad = gvec[...]
        z = dot(rows, up)
        t, act = gelu_parts(z)
        hid = act.astype(BF16)
        copies[2].wait()
        gs2[j] += dot(hid, grad, TN)
        send_two(j).start()
        copies[1].wait()
        grad_hid = dot(grad, w2b[slot].astype(BF16), NT)
        grad_pre = (gelu_slope(z, t) * grad_hid).astype(BF16)
        copies[3].wait()
        gs1[j] += dot(rows, grad_pre, TN)
        send_one(j).start()

        @pl.when(is_last)
        def _():
            part[...] += dot(grad_pre, up, NT).reshape(part.shape)

        @pl.when(j + 2 < n_chunk)
        def _():
            for copy in loads(j + 2):
                copy.start()

    @pl.when(is_last)
    def _():
        swap_part.start()
        swap_part.wait()
        total = (part[...] + got[:2]).reshape(gvec.shape)
        x_buf[0] = (gvec[...].astype(F32) + total).astype(BF16)
        hand_over.start()

    n_up = n_chunk // 2
    n_pair = 2 * n_up

    def fetch(p):
        base = lax.rem(p, 3) * 6

        @pl.when(p < n_up)
        def _():
            for q, ref in enumerate((w1, m1, v1)):
                for h in (0, 1):
                    cols = pl.ds(pl.multiple_of((2 * p + h) * width, width), width)
                    pltpu.make_async_copy(ref.at[:, cols], gs1.at[base + 2 * q + h], f_sem.at[base + 2 * q + h]).start()

        @pl.when(p >= n_up)
        def _():
            rows = pl.ds(pl.multiple_of(lax.rem(p - n_up, 2) * d_model, d_model), d_model)
            for q, ref in enumerate((w2, m2, v2)):
                for h in (0, 1):
                    cols = pl.ds(pl.multiple_of((2 * ((p - n_up) // 2) + h) * width, width), width)
                    pltpu.make_async_copy(ref.at[rows, cols], gs1.at[base + 2 * q + h], f_sem.at[base + 2 * q + h]).start()

    def free_and_fetch(lo, hi, p):
        for i in range(lo, hi):
            send_one(i).wait_send()

        @pl.when(is_first)
        def _():
            fetch(jnp.int32(p))

    sq1[...] = jnp.zeros_like(sq1)
    sq2[...] = jnp.zeros_like(sq2)

    @pl.loop(0, n_chunk)
    def _(j):
        send_two(j).wait_recv()
        mean = (gs2[j] + gr2[j]) * 0.5
        gr2[j] = mean
        sq2[...] += jnp.sum((mean * mean).reshape(-1, 8, mean.shape[1]), axis=0)
        send_one(j).wait_recv()
        mean = (gs1[j] + gr1[j]) * 0.5
        gr1[j] = mean
        sq1[...] += jnp.sum((mean * mean).reshape(-1, 8, mean.shape[1]), axis=0)

        @pl.when(j == 10)
        def _():
            free_and_fetch(0, 6, 0)

        @pl.when(j == 15)
        def _():
            free_and_fetch(6, 12, 1)

    sq_out[...] = jnp.full(sq_out.shape, jnp.sum(sq1[...]) + jnp.sum(sq2[...]), F32)
    mine = 2 * m + s
    others = ((peer_y, 2 * (1 - m) + s), (peer_c, 2 * m + 1 - s), (peer_d, 2 * (1 - m) + 1 - s))
    shares = [remote(sq_out, sq_in.at[mine], sq_send.at[k], sq_recv.at[mine], peer) for k, (peer, _) in enumerate(others)]
    for copy in shares:
        copy.start()
    free_and_fetch(12, n_chunk, 2)
    sq_in[mine] = sq_out[...]
    for peer, index in others:
        remote(sq_out, sq_in.at[index], sq_send.at[0], sq_recv.at[index], peer).wait_recv()
    total = (sq_in[0] + sq_in[1]) + (sq_in[2] + sq_in[3])
    clip[...] = jnp.minimum(1.0, max_norm[0] / (jnp.sqrt(total) + NORM_EPS))

    for j in range(n_chunk):
        send_two(j).wait_send()
    for copy in shares:
        copy.wait_send()

    @pl.when(is_last)
    def _():
        hand_over.wait_send()

    @pl.when(is_first)
    def _():
        scale = clip[0, 0]
        step_rate = rate[0]
        n_micro, n_row = x_buf.shape[:2]
        group = 2 * n_micro
        half = n_row // 2
        wide = 2 * width
        n_block = d_model // wide

        def new_weights(base, means):
            parts = [adamw(scale, step_rate, gs1[base + h], gs1[base + 2 + h], gs1[base + 4 + h], means[h])[0].astype(BF16) for h in (0, 1)]
            return jnp.concatenate(parts, axis=1)

        def block_copy(c):
            cols = pl.ds(pl.multiple_of(c * wide, wide), wide)
            return remote(gs2.at[2 * group + n_micro:2 * group + 2 * n_micro, :, cols], got.at[:, :, cols], rs_send.at[c], rs_recv.at[c], peer_y)

        @pl.loop(0, n_pair)
        def _(p):
            base = lax.rem(p, 3) * 6
            for i in range(6):
                pltpu.make_async_copy(w1.at[:, :width], gs1.at[base + i], f_sem.at[base + i]).wait()

            @pl.when(p < n_up)
            def _():
                new = new_weights(base, [gr1[2 * p], gr1[2 * p + 1]])
                act = gelu_parts(dot(x_buf[...].reshape(-1, d_model), new))[1].astype(BF16).astype(F32)
                cols = pl.ds(pl.multiple_of(lax.rem(p, n_block) * wide, wide), wide)
                gs2[pl.ds((p // n_block) * group, group), :, cols] = act.reshape(group, half, wide)

            @pl.when(p >= n_up)
            def _():
                c = (p - n_up) // 2
                upper = lax.rem(p - n_up, 2)
                means = []
                for h in (0, 1):
                    cols = pl.ds(pl.multiple_of((2 * c + h) * width, width), width)
                    means.append(gr2[pl.ds(upper * n_up, n_up), :, cols].reshape(d_model, width))
                new = new_weights(base, means)
                cols = pl.ds(pl.multiple_of(c * wide, wide), wide)
                spot = [(g // n_block, slice(None), slice(g % n_block * wide, g % n_block * wide + wide)) for g in range(group)]
                for lo in range(0, group, n_micro):
                    rows = gs2[pl.ds(upper * group + lo, n_micro)].reshape(-1, d_model).astype(BF16)
                    res = dot(rows, new).reshape(n_micro, half, wide)

                    @pl.when(upper == 0)
                    def _():
                        for g in range(n_micro):
                            part[spot[lo + g]] = res[g]

                    @pl.when(upper == 1)
                    def _():
                        for g in range(n_micro):
                            part[spot[lo + g]] += res[g]

                @pl.when(upper == 1)
                def _():
                    for k in range(n_micro):
                        even, odd = part[spot[2 * k]], part[spot[2 * k + 1]]
                        gs2[2 * group + k, :, cols] = jnp.where(m == 0, even, odd)
                        gs2[2 * group + n_micro + k, :, cols] = jnp.where(m == 0, odd, even)
                    block_copy(c).start()

            @pl.when(p + 3 < n_pair)
            def _():
                fetch(p + 3)

        for c in range(n_block):
            block_copy(c).wait_recv()
            cols = slice(c * wide, (c + 1) * wide)
            for k in range(n_micro):
                rows = x_buf[k, pl.ds(pl.multiple_of(m * half, half), half), cols].astype(F32)
                act_half[k, :, cols] = (rows + (gs2[2 * group + k, :, cols] + got[k, :, cols])).astype(BF16)
        for c in range(n_block):
            block_copy(c).wait_send()


def update_kernel(clip, rate, w1, m1, v1, gb1, w2, m2, v2, gb2, nw1, nm1, nv1, nw2, nm2, nv2, ring, in_sem, out_sem):
    n_up, deep, wide = gb1.shape
    n_slot = ring.shape[1]
    last = 2 * n_up
    block = deep // gb2.shape[1]
    scale = clip[0, 0]
    step_rate = rate[0]

    def place(i):
        col = pl.multiple_of(((i - n_up) // 2) * wide, wide)
        row = pl.multiple_of(lax.rem(i - n_up, 2) * deep, deep)
        return pl.ds(row, deep), pl.ds(col, wide)

    def start(i, fetch):
        slot = lax.rem(i, n_slot)
        sem = in_sem if fetch else out_sem

        def go(k, far):
            near = ring.at[k, slot]
            pair = (far, near) if fetch else (near, far)
            pltpu.make_async_copy(*pair, sem.at[k, slot]).start()

        @pl.when(i < n_up)
        def _():
            cols = pl.ds(pl.multiple_of(i * wide, wide), wide)
            for k, ref in enumerate((w1, m1, v1) if fetch else (nw1, nm1, nv1)):
                go(k, ref.at[0, :, cols])

        @pl.when(i >= n_up)
        def _():
            rows, cols = place(i)
            for k, ref in enumerate((w2, m2, v2) if fetch else (nw2, nm2, nv2)):
                go(k, ref.at[0, rows, cols])

    def finish(i, fetch):
        slot = lax.rem(i, n_slot)
        for k, ref in enumerate((w2, m2, v2) if fetch else (nw2, nm2, nv2)):
            far, near = ref.at[0, :deep, :wide], ring.at[k, slot]
            sem = (in_sem if fetch else out_sem).at[k, slot]
            (pltpu.make_async_copy(far, near, sem) if fetch else pltpu.make_async_copy(near, far, sem)).wait()

    for i in range(AHEAD):
        start(jnp.int32(i), True)

    def step(slot, mean):
        new, mom, sec = adamw(scale, step_rate, ring[0, slot], ring[1, slot], ring[2, slot], mean)
        ring[0, slot] = new
        ring[1, slot] = mom
        ring[2, slot] = sec

    @pl.loop(0, last)
    def _(i):
        slot = lax.rem(i, n_slot)
        finish(i, True)

        @pl.when(i < n_up)
        def _():
            step(slot, gb1[i])

        @pl.when(i >= n_up)
        def _():
            cols = place(i)[1]
            step(slot, gb2[pl.ds(lax.rem(i - n_up, 2) * block, block), :, cols].reshape(deep, wide))

        start(i, False)

        @pl.when(i + AHEAD < last)
        def _():
            @pl.when(i + AHEAD - n_slot >= 0)
            def _():
                finish(i + AHEAD - n_slot, False)
            start(i + AHEAD, True)

    for i in range(last - n_slot, last):
        finish(jnp.int32(i), False)


def forward_kernel(n_chunk, width, from_core, from_diag, nw1, nw2, y,
                   w1, w2, w1f, w2f, act, own_half, peer_half, part, part_in,
                   w_sem, p_send, p_recv, y_send, y_recv, f_send, f_recv, ready):
    m, d, s = positions()
    n_micro, half = own_half.shape[:2]
    peer_y = (1 - m, d, s)
    peer_c = (m, d, 1 - s)

    def loads(j):
        slot = lax.rem(j, 2)
        cols = pl.ds(pl.multiple_of(j * width, width), width)
        return (pltpu.make_async_copy(nw1.at[0, :, cols], w1f.at[slot], w_sem.at[0, slot]),
                pltpu.make_async_copy(nw2.at[0, cols, :], w2f.at[slot], w_sem.at[1, slot]))

    barrier = pltpu.get_barrier_semaphore()

    @pl.when(s == 1)
    def _():
        for first in (0, 1):
            for copy in loads(first):
                copy.start()
        pl.semaphore_signal(barrier, inc=1, device_id=peer_y, device_id_type=MESH)
        pl.semaphore_signal(barrier, inc=1, device_id=peer_c, device_id_type=MESH)

    pl.semaphore_wait(barrier, 1)

    @pl.when(s == 0)
    def _():
        pl.semaphore_signal(ready, inc=1, device_id=peer_c, device_id_type=MESH)

    mine = pl.ds(pl.multiple_of(m * half, half), half)
    theirs = pl.ds(pl.multiple_of((1 - m) * half, half), half)

    def send_part(k):
        return remote(part.at[k, theirs, :], part_in.at[k], p_send.at[k], p_recv.at[k], peer_y)

    def swap_y(k):
        return remote(own_half.at[k], peer_half.at[k], y_send.at[0, k], y_recv.at[0, k], peer_y)

    def give_own(k):
        return remote(own_half.at[k], y.at[k, mine, :], y_send.at[1, k], y_recv.at[1, k], peer_c)

    def pass_on(k):
        return remote(peer_half.at[k], y.at[k, theirs, :], f_send.at[k], f_recv.at[k], peer_c)

    @pl.when(s == 0)
    def _():
        for k in range(n_micro):
            give_own(k).wait_recv()
            pass_on(k).wait_recv()

    @pl.when(s == 1)
    def _():
        act[:, mine, :] = from_core[...]
        act[:, theirs, :] = from_diag[...]

        def chunk(k, j):
            hid = gelu_parts(dot(act[k], w1[j]))[1].astype(BF16)
            part[k] += dot(hid, w2[j])

        def finish(k):
            send_part(k).wait_recv()
            out = act[k, mine, :].astype(F32) + (part[k, mine, :] + part_in[k])
            own_half[k] = out.astype(BF16)
            swap_y(k).start()
            y[k, mine, :] = own_half[k]

        for k in range(n_micro):
            part[k] = jnp.zeros_like(part[k])

            @pl.loop(0, n_chunk)
            def _(j):
                if k == 0:
                    slot = lax.rem(j, 2)
                    copies = loads(j)
                    copies[0].wait()
                    w1[j] = w1f[slot].astype(BF16)
                    copies[1].wait()
                    w2[j] = w2f[slot].astype(BF16)

                    @pl.when(j + 2 < n_chunk)
                    def _():
                        for copy in loads(j + 2):
                            copy.start()
                chunk(k, j)

            send_part(k).start()
            if k > 0:
                finish(k - 1)
        finish(n_micro - 1)
        pl.semaphore_wait(ready, 1)
        for k in range(n_micro):
            give_own(k).start()
        for k in range(n_micro):
            swap_y(k).wait_recv()
            pass_on(k).start()
            y[k, theirs, :] = peer_half[k]
        for k in range(n_micro):
            send_part(k).wait_send()
            swap_y(k).wait_send()
            give_own(k).wait_send()
            pass_on(k).wait_send()


def solution(mesh):
    up_spec = P('stage', None, 'model')
    down_spec = P('stage', 'model', None)
    row_spec = P(None, 'data', None)
    in_specs = (up_spec, down_spec, up_spec, down_spec, up_spec, down_spec, P('data', 'stage', None, 'model'), P('data', 'stage', 'model', None), P('stage', 'data', None), P('data', None), row_spec, P(None), P(None))
    out_specs = (up_spec, down_spec, up_spec, down_spec, up_spec, down_spec, row_spec)

    def device_step(w_up, w_down, m_up, m_down, v_up, v_down, g_up, g_down, acts_last, grad_out, x_next, learn_rate, max_norm):
        d_model, ff = w_up.shape[1:]
        rows = grad_out.shape[0]
        n_micro = x_next.shape[0]
        width = CHUNK
        n_chunk = ff // width
        half = rows // 2
        hbm = pl.BlockSpec(memory_space=pl.ANY)
        vmem = pl.BlockSpec(memory_space=pltpu.VMEM)
        smem = pl.BlockSpec(memory_space=pltpu.SMEM)
        dma = pltpu.SemaphoreType.DMA
        resident = 4 * 2 * d_model * ff
        n_block = d_model // (2 * width)

        mean_up, mean_down, clip, act_half = pl.pallas_call(
            functools.partial(grad_kernel, n_chunk, width),
            out_shape=(pltpu.VMEM((n_chunk, d_model, width), F32),
                       pltpu.VMEM((n_chunk, width, d_model), F32),
                       jax.ShapeDtypeStruct((8, 128), F32),
                       jax.ShapeDtypeStruct((n_micro, half, d_model), BF16)),
            in_specs=[hbm] * 8 + [vmem, hbm, hbm, smem, smem],
            out_specs=(vmem, vmem, vmem, vmem),
            scratch_shapes=[
                pltpu.VMEM((n_chunk, d_model, width), F32),
                pltpu.VMEM((n_chunk, width, d_model), F32),
                pltpu.VMEM((2, d_model, width), F32),
                pltpu.VMEM((2, width, d_model), F32),
                pltpu.VMEM((rows, d_model), BF16),
                pltpu.VMEM((2, half, d_model), F32),
                pltpu.VMEM((n_micro, half, d_model), F32),
                pltpu.VMEM((n_micro, rows, d_model), BF16),
                pltpu.VMEM((8, width), F32),
                pltpu.VMEM((8, d_model), F32),
                pltpu.VMEM((8, 128), F32),
                pltpu.VMEM((4, 8, 128), F32),
                dma((2, 2)), dma((2, 2)),
                dma((n_chunk,)), dma((n_chunk,)), dma((n_chunk,)), dma((n_chunk,)),
                dma((2,)), dma((2,)), dma((3,)), dma((4,)),
                dma(()), dma((18,)), dma((n_block,)), dma((n_block,)),
            ],
            compiler_params=pltpu.CompilerParams(collective_id=0, has_side_effects=True, vmem_limit_bytes=VMEM_MAX - resident - SPARE),
            name="grad_exchange",
        )(w_up[0], w_down[0], g_up[0, 0], g_down[0, 0], m_up[0], v_up[0], m_down[0], v_down[0], acts_last[0], grad_out, x_next, max_norm, learn_rate)

        from_diag = lax.ppermute(act_half, ('model', 'stage'), [(0, 3), (2, 1)])
        from_core = lax.ppermute(act_half, ('model', 'stage'), [(0, 1), (2, 3)])

        def stay(array):
            return pltpu.with_memory_space_constraint(array, pltpu.VMEM)

        up_out = jax.ShapeDtypeStruct(w_up.shape, F32)
        down_out = jax.ShapeDtypeStruct(w_down.shape, F32)
        nw1, nm1, nv1, nw2, nm2, nv2 = pl.pallas_call(
            update_kernel,
            out_shape=(up_out, up_out, up_out, down_out, down_out, down_out),
            in_specs=[smem, smem, hbm, hbm, hbm, vmem, hbm, hbm, hbm, vmem],
            out_specs=(hbm,) * 6,
            scratch_shapes=[pltpu.VMEM((3, SLOTS, d_model, width), F32), dma((3, SLOTS)), dma((3, SLOTS))],
            compiler_params=pltpu.CompilerParams(vmem_limit_bytes=VMEM_MAX - resident - SPARE),
            cost_estimate=pl.CostEstimate(flops=2000 * d_model * ff, bytes_accessed=48 * d_model * ff, transcendentals=4 * d_model * ff),
            name="update",
        )(clip, learn_rate, w_up, m_up, v_up, stay(mean_up), w_down, m_down, v_down, stay(mean_down))

        f_width = 2 * width
        f_chunk = ff // f_width
        y_next = pl.pallas_call(
            functools.partial(forward_kernel, f_chunk, f_width),
            out_shape=jax.ShapeDtypeStruct(x_next.shape, BF16),
            in_specs=[vmem, vmem, hbm, hbm],
            out_specs=vmem,
            scratch_shapes=[
                pltpu.VMEM((f_chunk, d_model, f_width), BF16),
                pltpu.VMEM((f_chunk, f_width, d_model), BF16),
                pltpu.VMEM((2, d_model, f_width), F32),
                pltpu.VMEM((2, f_width, d_model), F32),
                pltpu.VMEM((n_micro, rows, d_model), BF16),
                pltpu.VMEM((n_micro, half, d_model), BF16),
                pltpu.VMEM((n_micro, half, d_model), BF16),
                pltpu.VMEM((n_micro, rows, d_model), F32),
                pltpu.VMEM((n_micro, half, d_model), F32),
                dma((2, 2)), dma((n_micro,)), dma((n_micro,)), dma((2, n_micro)), dma((2, n_micro)), dma((n_micro,)), dma((n_micro,)),
                pltpu.SemaphoreType.REGULAR,
            ],
            compiler_params=pltpu.CompilerParams(collective_id=1, has_side_effects=True, vmem_limit_bytes=VMEM_MAX),
            name="forward_exchange",
        )(from_core, from_diag, nw1, nw2)
        return nw1, nw2, nm1, nm2, nv1, nv2, y_next

    return jax.shard_map(device_step, mesh=mesh, in_specs=in_specs, out_specs=out_specs, check_vma=False)
```

```python
import functools

import jax
import jax.numpy as jnp
from jax import lax
from jax.experimental import pallas as pl
from jax.experimental.pallas import tpu as pltpu
from jax.sharding import PartitionSpec as P

ADAM_STEP = 10
BETA_ONE = 0.9
BETA_TWO = 0.95
ADAM_EPS = 1e-8
WEIGHT_DECAY = 0.1
NORM_EPS = 1e-6
ONE_CORR = 1.0 - BETA_ONE ** ADAM_STEP
TWO_CORR = 1.0 - BETA_TWO ** ADAM_STEP
ROOT_EPS = ADAM_EPS * TWO_CORR ** 0.5
ROOT_GAIN = TWO_CORR ** 0.5 / ONE_CORR
TINY = 1.1754944e-38
HUGE = 3.4028235e38
GELU_A = 0.7978845608028654
GELU_B = 0.044715
NT = (((1,), (1,)), ((), ()))
TN = (((0,), (0,)), ((), ()))
MESH = pl.DeviceIdType.MESH
VMEM_MAX = 67_043_328
CHUNK = 128
SLOTS = 8
AHEAD = 5
SPARE = 1 << 20
F32 = jnp.float32
BF16 = jnp.bfloat16


def gelu_parts(z):
    t = jnp.tanh(GELU_A * (z + GELU_B * (z * z * z)))
    return t, z * (0.5 * (1.0 + t))


def gelu_slope(z, t):
    return 0.5 * (1.0 + t) + 0.5 * z * (1.0 - t * t) * (GELU_A * (1.0 + 3.0 * GELU_B * z * z))


def dot(a, b, dims=(((1,), (0,)), ((), ()))):
    return lax.dot_general(a, b, dims, preferred_element_type=F32)


def positions():
    return lax.axis_index("model"), lax.axis_index("data"), lax.axis_index("stage")


def entry_barrier(peers):
    barrier = pltpu.get_barrier_semaphore()
    for peer in peers:
        pl.semaphore_signal(barrier, inc=1, device_id=peer, device_id_type=MESH)
    pl.semaphore_wait(barrier, len(peers))


def remote(src, dst, send, recv, peer):
    return pltpu.make_async_remote_copy(src_ref=src, dst_ref=dst, send_sem=send, recv_sem=recv, device_id=peer, device_id_type=MESH)


def adamw(scale, rate, w, mom, sec, mean):
    grad = scale * mean
    mom_new = BETA_ONE * mom + (1.0 - BETA_ONE) * grad
    sec_new = BETA_TWO * sec + ((1.0 - BETA_TWO) * grad) * grad
    root = sec_new * lax.rsqrt(jnp.minimum(sec_new + TINY, HUGE))
    w_new = w * (1.0 - rate * WEIGHT_DECAY) - (rate * ROOT_GAIN) * (mom_new / (root + ROOT_EPS))
    return w_new, mom_new, sec_new


def grad_kernel(n_chunk, width, w1, w2, g1, g2, m1, v1, m2, v2, acts, dy, x, max_norm, rate,
                gr1, gr2, clip, act_half,
                gs1, gs2, w1b, w2b, gvec, part, got, x_buf, sq1, sq2, sq_out, sq_in,
                w_sem, g_sem, send1, send2, recv1, recv2, part_sem, gvec_sem, sq_send, sq_recv,
                row_sem, f_sem, rs_send, rs_recv):
    m, d, s = positions()
    peer_x = (m, 1 - d, s)
    peer_y = (1 - m, d, s)
    peer_c = (m, d, 1 - s)
    peer_d = (1 - m, d, 1 - s)
    d_model = w1.shape[0]
    is_last = s == 1
    is_first = s == 0

    def loads(j):
        slot = lax.rem(j, 2)
        cols = pl.ds(pl.multiple_of(j * width, width), width)
        return (pltpu.make_async_copy(w1.at[:, cols], w1b.at[slot], w_sem.at[0, slot]),
                pltpu.make_async_copy(w2.at[cols, :], w2b.at[slot], w_sem.at[1, slot]),
                pltpu.make_async_copy(g2.at[cols, :], gs2.at[j], g_sem.at[0, slot]),
                pltpu.make_async_copy(g1.at[:, cols], gs1.at[j], g_sem.at[1, slot]))

    load_dy = pltpu.make_async_copy(dy, gvec, row_sem)
    load_x = pltpu.make_async_copy(x, x_buf, row_sem)

    @pl.when(is_last)
    def _():
        load_dy.start()

    for first in (0, 1):
        for copy in loads(first):
            copy.start()

    @pl.when(is_first)
    def _():
        load_x.start()

    entry_barrier((peer_x, peer_y, peer_c, peer_d))

    hand_over = remote(x_buf.at[0], gvec, gvec_sem.at[0], gvec_sem.at[1], peer_c)
    swap_part = remote(part, got.at[:2], part_sem.at[0], part_sem.at[1], peer_y)

    @pl.when(is_last)
    def _():
        part[...] = jnp.zeros_like(part)
        load_dy.wait()

    @pl.when(is_first)
    def _():
        load_x.wait()
        hand_over.wait_recv()

    def send_two(j):
        return remote(gs2.at[j], gr2.at[j], send2.at[j], recv2.at[j], peer_x)

    def send_one(j):
        return remote(gs1.at[j], gr1.at[j], send1.at[j], recv1.at[j], peer_x)

    @pl.loop(0, n_chunk)
    def _(j):
        slot = lax.rem(j, 2)
        copies = loads(j)
        copies[0].wait()
        up = w1b[slot].astype(BF16)
        rows = acts[...]
        grad = gvec[...]
        z = dot(rows, up)
        t, act = gelu_parts(z)
        hid = act.astype(BF16)
        copies[2].wait()
        gs2[j] += dot(hid, grad, TN)
        send_two(j).start()
        copies[1].wait()
        grad_hid = dot(grad, w2b[slot].astype(BF16), NT)
        grad_pre = (gelu_slope(z, t) * grad_hid).astype(BF16)
        copies[3].wait()
        gs1[j] += dot(rows, grad_pre, TN)
        send_one(j).start()

        @pl.when(is_last)
        def _():
            part[...] += dot(grad_pre, up, NT).reshape(part.shape)

        @pl.when(j + 2 < n_chunk)
        def _():
            for copy in loads(j + 2):
                copy.start()

    @pl.when(is_last)
    def _():
        swap_part.start()
        swap_part.wait()
        total = (part[...] + got[:2]).reshape(gvec.shape)
        x_buf[0] = (gvec[...].astype(F32) + total).astype(BF16)
        hand_over.start()

    n_up = n_chunk // 2
    n_pair = 2 * n_up

    def fetch(p):
        base = lax.rem(p, 3) * 6

        @pl.when(p < n_up)
        def _():
            for q, ref in enumerate((w1, m1, v1)):
                for h in (0, 1):
                    cols = pl.ds(pl.multiple_of((2 * p + h) * width, width), width)
                    pltpu.make_async_copy(ref.at[:, cols], gs1.at[base + 2 * q + h], f_sem.at[base + 2 * q + h]).start()

        @pl.when(p >= n_up)
        def _():
            rows = pl.ds(pl.multiple_of(lax.rem(p - n_up, 2) * d_model, d_model), d_model)
            for q, ref in enumerate((w2, m2, v2)):
                for h in (0, 1):
                    cols = pl.ds(pl.multiple_of((2 * ((p - n_up) // 2) + h) * width, width), width)
                    pltpu.make_async_copy(ref.at[rows, cols], gs1.at[base + 2 * q + h], f_sem.at[base + 2 * q + h]).start()

    def free_and_fetch(lo, hi, p):
        for i in range(lo, hi):
            send_one(i).wait_send()

        @pl.when(is_first)
        def _():
            fetch(jnp.int32(p))

    sq1[...] = jnp.zeros_like(sq1)
    sq2[...] = jnp.zeros_like(sq2)

    @pl.loop(0, n_chunk)
    def _(j):
        send_two(j).wait_recv()
        mean = (gs2[j] + gr2[j]) * 0.5
        gr2[j] = mean
        sq2[...] += jnp.sum((mean * mean).reshape(-1, 8, mean.shape[1]), axis=0)
        send_one(j).wait_recv()
        mean = (gs1[j] + gr1[j]) * 0.5
        gr1[j] = mean
        sq1[...] += jnp.sum((mean * mean).reshape(-1, 8, mean.shape[1]), axis=0)

        @pl.when(j == 10)
        def _():
            free_and_fetch(0, 6, 0)

        @pl.when(j == 15)
        def _():
            free_and_fetch(6, 12, 1)

    sq_out[...] = jnp.full(sq_out.shape, jnp.sum(sq1[...]) + jnp.sum(sq2[...]), F32)
    mine = 2 * m + s
    others = ((peer_y, 2 * (1 - m) + s), (peer_c, 2 * m + 1 - s), (peer_d, 2 * (1 - m) + 1 - s))
    shares = [remote(sq_out, sq_in.at[mine], sq_send.at[k], sq_recv.at[mine], peer) for k, (peer, _) in enumerate(others)]
    for copy in shares:
        copy.start()
    free_and_fetch(12, n_chunk, 2)
    sq_in[mine] = sq_out[...]
    for peer, index in others:
        remote(sq_out, sq_in.at[index], sq_send.at[0], sq_recv.at[index], peer).wait_recv()
    total = (sq_in[0] + sq_in[1]) + (sq_in[2] + sq_in[3])
    clip[...] = jnp.minimum(1.0, max_norm[0] / (jnp.sqrt(total) + NORM_EPS))

    for j in range(n_chunk):
        send_two(j).wait_send()
    for copy in shares:
        copy.wait_send()

    @pl.when(is_last)
    def _():
        hand_over.wait_send()

    @pl.when(is_first)
    def _():
        scale = clip[0, 0]
        step_rate = rate[0]
        n_micro, n_row = x_buf.shape[:2]
        group = 2 * n_micro
        half = n_row // 2
        wide = 2 * width
        n_block = d_model // wide

        def new_weights(base, means):
            parts = [adamw(scale, step_rate, gs1[base + h], gs1[base + 2 + h], gs1[base + 4 + h], means[h])[0].astype(BF16) for h in (0, 1)]
            return jnp.concatenate(parts, axis=1)

        def block_copy(c):
            cols = pl.ds(pl.multiple_of(c * wide, wide), wide)
            return remote(gs2.at[2 * group + n_micro:2 * group + 2 * n_micro, :, cols], got.at[:, :, cols], rs_send.at[c], rs_recv.at[c], peer_y)

        @pl.loop(0, n_pair)
        def _(p):
            base = lax.rem(p, 3) * 6
            for i in range(6):
                pltpu.make_async_copy(w1.at[:, :width], gs1.at[base + i], f_sem.at[base + i]).wait()

            @pl.when(p < n_up)
            def _():
                new = new_weights(base, [gr1[2 * p], gr1[2 * p + 1]])
                act = gelu_parts(dot(x_buf[...].reshape(-1, d_model), new))[1].astype(BF16).astype(F32)
                cols = pl.ds(pl.multiple_of(lax.rem(p, n_block) * wide, wide), wide)
                gs2[pl.ds((p // n_block) * group, group), :, cols] = act.reshape(group, half, wide)

            @pl.when(p >= n_up)
            def _():
                c = (p - n_up) // 2
                upper = lax.rem(p - n_up, 2)
                means = []
                for h in (0, 1):
                    cols = pl.ds(pl.multiple_of((2 * c + h) * width, width), width)
                    means.append(gr2[pl.ds(upper * n_up, n_up), :, cols].reshape(d_model, width))
                new = new_weights(base, means)
                cols = pl.ds(pl.multiple_of(c * wide, wide), wide)
                spot = [(g // n_block, slice(None), slice(g % n_block * wide, g % n_block * wide + wide)) for g in range(group)]
                for lo in range(0, group, n_micro):
                    rows = gs2[pl.ds(upper * group + lo, n_micro)].reshape(-1, d_model).astype(BF16)
                    res = dot(rows, new).reshape(n_micro, half, wide)

                    @pl.when(upper == 0)
                    def _():
                        for g in range(n_micro):
                            part[spot[lo + g]] = res[g]

                    @pl.when(upper == 1)
                    def _():
                        for g in range(n_micro):
                            part[spot[lo + g]] += res[g]

                @pl.when(upper == 1)
                def _():
                    for k in range(n_micro):
                        even, odd = part[spot[2 * k]], part[spot[2 * k + 1]]
                        gs2[2 * group + k, :, cols] = jnp.where(m == 0, even, odd)
                        gs2[2 * group + n_micro + k, :, cols] = jnp.where(m == 0, odd, even)
                    block_copy(c).start()

            @pl.when(p + 3 < n_pair)
            def _():
                fetch(p + 3)

        for c in range(n_block):
            block_copy(c).wait_recv()
            cols = slice(c * wide, (c + 1) * wide)
            for k in range(n_micro):
                rows = x_buf[k, pl.ds(pl.multiple_of(m * half, half), half), cols].astype(F32)
                act_half[k, :, cols] = (rows + (gs2[2 * group + k, :, cols] + got[k, :, cols])).astype(BF16)
        for c in range(n_block):
            block_copy(c).wait_send()


def update_kernel(clip, rate, w1, m1, v1, gb1, w2, m2, v2, gb2, nw1, nm1, nv1, nw2, nm2, nv2, keep1, keep2, ring, in_sem, out_sem):
    n_up, deep, wide = gb1.shape
    n_slot = ring.shape[1]
    last = 2 * n_up
    block = deep // gb2.shape[1]
    scale = clip[0, 0]
    step_rate = rate[0]

    def place(i):
        col = pl.multiple_of(((i - n_up) // 2) * wide, wide)
        row = pl.multiple_of(lax.rem(i - n_up, 2) * deep, deep)
        return pl.ds(row, deep), pl.ds(col, wide)

    def start(i, fetch):
        slot = lax.rem(i, n_slot)
        sem = in_sem if fetch else out_sem

        def go(k, far):
            near = ring.at[k, slot]
            pair = (far, near) if fetch else (near, far)
            pltpu.make_async_copy(*pair, sem.at[k, slot]).start()

        @pl.when(i < n_up)
        def _():
            cols = pl.ds(pl.multiple_of(i * wide, wide), wide)
            for k, ref in enumerate((w1, m1, v1) if fetch else (nw1, nm1, nv1)):
                go(k, ref.at[0, :, cols])

        @pl.when(i >= n_up)
        def _():
            rows, cols = place(i)
            for k, ref in enumerate((w2, m2, v2) if fetch else (nw2, nm2, nv2)):
                go(k, ref.at[0, rows, cols])

    def finish(i, fetch):
        slot = lax.rem(i, n_slot)
        for k, ref in enumerate((w2, m2, v2) if fetch else (nw2, nm2, nv2)):
            far, near = ref.at[0, :deep, :wide], ring.at[k, slot]
            sem = (in_sem if fetch else out_sem).at[k, slot]
            (pltpu.make_async_copy(far, near, sem) if fetch else pltpu.make_async_copy(near, far, sem)).wait()

    for i in range(AHEAD):
        start(jnp.int32(i), True)

    def step(slot, mean):
        new, mom, sec = adamw(scale, step_rate, ring[0, slot], ring[1, slot], ring[2, slot], mean)
        ring[0, slot] = new
        ring[1, slot] = mom
        ring[2, slot] = sec
        return new

    @pl.loop(0, last)
    def _(i):
        slot = lax.rem(i, n_slot)
        finish(i, True)

        @pl.when(i < n_up)
        def _():
            keep1[i] = step(slot, gb1[i])

        @pl.when(i >= n_up)
        def _():
            cols = place(i)[1]
            rows = pl.ds(lax.rem(i - n_up, 2) * block, block)
            new = step(slot, gb2[rows, :, cols].reshape(deep, wide))
            keep2[rows, :, cols] = new.reshape(block, -1, wide)

        start(i, False)

        @pl.when(i + AHEAD < last)
        def _():
            @pl.when(i + AHEAD - n_slot >= 0)
            def _():
                finish(i + AHEAD - n_slot, False)
            start(i + AHEAD, True)

    for i in range(last - n_slot, last):
        finish(jnp.int32(i), False)


def forward_kernel(from_core, from_diag, new1, new2, y,
                   w1, w2, act, own_half, peer_half, part, part_in,
                   p_send, p_recv, y_send, y_recv, f_send, f_recv, ready):
    m, d, s = positions()
    n_micro, half = own_half.shape[:2]
    peer_y = (1 - m, d, s)
    peer_c = (m, d, 1 - s)

    n_chunk = w1.shape[0]
    barrier = pltpu.get_barrier_semaphore()

    @pl.when(s == 1)
    def _():
        pl.semaphore_signal(barrier, inc=1, device_id=peer_y, device_id_type=MESH)
        pl.semaphore_signal(barrier, inc=1, device_id=peer_c, device_id_type=MESH)

    pl.semaphore_wait(barrier, 1)

    @pl.when(s == 0)
    def _():
        pl.semaphore_signal(ready, inc=1, device_id=peer_c, device_id_type=MESH)

    mine = pl.ds(pl.multiple_of(m * half, half), half)
    theirs = pl.ds(pl.multiple_of((1 - m) * half, half), half)

    def send_part(k):
        return remote(part.at[k, theirs, :], part_in.at[k], p_send.at[k], p_recv.at[k], peer_y)

    def swap_y(k):
        return remote(own_half.at[k], peer_half.at[k], y_send.at[0, k], y_recv.at[0, k], peer_y)

    def give_own(k):
        return remote(own_half.at[k], y.at[k, mine, :], y_send.at[1, k], y_recv.at[1, k], peer_c)

    def pass_on(k):
        return remote(peer_half.at[k], y.at[k, theirs, :], f_send.at[k], f_recv.at[k], peer_c)

    @pl.when(s == 0)
    def _():
        for k in range(n_micro):
            give_own(k).wait_recv()
            pass_on(k).wait_recv()

    @pl.when(s == 1)
    def _():
        act[:, mine, :] = from_core[...]
        act[:, theirs, :] = from_diag[...]

        def chunk(k, j):
            hid = gelu_parts(dot(act[k], w1[j]))[1].astype(BF16)
            part[k] += dot(hid, w2[j])

        def finish(k):
            send_part(k).wait_recv()
            out = act[k, mine, :].astype(F32) + (part[k, mine, :] + part_in[k])
            own_half[k] = out.astype(BF16)
            swap_y(k).start()
            y[k, mine, :] = own_half[k]

        for k in range(n_micro):
            part[k] = jnp.zeros_like(part[k])

            @pl.loop(0, n_chunk)
            def _(j):
                if k == 0:
                    w1[j] = jnp.concatenate([new1[2 * j].astype(BF16), new1[2 * j + 1].astype(BF16)], axis=1)
                    w2[j] = new2[pl.ds(2 * j, 2)].reshape(w2.shape[1:]).astype(BF16)
                chunk(k, j)

            send_part(k).start()
            if k > 0:
                finish(k - 1)
        finish(n_micro - 1)
        pl.semaphore_wait(ready, 1)
        for k in range(n_micro):
            give_own(k).start()
        for k in range(n_micro):
            swap_y(k).wait_recv()
            pass_on(k).start()
            y[k, theirs, :] = peer_half[k]
        for k in range(n_micro):
            send_part(k).wait_send()
            swap_y(k).wait_send()
            give_own(k).wait_send()
            pass_on(k).wait_send()


def solution(mesh):
    up_spec = P('stage', None, 'model')
    down_spec = P('stage', 'model', None)
    row_spec = P(None, 'data', None)
    in_specs = (up_spec, down_spec, up_spec, down_spec, up_spec, down_spec, P('data', 'stage', None, 'model'), P('data', 'stage', 'model', None), P('stage', 'data', None), P('data', None), row_spec, P(None), P(None))
    out_specs = (up_spec, down_spec, up_spec, down_spec, up_spec, down_spec, row_spec)

    def device_step(w_up, w_down, m_up, m_down, v_up, v_down, g_up, g_down, acts_last, grad_out, x_next, learn_rate, max_norm):
        d_model, ff = w_up.shape[1:]
        rows = grad_out.shape[0]
        n_micro = x_next.shape[0]
        width = CHUNK
        n_chunk = ff // width
        half = rows // 2
        hbm = pl.BlockSpec(memory_space=pl.ANY)
        vmem = pl.BlockSpec(memory_space=pltpu.VMEM)
        smem = pl.BlockSpec(memory_space=pltpu.SMEM)
        dma = pltpu.SemaphoreType.DMA
        resident = 4 * 2 * d_model * ff
        n_block = d_model // (2 * width)

        mean_up, mean_down, clip, act_half = pl.pallas_call(
            functools.partial(grad_kernel, n_chunk, width),
            out_shape=(pltpu.VMEM((n_chunk, d_model, width), F32),
                       pltpu.VMEM((n_chunk, width, d_model), F32),
                       jax.ShapeDtypeStruct((8, 128), F32),
                       jax.ShapeDtypeStruct((n_micro, half, d_model), BF16)),
            in_specs=[hbm] * 8 + [vmem, hbm, hbm, smem, smem],
            out_specs=(vmem, vmem, vmem, vmem),
            scratch_shapes=[
                pltpu.VMEM((n_chunk, d_model, width), F32),
                pltpu.VMEM((n_chunk, width, d_model), F32),
                pltpu.VMEM((2, d_model, width), F32),
                pltpu.VMEM((2, width, d_model), F32),
                pltpu.VMEM((rows, d_model), BF16),
                pltpu.VMEM((2, half, d_model), F32),
                pltpu.VMEM((n_micro, half, d_model), F32),
                pltpu.VMEM((n_micro, rows, d_model), BF16),
                pltpu.VMEM((8, width), F32),
                pltpu.VMEM((8, d_model), F32),
                pltpu.VMEM((8, 128), F32),
                pltpu.VMEM((4, 8, 128), F32),
                dma((2, 2)), dma((2, 2)),
                dma((n_chunk,)), dma((n_chunk,)), dma((n_chunk,)), dma((n_chunk,)),
                dma((2,)), dma((2,)), dma((3,)), dma((4,)),
                dma(()), dma((18,)), dma((n_block,)), dma((n_block,)),
            ],
            compiler_params=pltpu.CompilerParams(collective_id=0, has_side_effects=True, vmem_limit_bytes=VMEM_MAX - resident - SPARE),
            name="grad_exchange",
        )(w_up[0], w_down[0], g_up[0, 0], g_down[0, 0], m_up[0], v_up[0], m_down[0], v_down[0], acts_last[0], grad_out, x_next, max_norm, learn_rate)

        from_diag = lax.ppermute(act_half, ('model', 'stage'), [(0, 3), (2, 1)])
        from_core = lax.ppermute(act_half, ('model', 'stage'), [(0, 1), (2, 3)])

        def stay(array):
            return pltpu.with_memory_space_constraint(array, pltpu.VMEM)

        up_out = jax.ShapeDtypeStruct(w_up.shape, F32)
        down_out = jax.ShapeDtypeStruct(w_down.shape, F32)
        nw1, nm1, nv1, nw2, nm2, nv2, new1, new2 = pl.pallas_call(
            update_kernel,
            out_shape=(up_out, up_out, up_out, down_out, down_out, down_out,
                       pltpu.VMEM(mean_up.shape, F32), pltpu.VMEM(mean_down.shape, F32)),
            in_specs=[smem, smem, hbm, hbm, hbm, vmem, hbm, hbm, hbm, vmem],
            out_specs=(hbm,) * 6 + (vmem, vmem),
            input_output_aliases={5: 6, 9: 7},
            scratch_shapes=[pltpu.VMEM((3, SLOTS, d_model, width), F32), dma((3, SLOTS)), dma((3, SLOTS))],
            compiler_params=pltpu.CompilerParams(vmem_limit_bytes=VMEM_MAX - resident - SPARE),
            cost_estimate=pl.CostEstimate(flops=2000 * d_model * ff, bytes_accessed=48 * d_model * ff, transcendentals=4 * d_model * ff),
            name="update",
        )(clip, learn_rate, w_up, m_up, v_up, stay(mean_up), w_down, m_down, v_down, stay(mean_down))

        f_width = 2 * width
        f_chunk = ff // f_width
        y_next = pl.pallas_call(
            forward_kernel,
            out_shape=jax.ShapeDtypeStruct(x_next.shape, BF16),
            in_specs=[vmem, vmem, vmem, vmem],
            out_specs=vmem,
            scratch_shapes=[
                pltpu.VMEM((f_chunk, d_model, f_width), BF16),
                pltpu.VMEM((f_chunk, f_width, d_model), BF16),
                pltpu.VMEM((n_micro, rows, d_model), BF16),
                pltpu.VMEM((n_micro, half, d_model), BF16),
                pltpu.VMEM((n_micro, half, d_model), BF16),
                pltpu.VMEM((n_micro, rows, d_model), F32),
                pltpu.VMEM((n_micro, half, d_model), F32),
                dma((n_micro,)), dma((n_micro,)), dma((2, n_micro)), dma((2, n_micro)), dma((n_micro,)), dma((n_micro,)),
                pltpu.SemaphoreType.REGULAR,
            ],
            compiler_params=pltpu.CompilerParams(collective_id=1, has_side_effects=True, vmem_limit_bytes=VMEM_MAX - resident - SPARE),
            name="forward_exchange",
        )(from_core, from_diag, stay(new1), stay(new2))
        return nw1, nw2, nm1, nm2, nv1, nv2, y_next

    return jax.shard_map(device_step, mesh=mesh, in_specs=in_specs, out_specs=out_specs, check_vma=False)
```

```python
import functools

import jax
import jax.numpy as jnp
from jax import lax
from jax.experimental import pallas as pl
from jax.experimental.pallas import tpu as pltpu
from jax.sharding import PartitionSpec as P

ADAM_STEP = 10
BETA_ONE = 0.9
BETA_TWO = 0.95
ADAM_EPS = 1e-8
WEIGHT_DECAY = 0.1
NORM_EPS = 1e-6
ONE_CORR = 1.0 - BETA_ONE ** ADAM_STEP
TWO_CORR = 1.0 - BETA_TWO ** ADAM_STEP
ROOT_EPS = ADAM_EPS * TWO_CORR ** 0.5
ROOT_GAIN = TWO_CORR ** 0.5 / ONE_CORR
TINY = 1.1754944e-38
HUGE = 3.4028235e38
GELU_A = 0.7978845608028654
GELU_B = 0.044715
NT = (((1,), (1,)), ((), ()))
TN = (((0,), (0,)), ((), ()))
MESH = pl.DeviceIdType.MESH
VMEM_MAX = 67_043_328
CHUNK = 128
SLOTS = 8
AHEAD = 5
SPARE = 1 << 20
F32 = jnp.float32
BF16 = jnp.bfloat16


def gelu_parts(z):
    t = jnp.tanh(GELU_A * (z + GELU_B * (z * z * z)))
    return t, z * (0.5 * (1.0 + t))


def gelu_slope(z, t):
    return 0.5 * (1.0 + t) + 0.5 * z * (1.0 - t * t) * (GELU_A * (1.0 + 3.0 * GELU_B * z * z))


def dot(a, b, dims=(((1,), (0,)), ((), ()))):
    return lax.dot_general(a, b, dims, preferred_element_type=F32)


def positions():
    return lax.axis_index("model"), lax.axis_index("data"), lax.axis_index("stage")


def entry_barrier(peers):
    barrier = pltpu.get_barrier_semaphore()
    for peer in peers:
        pl.semaphore_signal(barrier, inc=1, device_id=peer, device_id_type=MESH)
    pl.semaphore_wait(barrier, len(peers))


def remote(src, dst, send, recv, peer):
    return pltpu.make_async_remote_copy(src_ref=src, dst_ref=dst, send_sem=send, recv_sem=recv, device_id=peer, device_id_type=MESH)


def adamw(scale, rate, w, mom, sec, mean):
    grad = scale * mean
    mom_new = BETA_ONE * mom + (1.0 - BETA_ONE) * grad
    sec_new = BETA_TWO * sec + ((1.0 - BETA_TWO) * grad) * grad
    root = sec_new * lax.rsqrt(jnp.minimum(sec_new + TINY, HUGE))
    w_new = w * (1.0 - rate * WEIGHT_DECAY) - (rate * ROOT_GAIN) * (mom_new / (root + ROOT_EPS))
    return w_new, mom_new, sec_new


def grad_kernel(n_chunk, width, w1, w2, g1, g2, m1, v1, m2, v2, acts, dy, x, max_norm, rate,
                gr1, gr2, clip, act_half,
                gs1, gs2, w1b, w2b, part, got, x_buf, even_buf, odd_buf, sq1, sq2, sq_out, sq_in,
                w_sem, g_sem, send1, send2, recv1, recv2, part_sem, gvec_sem, sq_send, sq_recv,
                row_sem, act_sem, f_sem, rs_send, rs_recv):
    m, d, s = positions()
    peer_x = (m, 1 - d, s)
    peer_y = (1 - m, d, s)
    peer_c = (m, d, 1 - s)
    peer_d = (1 - m, d, 1 - s)
    d_model = w1.shape[0]
    is_last = s == 1
    is_first = s == 0

    def loads(j):
        slot = lax.rem(j, 2)
        cols = pl.ds(pl.multiple_of(j * width, width), width)
        return (pltpu.make_async_copy(w1.at[:, cols], w1b.at[slot], w_sem.at[0, slot]),
                pltpu.make_async_copy(w2.at[cols, :], w2b.at[slot], w_sem.at[1, slot]),
                pltpu.make_async_copy(g2.at[cols, :], gs2.at[j], g_sem.at[0, slot]),
                pltpu.make_async_copy(g1.at[:, cols], gs1.at[j], g_sem.at[1, slot]))

    acts_buf, gvec = x_buf.at[2:4], x_buf.at[4:6]
    load_acts = pltpu.make_async_copy(acts, acts_buf, act_sem)
    load_dy = pltpu.make_async_copy(dy, gvec, row_sem)
    load_x = pltpu.make_async_copy(x, x_buf, row_sem)

    load_acts.start()

    @pl.when(is_last)
    def _():
        load_dy.start()

    for first in (0, 1):
        for copy in loads(first):
            copy.start()

    entry_barrier((peer_x, peer_y, peer_c, peer_d))

    hand_over = remote(x_buf.at[:2], gvec, gvec_sem.at[0], gvec_sem.at[1], peer_c)
    swap_part = remote(part, got.at[:2], part_sem.at[0], part_sem.at[1], peer_y)

    @pl.when(is_last)
    def _():
        part[...] = jnp.zeros_like(part)
        load_dy.wait()

    @pl.when(is_first)
    def _():
        hand_over.wait_recv()

    load_acts.wait()

    def send_two(j):
        return remote(gs2.at[j], gr2.at[j], send2.at[j], recv2.at[j], peer_x)

    def send_one(j):
        return remote(gs1.at[j], gr1.at[j], send1.at[j], recv1.at[j], peer_x)

    @pl.loop(0, n_chunk)
    def _(j):
        slot = lax.rem(j, 2)
        copies = loads(j)
        copies[0].wait()
        up = w1b[slot].astype(BF16)
        rows = acts_buf[...].reshape(-1, d_model)
        grad = gvec[...].reshape(-1, d_model)
        z = dot(rows, up)
        t, act = gelu_parts(z)
        hid = act.astype(BF16)
        copies[2].wait()
        gs2[j] += dot(hid, grad, TN)
        send_two(j).start()
        copies[1].wait()
        grad_hid = dot(grad, w2b[slot].astype(BF16), NT)
        grad_pre = (gelu_slope(z, t) * grad_hid).astype(BF16)
        copies[3].wait()
        gs1[j] += dot(rows, grad_pre, TN)
        send_one(j).start()

        @pl.when(is_last)
        def _():
            part[...] += dot(grad_pre, up, NT).reshape(part.shape)

        @pl.when(j + 2 < n_chunk)
        def _():
            for copy in loads(j + 2):
                copy.start()

    @pl.when(is_last)
    def _():
        swap_part.start()
        swap_part.wait()
        x_buf[:2] = (gvec[...].astype(F32) + (part[...] + got[:2])).astype(BF16)
        hand_over.start()

    @pl.when(is_first)
    def _():
        load_x.start()

    n_up = n_chunk // 2
    n_pair = 2 * n_up

    def fetch(p):
        base = lax.rem(p, 3) * 6

        @pl.when(p < n_up)
        def _():
            for q, ref in enumerate((w1, m1, v1)):
                for h in (0, 1):
                    cols = pl.ds(pl.multiple_of((2 * p + h) * width, width), width)
                    pltpu.make_async_copy(ref.at[:, cols], gs1.at[base + 2 * q + h], f_sem.at[base + 2 * q + h]).start()

        @pl.when(p >= n_up)
        def _():
            rows = pl.ds(pl.multiple_of(lax.rem(p - n_up, 2) * d_model, d_model), d_model)
            for q, ref in enumerate((w2, m2, v2)):
                for h in (0, 1):
                    cols = pl.ds(pl.multiple_of((2 * ((p - n_up) // 2) + h) * width, width), width)
                    pltpu.make_async_copy(ref.at[rows, cols], gs1.at[base + 2 * q + h], f_sem.at[base + 2 * q + h]).start()

    def free_and_fetch(lo, hi, p):
        for i in range(lo, hi):
            send_one(i).wait_send()

        @pl.when(is_first)
        def _():
            fetch(jnp.int32(p))

    sq1[...] = jnp.zeros_like(sq1)
    sq2[...] = jnp.zeros_like(sq2)

    @pl.loop(0, n_chunk)
    def _(j):
        send_two(j).wait_recv()
        mean = (gs2[j] + gr2[j]) * 0.5
        gr2[j] = mean
        sq2[...] += jnp.sum((mean * mean).reshape(-1, 8, mean.shape[1]), axis=0)
        send_one(j).wait_recv()
        mean = (gs1[j] + gr1[j]) * 0.5
        gr1[j] = mean
        sq1[...] += jnp.sum((mean * mean).reshape(-1, 8, mean.shape[1]), axis=0)

        @pl.when(j == 10)
        def _():
            free_and_fetch(0, 6, 0)

        @pl.when(j == 15)
        def _():
            free_and_fetch(6, 12, 1)

    sq_out[...] = jnp.full(sq_out.shape, jnp.sum(sq1[...]) + jnp.sum(sq2[...]), F32)
    mine = 2 * m + s
    others = ((peer_y, 2 * (1 - m) + s), (peer_c, 2 * m + 1 - s), (peer_d, 2 * (1 - m) + 1 - s))
    shares = [remote(sq_out, sq_in.at[mine], sq_send.at[k], sq_recv.at[mine], peer) for k, (peer, _) in enumerate(others)]
    for copy in shares:
        copy.start()
    free_and_fetch(12, n_chunk, 2)
    sq_in[mine] = sq_out[...]
    for peer, index in others:
        remote(sq_out, sq_in.at[index], sq_send.at[0], sq_recv.at[index], peer).wait_recv()
    total = (sq_in[0] + sq_in[1]) + (sq_in[2] + sq_in[3])
    clip[...] = jnp.minimum(1.0, max_norm[0] / (jnp.sqrt(total) + NORM_EPS))

    for j in range(n_chunk):
        send_two(j).wait_send()
    for copy in shares:
        copy.wait_send()

    @pl.when(is_last)
    def _():
        hand_over.wait_send()

    @pl.when(is_first)
    def _():
        scale = clip[0, 0]
        step_rate = rate[0]
        group, half = x_buf.shape[:2]
        n_micro = group // 2
        third = group // 2
        deep = d_model // 2
        wide = 2 * width
        n_block = d_model // wide

        def arrive(p):
            base = lax.rem(p, 3) * 6
            for i in range(6):
                pltpu.make_async_copy(w1.at[:, :width], gs1.at[base + i], f_sem.at[base + i]).wait()

        def new_weights(p, t, buf, means):
            base = lax.rem(p, 3) * 6
            some = pl.ds(pl.multiple_of(t * deep, deep), deep)
            for h in (0, 1):
                new = adamw(scale, step_rate, gs1[base + h, some], gs1[base + 2 + h, some], gs1[base + 4 + h, some], means[h])[0]
                buf[some, h * width:(h + 1) * width] = new.astype(BF16)

        def up_means(p, t):
            some = pl.ds(pl.multiple_of(t * deep, deep), deep)
            return [gr1[2 * p, some], gr1[2 * p + 1, some]]

        def down_means(p, t, upper):
            means = []
            for h in (0, 1):
                cols = pl.ds(pl.multiple_of((2 * ((p - n_up) // 2) + h) * width, width), width)
                means.append(gr2[pl.ds(upper * n_up + t * (n_up // 2), n_up // 2), :, cols].reshape(deep, width))
            return means

        def up_product(p, t, buf):
            rows = x_buf[pl.ds(t * third, third)].reshape(-1, d_model)
            act = gelu_parts(dot(rows, buf[...]))[1].astype(BF16).astype(F32)
            cols = pl.ds(pl.multiple_of(lax.rem(p, n_block) * wide, wide), wide)
            gs2[pl.ds((p // n_block) * group + t * third, third), :, cols] = act.reshape(third, half, wide)

        def down_product(p, t, buf, upper):
            rows = gs2[pl.ds(upper * group + t * third, third)].reshape(-1, d_model).astype(BF16)
            res = dot(rows, buf[...]).reshape(third, half, wide)
            for g in range(third):
                spot = slice(g * wide, (g + 1) * wide)
                if upper:
                    part[t, :, spot] += res[g]
                else:
                    part[t, :, spot] = res[g]

        def give_block(c):
            cols = pl.ds(pl.multiple_of(c * wide, wide), wide)
            for k in range(n_micro):
                even, odd = [part[g // third, :, g % third * wide:(g % third + 1) * wide] for g in (2 * k, 2 * k + 1)]
                gs2[2 * group + k, :, cols] = jnp.where(m == 0, even, odd)
                gs2[2 * group + n_micro + k, :, cols] = jnp.where(m == 0, odd, even)
            block_copy(c).start()

        def block_copy(c):
            cols = pl.ds(pl.multiple_of(c * wide, wide), wide)
            return remote(gs2.at[2 * group + n_micro:2 * group + 2 * n_micro, :, cols], got.at[:, :, cols], rs_send.at[c], rs_recv.at[c], peer_y)

        def ahead(p):
            if isinstance(p, int):
                if p < n_pair:
                    fetch(jnp.int32(p))
                return

            @pl.when(p < n_pair)
            def _():
                fetch(p)

        bufs = (even_buf, odd_buf)

        def up_step(p, odd, down):
            arrive(p + 1)

            @pl.loop(0, 2)
            def _(t):
                up_product(p, t, bufs[odd])
                new_weights(p + 1, t, bufs[1 - odd], down_means(p + 1, t, 0) if down else up_means(p + 1, t))

            ahead(p + 4)

        def down_step(p, odd):
            arrive(p + 1)

            @pl.loop(0, 2)
            def _(t):
                down_product(p, t, bufs[odd], odd)
                new_weights(p + 1, t, bufs[1 - odd], down_means(p + 1, t, 1 - odd))

            ahead(p + 4)
            if odd:
                give_block((p - n_up) // 2)

        load_x.wait()
        arrive(0)

        @pl.loop(0, 2)
        def _(t):
            new_weights(0, t, even_buf, up_means(0, t))

        ahead(3)

        @pl.loop(0, n_up // 2 - 1)
        def _(i):
            up_step(2 * i, 0, False)
            up_step(2 * i + 1, 1, False)

        up_step(n_up - 2, 0, False)
        up_step(n_up - 1, 1, True)

        @pl.loop(n_up // 2, n_pair // 2 - 1)
        def _(i):
            down_step(2 * i, 0)
            down_step(2 * i + 1, 1)

        down_step(n_pair - 2, 0)

        @pl.loop(0, 2)
        def _(t):
            down_product(n_pair - 1, t, odd_buf, 1)

        give_block(n_block - 1)

        for c in range(n_block):
            block_copy(c).wait_recv()
            cols = slice(c * wide, (c + 1) * wide)
            for k in range(n_micro):
                rows = x_buf[2 * k + m, :, cols].astype(F32)
                x_buf[k, :, cols] = (rows + (gs2[2 * group + k, :, cols] + got[k, :, cols])).astype(BF16)
        store = pltpu.make_async_copy(x_buf.at[:n_micro], act_half, row_sem)
        store.start()
        for c in range(n_block):
            block_copy(c).wait_send()
        store.wait()


def update_kernel(clip, rate, w1, m1, v1, gb1, w2, m2, v2, gb2, nw1, nm1, nv1, nw2, nm2, nv2, keep1, keep2, ring, in_sem, out_sem):
    n_up, deep, wide = gb1.shape
    n_slot = ring.shape[1]
    last = 2 * n_up
    block = deep // gb2.shape[1]
    scale = clip[0, 0]
    step_rate = rate[0]

    def place(i):
        col = pl.multiple_of(((i - n_up) // 2) * wide, wide)
        row = pl.multiple_of(lax.rem(i - n_up, 2) * deep, deep)
        return pl.ds(row, deep), pl.ds(col, wide)

    def start(i, fetch):
        slot = lax.rem(i, n_slot)
        sem = in_sem if fetch else out_sem

        def go(k, far):
            near = ring.at[k, slot]
            pair = (far, near) if fetch else (near, far)
            pltpu.make_async_copy(*pair, sem.at[k, slot]).start()

        @pl.when(i < n_up)
        def _():
            cols = pl.ds(pl.multiple_of(i * wide, wide), wide)
            for k, ref in enumerate((w1, m1, v1) if fetch else (nw1, nm1, nv1)):
                go(k, ref.at[0, :, cols])

        @pl.when(i >= n_up)
        def _():
            rows, cols = place(i)
            for k, ref in enumerate((w2, m2, v2) if fetch else (nw2, nm2, nv2)):
                go(k, ref.at[0, rows, cols])

    def finish(i, fetch):
        slot = lax.rem(i, n_slot)
        for k, ref in enumerate((w2, m2, v2) if fetch else (nw2, nm2, nv2)):
            far, near = ref.at[0, :deep, :wide], ring.at[k, slot]
            sem = (in_sem if fetch else out_sem).at[k, slot]
            (pltpu.make_async_copy(far, near, sem) if fetch else pltpu.make_async_copy(near, far, sem)).wait()

    for i in range(AHEAD):
        start(jnp.int32(i), True)

    def step(slot, mean):
        new, mom, sec = adamw(scale, step_rate, ring[0, slot], ring[1, slot], ring[2, slot], mean)
        ring[0, slot] = new
        ring[1, slot] = mom
        ring[2, slot] = sec
        return new

    @pl.loop(0, last)
    def _(i):
        slot = lax.rem(i, n_slot)
        finish(i, True)

        @pl.when(i < n_up)
        def _():
            keep1[i] = step(slot, gb1[i])

        @pl.when(i >= n_up)
        def _():
            cols = place(i)[1]
            rows = pl.ds(lax.rem(i - n_up, 2) * block, block)
            new = step(slot, gb2[rows, :, cols].reshape(deep, wide))
            keep2[rows, :, cols] = new.reshape(block, -1, wide)

        start(i, False)

        @pl.when(i + AHEAD < last)
        def _():
            @pl.when(i + AHEAD - n_slot >= 0)
            def _():
                finish(i + AHEAD - n_slot, False)
            start(i + AHEAD, True)

    for i in range(last - n_slot, last):
        finish(jnp.int32(i), False)


def forward_kernel(from_core, from_diag, new1, new2, y,
                   w1, w2, hid, act, own_half, peer_half, part, part_in,
                   p_send, p_recv, y_send, y_recv, g_send, g_recv, f_send, f_recv, ready):
    m, d, s = positions()
    n_micro, half, d_model = own_half.shape
    n_chunk, _, width = w1.shape
    n_block = d_model // width
    peer_y = (1 - m, d, s)
    peer_c = (m, d, 1 - s)
    barrier = pltpu.get_barrier_semaphore()

    @pl.when(s == 1)
    def _():
        pl.semaphore_signal(barrier, inc=1, device_id=peer_y, device_id_type=MESH)
        pl.semaphore_signal(barrier, inc=1, device_id=peer_c, device_id_type=MESH)

    pl.semaphore_wait(barrier, 1)

    @pl.when(s == 0)
    def _():
        pl.semaphore_signal(ready, inc=1, device_id=peer_c, device_id_type=MESH)

    mine = pl.ds(pl.multiple_of(m * half, half), half)
    theirs = pl.ds(pl.multiple_of((1 - m) * half, half), half)

    def span(c):
        return pl.ds(pl.multiple_of(c * width, width), width)

    def send_part(k, c):
        return remote(part.at[k, theirs, span(c)], part_in.at[k, :, span(c)], p_send.at[k, c], p_recv.at[k, c], peer_y)

    def swap_y(k, c):
        return remote(own_half.at[k, :, span(c)], peer_half.at[k, :, span(c)], y_send.at[k, c], y_recv.at[k, c], peer_y)

    def give_own(k):
        return remote(own_half.at[k], y.at[k, mine, :], g_send.at[k], g_recv.at[k], peer_c)

    def pass_on(k):
        return remote(peer_half.at[k], y.at[k, theirs, :], f_send.at[k], f_recv.at[k], peer_c)

    @pl.when(s == 0)
    def _():
        for k in range(n_micro):
            give_own(k).wait_recv()
            pass_on(k).wait_recv()

    @pl.when(s == 1)
    def _():
        act[:, mine, :] = from_core[...]
        act[:, theirs, :] = from_diag[...]

        for k in range(n_micro):
            @pl.loop(0, n_chunk)
            def _(j):
                if k == 0:
                    w1[j] = jnp.concatenate([new1[2 * j].astype(BF16), new1[2 * j + 1].astype(BF16)], axis=1)
                hid[:, span(j)] = gelu_parts(dot(act[k], w1[j]))[1].astype(BF16)

            @pl.loop(0, n_block)
            def _(c):
                if k == 0:
                    w2[:, span(c)] = new2[:, :, span(c)].reshape(-1, width).astype(BF16)
                part[k, :, span(c)] = dot(hid[...], w2[:, span(c)])
                send_part(k, c).start()

        for k in range(n_micro):
            @pl.loop(0, n_block)
            def _(c):
                send_part(k, c).wait_recv()
                out = act[k, mine, span(c)].astype(F32) + (part[k, mine, span(c)] + part_in[k, :, span(c)])
                own_half[k, :, span(c)] = out.astype(BF16)
                swap_y(k, c).start()

        pl.semaphore_wait(ready, 1)
        for k in range(n_micro):
            give_own(k).start()
            y[k, mine, :] = own_half[k]
        for k in range(n_micro):
            @pl.loop(0, n_block)
            def _(c):
                swap_y(k, c).wait_recv()

            pass_on(k).start()
            y[k, theirs, :] = peer_half[k]
        for k in range(n_micro):
            @pl.loop(0, n_block)
            def _(c):
                send_part(k, c).wait_send()
                swap_y(k, c).wait_send()

            give_own(k).wait_send()
            pass_on(k).wait_send()


def solution(mesh):
    up_spec = P('stage', None, 'model')
    down_spec = P('stage', 'model', None)
    row_spec = P(None, 'data', None)
    in_specs = (up_spec, down_spec, up_spec, down_spec, up_spec, down_spec, P('data', 'stage', None, 'model'), P('data', 'stage', 'model', None), P('stage', 'data', None), P('data', None), row_spec, P(None), P(None))
    out_specs = (up_spec, down_spec, up_spec, down_spec, up_spec, down_spec, row_spec)

    def device_step(w_up, w_down, m_up, m_down, v_up, v_down, g_up, g_down, acts_last, grad_out, x_next, learn_rate, max_norm):
        d_model, ff = w_up.shape[1:]
        rows = grad_out.shape[0]
        n_micro = x_next.shape[0]
        width = CHUNK
        n_chunk = ff // width
        half = rows // 2
        hbm = pl.BlockSpec(memory_space=pl.ANY)
        vmem = pl.BlockSpec(memory_space=pltpu.VMEM)
        smem = pl.BlockSpec(memory_space=pltpu.SMEM)
        dma = pltpu.SemaphoreType.DMA
        resident = 4 * 2 * d_model * ff
        n_block = d_model // (2 * width)

        mean_up, mean_down, clip, act_half = pl.pallas_call(
            functools.partial(grad_kernel, n_chunk, width),
            out_shape=(pltpu.VMEM((n_chunk, d_model, width), F32),
                       pltpu.VMEM((n_chunk, width, d_model), F32),
                       jax.ShapeDtypeStruct((8, 128), F32),
                       jax.ShapeDtypeStruct((n_micro, half, d_model), BF16)),
            in_specs=[hbm] * 11 + [smem, smem],
            out_specs=(vmem, vmem, vmem, hbm),
            scratch_shapes=[
                pltpu.VMEM((n_chunk, d_model, width), F32),
                pltpu.VMEM((n_chunk, width, d_model), F32),
                pltpu.VMEM((2, d_model, width), F32),
                pltpu.VMEM((2, width, d_model), F32),
                pltpu.VMEM((2, half, d_model), F32),
                pltpu.VMEM((n_micro, half, d_model), F32),
                pltpu.VMEM((2 * n_micro, half, d_model), BF16),
                pltpu.VMEM((d_model, 2 * width), BF16),
                pltpu.VMEM((d_model, 2 * width), BF16),
                pltpu.VMEM((8, width), F32),
                pltpu.VMEM((8, d_model), F32),
                pltpu.VMEM((8, 128), F32),
                pltpu.VMEM((4, 8, 128), F32),
                dma((2, 2)), dma((2, 2)),
                dma((n_chunk,)), dma((n_chunk,)), dma((n_chunk,)), dma((n_chunk,)),
                dma((2,)), dma((2,)), dma((3,)), dma((4,)),
                dma(()), dma(()), dma((18,)), dma((n_block,)), dma((n_block,)),
            ],
            compiler_params=pltpu.CompilerParams(collective_id=0, has_side_effects=True, vmem_limit_bytes=VMEM_MAX - resident - SPARE),
            name="grad_exchange",
        )(w_up[0], w_down[0], g_up[0, 0], g_down[0, 0], m_up[0], v_up[0], m_down[0], v_down[0], acts_last.reshape(2, half, d_model), grad_out.reshape(2, half, d_model), x_next.reshape(2 * n_micro, half, d_model), max_norm, learn_rate)

        from_diag = lax.ppermute(act_half, ('model', 'stage'), [(0, 3), (2, 1)])
        from_core = lax.ppermute(act_half, ('model', 'stage'), [(0, 1), (2, 3)])

        def stay(array):
            return pltpu.with_memory_space_constraint(array, pltpu.VMEM)

        up_out = jax.ShapeDtypeStruct(w_up.shape, F32)
        down_out = jax.ShapeDtypeStruct(w_down.shape, F32)
        nw1, nm1, nv1, nw2, nm2, nv2, new1, new2 = pl.pallas_call(
            update_kernel,
            out_shape=(up_out, up_out, up_out, down_out, down_out, down_out,
                       pltpu.VMEM(mean_up.shape, F32), pltpu.VMEM(mean_down.shape, F32)),
            in_specs=[smem, smem, hbm, hbm, hbm, vmem, hbm, hbm, hbm, vmem],
            out_specs=(hbm,) * 6 + (vmem, vmem),
            input_output_aliases={5: 6, 9: 7},
            scratch_shapes=[pltpu.VMEM((3, SLOTS, d_model, width), F32), dma((3, SLOTS)), dma((3, SLOTS))],
            compiler_params=pltpu.CompilerParams(vmem_limit_bytes=VMEM_MAX - resident - SPARE),
            cost_estimate=pl.CostEstimate(flops=2000 * d_model * ff, bytes_accessed=48 * d_model * ff, transcendentals=4 * d_model * ff),
            name="update",
        )(clip, learn_rate, w_up, m_up, v_up, stay(mean_up), w_down, m_down, v_down, stay(mean_down))

        f_width = 2 * width
        f_chunk = ff // f_width
        y_next = pl.pallas_call(
            forward_kernel,
            out_shape=jax.ShapeDtypeStruct(x_next.shape, BF16),
            in_specs=[vmem, vmem, vmem, vmem],
            out_specs=vmem,
            scratch_shapes=[
                pltpu.VMEM((f_chunk, d_model, f_width), BF16),
                pltpu.VMEM((ff, d_model), BF16),
                pltpu.VMEM((rows, ff), BF16),
                pltpu.VMEM((n_micro, rows, d_model), BF16),
                pltpu.VMEM((n_micro, half, d_model), BF16),
                pltpu.VMEM((n_micro, half, d_model), BF16),
                pltpu.VMEM((n_micro, rows, d_model), F32),
                pltpu.VMEM((n_micro, half, d_model), F32),
                dma((n_micro, n_block)), dma((n_micro, n_block)), dma((n_micro, n_block)), dma((n_micro, n_block)),
                dma((n_micro,)), dma((n_micro,)), dma((n_micro,)), dma((n_micro,)),
                pltpu.SemaphoreType.REGULAR,
            ],
            compiler_params=pltpu.CompilerParams(collective_id=1, has_side_effects=True, vmem_limit_bytes=VMEM_MAX - resident - SPARE),
            name="forward_exchange",
        )(from_core, from_diag, stay(new1), stay(new2))
        return nw1, nw2, nm1, nm2, nv1, nv2, y_next

    return jax.shard_map(device_step, mesh=mesh, in_specs=in_specs, out_specs=out_specs, check_vma=False)
```

```python
import functools

import jax
import jax.numpy as jnp
from jax import lax
from jax.experimental import pallas as pl
from jax.experimental.pallas import tpu as pltpu
from jax.sharding import PartitionSpec as P

ADAM_STEP = 10
BETA_ONE = 0.9
BETA_TWO = 0.95
ADAM_EPS = 1e-8
WEIGHT_DECAY = 0.1
NORM_EPS = 1e-6
ONE_CORR = 1.0 - BETA_ONE ** ADAM_STEP
TWO_CORR = 1.0 - BETA_TWO ** ADAM_STEP
ROOT_EPS = ADAM_EPS * TWO_CORR ** 0.5
ROOT_GAIN = TWO_CORR ** 0.5 / ONE_CORR
TINY = 1.1754944e-38
HUGE = 3.4028235e38
GELU_A = 0.7978845608028654
GELU_B = 0.044715
NT = (((1,), (1,)), ((), ()))
TN = (((0,), (0,)), ((), ()))
MESH = pl.DeviceIdType.MESH
VMEM_MAX = 67_043_328
CHUNK = 128
SLOTS = 8
AHEAD = 5
SPARE = 5 << 19
F32 = jnp.float32
BF16 = jnp.bfloat16


def gelu_parts(z):
    t = jnp.tanh(GELU_A * (z + GELU_B * (z * z * z)))
    return t, z * (0.5 * (1.0 + t))


def gelu_slope(z, t):
    return 0.5 * (1.0 + t) + 0.5 * z * (1.0 - t * t) * (GELU_A * (1.0 + 3.0 * GELU_B * z * z))


def dot(a, b, dims=(((1,), (0,)), ((), ()))):
    return lax.dot_general(a, b, dims, preferred_element_type=F32)


def positions():
    return lax.axis_index("model"), lax.axis_index("data"), lax.axis_index("stage")


def entry_barrier(peers):
    barrier = pltpu.get_barrier_semaphore()
    for peer in peers:
        pl.semaphore_signal(barrier, inc=1, device_id=peer, device_id_type=MESH)
    pl.semaphore_wait(barrier, len(peers))


def remote(src, dst, send, recv, peer):
    return pltpu.make_async_remote_copy(src_ref=src, dst_ref=dst, send_sem=send, recv_sem=recv, device_id=peer, device_id_type=MESH)


def adamw(scale, rate, w, mom, sec, mean):
    grad = scale * mean
    mom_new = BETA_ONE * mom + (1.0 - BETA_ONE) * grad
    sec_new = BETA_TWO * sec + ((1.0 - BETA_TWO) * grad) * grad
    root = sec_new * lax.rsqrt(jnp.minimum(sec_new + TINY, HUGE))
    w_new = w * (1.0 - rate * WEIGHT_DECAY) - (rate * ROOT_GAIN) * (mom_new / (root + ROOT_EPS))
    return w_new, mom_new, sec_new


def grad_kernel(n_chunk, width, w1, w2, g1, g2, m1, v1, m2, v2, acts, dy, x, max_norm, rate,
                gr1, gr2, clip, act_half,
                gs1, gs2, w1b, w2b, part, got, x_buf, sq1, sq2, sq_out, sq_in,
                w_sem, g_sem, send1, send2, recv1, recv2, part_sem, gvec_sem, sq_send, sq_recv,
                row_sem, act_sem, f_sem, rs_send, rs_recv):
    m, d, s = positions()
    peer_x = (m, 1 - d, s)
    peer_y = (1 - m, d, s)
    peer_c = (m, d, 1 - s)
    peer_d = (1 - m, d, 1 - s)
    d_model = w1.shape[0]
    is_last = s == 1
    is_first = s == 0

    def loads(j):
        slot = lax.rem(j, 2)
        cols = pl.ds(pl.multiple_of(j * width, width), width)
        return (pltpu.make_async_copy(w1.at[:, cols], w1b.at[slot], w_sem.at[0, slot]),
                pltpu.make_async_copy(w2.at[cols, :], w2b.at[slot], w_sem.at[1, slot]),
                pltpu.make_async_copy(g2.at[cols, :], gs2.at[j], g_sem.at[0, slot]),
                pltpu.make_async_copy(g1.at[:, cols], gs1.at[j], g_sem.at[1, slot]))

    acts_buf, gvec = x_buf.at[2:4], x_buf.at[4:6]
    load_acts = pltpu.make_async_copy(acts, acts_buf, act_sem)
    load_dy = pltpu.make_async_copy(dy, gvec, row_sem)
    load_x = pltpu.make_async_copy(x, x_buf, row_sem)

    load_acts.start()

    @pl.when(is_last)
    def _():
        load_dy.start()

    for first in (0, 1):
        for copy in loads(first):
            copy.start()

    entry_barrier((peer_x, peer_y, peer_c, peer_d))

    hand_over = remote(x_buf.at[:2], gvec, gvec_sem.at[0], gvec_sem.at[1], peer_c)
    swap_part = remote(part, got.at[:2], part_sem.at[0], part_sem.at[1], peer_y)

    @pl.when(is_last)
    def _():
        part[...] = jnp.zeros_like(part)
        load_dy.wait()

    @pl.when(is_first)
    def _():
        hand_over.wait_recv()

    load_acts.wait()

    def send_two(j):
        return remote(gs2.at[j], gr2.at[j], send2.at[j], recv2.at[j], peer_x)

    def send_one(j):
        return remote(gs1.at[j], gr1.at[j], send1.at[j], recv1.at[j], peer_x)

    @pl.loop(0, n_chunk)
    def _(j):
        slot = lax.rem(j, 2)
        copies = loads(j)
        copies[0].wait()
        up = w1b[slot].astype(BF16)
        rows = acts_buf[...].reshape(-1, d_model)
        grad = gvec[...].reshape(-1, d_model)
        z = dot(rows, up)
        t, act = gelu_parts(z)
        hid = act.astype(BF16)
        copies[2].wait()
        gs2[j] += dot(hid, grad, TN)
        send_two(j).start()
        copies[1].wait()
        grad_hid = dot(grad, w2b[slot].astype(BF16), NT)
        grad_pre = (gelu_slope(z, t) * grad_hid).astype(BF16)
        copies[3].wait()
        gs1[j] += dot(rows, grad_pre, TN)
        send_one(j).start()

        @pl.when(is_last)
        def _():
            part[...] += dot(grad_pre, up, NT).reshape(part.shape)

        @pl.when(j + 2 < n_chunk)
        def _():
            for copy in loads(j + 2):
                copy.start()

    @pl.when(is_last)
    def _():
        swap_part.start()
        swap_part.wait()
        x_buf[:2] = (gvec[...].astype(F32) + (part[...] + got[:2])).astype(BF16)
        hand_over.start()

    @pl.when(is_first)
    def _():
        load_x.start()

    n_up = n_chunk // 2
    n_pair = 2 * n_up

    def fetch(p):
        base = lax.rem(p, 3) * 6

        @pl.when(p < n_up)
        def _():
            for q, ref in enumerate((w1, m1, v1)):
                for h in (0, 1):
                    cols = pl.ds(pl.multiple_of((2 * p + h) * width, width), width)
                    pltpu.make_async_copy(ref.at[:, cols], gs1.at[base + 2 * q + h], f_sem.at[base + 2 * q + h]).start()

        @pl.when(p >= n_up)
        def _():
            rows = pl.ds(pl.multiple_of(lax.rem(p - n_up, 2) * d_model, d_model), d_model)
            for q, ref in enumerate((w2, m2, v2)):
                for h in (0, 1):
                    cols = pl.ds(pl.multiple_of((2 * ((p - n_up) // 2) + h) * width, width), width)
                    pltpu.make_async_copy(ref.at[rows, cols], gs1.at[base + 2 * q + h], f_sem.at[base + 2 * q + h]).start()

    def free_and_fetch(lo, hi, p):
        for i in range(lo, hi):
            send_one(i).wait_send()

        @pl.when(is_first)
        def _():
            fetch(jnp.int32(p))

    sq1[...] = jnp.zeros_like(sq1)
    sq2[...] = jnp.zeros_like(sq2)

    @pl.loop(0, n_chunk)
    def _(j):
        send_two(j).wait_recv()
        mean = (gs2[j] + gr2[j]) * 0.5
        gr2[j] = mean
        sq2[...] += jnp.sum((mean * mean).reshape(-1, 8, mean.shape[1]), axis=0)
        send_one(j).wait_recv()
        mean = (gs1[j] + gr1[j]) * 0.5
        gr1[j] = mean
        sq1[...] += jnp.sum((mean * mean).reshape(-1, 8, mean.shape[1]), axis=0)

        @pl.when(j == 10)
        def _():
            free_and_fetch(0, 6, 0)

        @pl.when(j == 15)
        def _():
            free_and_fetch(6, 12, 1)

    sq_out[...] = jnp.full(sq_out.shape, jnp.sum(sq1[...]) + jnp.sum(sq2[...]), F32)
    mine = 2 * m + s
    others = ((peer_y, 2 * (1 - m) + s), (peer_c, 2 * m + 1 - s), (peer_d, 2 * (1 - m) + 1 - s))
    shares = [remote(sq_out, sq_in.at[mine], sq_send.at[k], sq_recv.at[mine], peer) for k, (peer, _) in enumerate(others)]
    for copy in shares:
        copy.start()
    free_and_fetch(12, n_chunk, 2)
    sq_in[mine] = sq_out[...]
    for peer, index in others:
        remote(sq_out, sq_in.at[index], sq_send.at[0], sq_recv.at[index], peer).wait_recv()
    total = (sq_in[0] + sq_in[1]) + (sq_in[2] + sq_in[3])
    clip[...] = jnp.minimum(1.0, max_norm[0] / (jnp.sqrt(total) + NORM_EPS))

    for j in range(n_chunk):
        send_two(j).wait_send()
    for copy in shares:
        copy.wait_send()

    @pl.when(is_last)
    def _():
        hand_over.wait_send()

    @pl.when(is_first)
    def _():
        scale = clip[0, 0]
        step_rate = rate[0]
        group, half = x_buf.shape[:2]
        n_micro = group // 2
        third = group // 2
        wide = 2 * width
        n_block = d_model // wide

        def arrive(p):
            base = lax.rem(p, 3) * 6
            for i in range(6):
                pltpu.make_async_copy(w1.at[:, :width], gs1.at[base + i], f_sem.at[base + i]).wait()

        def new_weights(p, means):
            base = lax.rem(p, 3) * 6
            parts = [adamw(scale, step_rate, gs1[base + h], gs1[base + 2 + h], gs1[base + 4 + h], means[h])[0].astype(BF16) for h in (0, 1)]
            return jnp.concatenate(parts, axis=1)

        def up_pair(p):
            new = new_weights(p, [gr1[2 * p], gr1[2 * p + 1]])
            act = gelu_parts(dot(x_buf[...].reshape(-1, d_model), new))[1].astype(BF16).astype(F32)
            cols = pl.ds(pl.multiple_of(lax.rem(p, n_block) * wide, wide), wide)
            gs2[pl.ds((p // n_block) * group, group), :, cols] = act.reshape(group, half, wide)

        def down_pair(p, upper):
            means = []
            for h in (0, 1):
                cols = pl.ds(pl.multiple_of((2 * ((p - n_up) // 2) + h) * width, width), width)
                means.append(gr2[upper * n_up:(upper + 1) * n_up, :, cols].reshape(d_model, width))
            new = new_weights(p, means)
            for lo in range(0, group, third):
                rows = gs2[upper * group + lo:upper * group + lo + third].reshape(-1, d_model).astype(BF16)
                res = dot(rows, new).reshape(third, half, wide)
                for g in range(third):
                    spot = slice(g * wide, (g + 1) * wide)
                    if upper:
                        part[lo // third, :, spot] += res[g]
                    else:
                        part[lo // third, :, spot] = res[g]

        def give_block(c):
            cols = pl.ds(pl.multiple_of(c * wide, wide), wide)
            for k in range(n_micro):
                even, odd = [part[g // third, :, g % third * wide:(g % third + 1) * wide] for g in (2 * k, 2 * k + 1)]
                gs2[2 * group + k, :, cols] = jnp.where(m == 0, even, odd)
                gs2[2 * group + n_micro + k, :, cols] = jnp.where(m == 0, odd, even)
            block_copy(c).start()

        def block_copy(c):
            cols = pl.ds(pl.multiple_of(c * wide, wide), wide)
            return remote(gs2.at[2 * group + n_micro:2 * group + 2 * n_micro, :, cols], got.at[:, :, cols], rs_send.at[c], rs_recv.at[c], peer_y)

        def ahead(p):
            @pl.when(p < n_pair)
            def _():
                fetch(p)

        load_x.wait()

        @pl.loop(0, n_up)
        def _(p):
            arrive(p)
            up_pair(p)
            ahead(p + 3)

        @pl.loop(0, n_block)
        def _(c):
            for upper in (0, 1):
                p = n_up + 2 * c + upper
                arrive(p)
                down_pair(p, upper)
                ahead(p + 3)
            give_block(c)

        for c in range(n_block):
            block_copy(c).wait_recv()
            cols = slice(c * wide, (c + 1) * wide)
            for k in range(n_micro):
                rows = x_buf[2 * k + m, :, cols].astype(F32)
                x_buf[k, :, cols] = (rows + (gs2[2 * group + k, :, cols] + got[k, :, cols])).astype(BF16)
        store = pltpu.make_async_copy(x_buf.at[:n_micro], act_half, row_sem)
        store.start()
        for c in range(n_block):
            block_copy(c).wait_send()
        store.wait()


def update_kernel(clip, rate, w1, m1, v1, gb1, w2, m2, v2, gb2, nw1, nm1, nv1, nw2, nm2, nv2, keep1, keep2, ring, in_sem, out_sem):
    n_up, deep, wide = gb1.shape
    n_slot = ring.shape[1]
    last = 2 * n_up
    block = deep // gb2.shape[1]
    scale = clip[0, 0]
    step_rate = rate[0]

    def place(i):
        col = pl.multiple_of(((i - n_up) // 2) * wide, wide)
        row = pl.multiple_of(lax.rem(i - n_up, 2) * deep, deep)
        return pl.ds(row, deep), pl.ds(col, wide)

    def start(i, fetch):
        slot = lax.rem(i, n_slot)
        sem = in_sem if fetch else out_sem

        def go(k, far):
            near = ring.at[k, slot]
            pair = (far, near) if fetch else (near, far)
            pltpu.make_async_copy(*pair, sem.at[k, slot]).start()

        @pl.when(i < n_up)
        def _():
            cols = pl.ds(pl.multiple_of(i * wide, wide), wide)
            for k, ref in enumerate((w1, m1, v1) if fetch else (nw1, nm1, nv1)):
                go(k, ref.at[0, :, cols])

        @pl.when(i >= n_up)
        def _():
            rows, cols = place(i)
            for k, ref in enumerate((w2, m2, v2) if fetch else (nw2, nm2, nv2)):
                go(k, ref.at[0, rows, cols])

    def finish(i, fetch):
        slot = lax.rem(i, n_slot)
        for k, ref in enumerate((w2, m2, v2) if fetch else (nw2, nm2, nv2)):
            far, near = ref.at[0, :deep, :wide], ring.at[k, slot]
            sem = (in_sem if fetch else out_sem).at[k, slot]
            (pltpu.make_async_copy(far, near, sem) if fetch else pltpu.make_async_copy(near, far, sem)).wait()

    for i in range(AHEAD):
        start(jnp.int32(i), True)

    def step(slot, mean):
        new, mom, sec = adamw(scale, step_rate, ring[0, slot], ring[1, slot], ring[2, slot], mean)
        ring[0, slot] = new
        ring[1, slot] = mom
        ring[2, slot] = sec
        return new

    @pl.loop(0, last)
    def _(i):
        slot = lax.rem(i, n_slot)
        finish(i, True)

        @pl.when(i < n_up)
        def _():
            keep1[i] = step(slot, gb1[i])

        @pl.when(i >= n_up)
        def _():
            cols = place(i)[1]
            rows = pl.ds(lax.rem(i - n_up, 2) * block, block)
            new = step(slot, gb2[rows, :, cols].reshape(deep, wide))
            keep2[rows, :, cols] = new.reshape(block, -1, wide)

        start(i, False)

        @pl.when(i + AHEAD < last)
        def _():
            @pl.when(i + AHEAD - n_slot >= 0)
            def _():
                finish(i + AHEAD - n_slot, False)
            start(i + AHEAD, True)

    for i in range(last - n_slot, last):
        finish(jnp.int32(i), False)


def forward_kernel(from_core, from_diag, new1, new2, y,
                   w1, w2, hid, act, own_half, peer_half, part, part_in,
                   p_send, p_recv, y_send, y_recv, g_send, g_recv, f_send, f_recv, ready):
    m, d, s = positions()
    n_micro, half, d_model = own_half.shape
    n_chunk, _, width = w1.shape
    n_block = d_model // width
    peer_y = (1 - m, d, s)
    peer_c = (m, d, 1 - s)
    barrier = pltpu.get_barrier_semaphore()

    @pl.when(s == 1)
    def _():
        pl.semaphore_signal(barrier, inc=1, device_id=peer_y, device_id_type=MESH)
        pl.semaphore_signal(barrier, inc=1, device_id=peer_c, device_id_type=MESH)

    pl.semaphore_wait(barrier, 1)

    @pl.when(s == 0)
    def _():
        pl.semaphore_signal(ready, inc=1, device_id=peer_c, device_id_type=MESH)

    mine = pl.ds(pl.multiple_of(m * half, half), half)
    theirs = pl.ds(pl.multiple_of((1 - m) * half, half), half)

    def span(c):
        return pl.ds(pl.multiple_of(c * width, width), width)

    def send_part(k, c):
        return remote(part.at[k, theirs, span(c)], part_in.at[k, :, span(c)], p_send.at[k, c], p_recv.at[k, c], peer_y)

    def swap_y(k, c):
        return remote(own_half.at[k, :, span(c)], peer_half.at[k, :, span(c)], y_send.at[k, c], y_recv.at[k, c], peer_y)

    def give_own(k):
        return remote(own_half.at[k], y.at[k, mine, :], g_send.at[k], g_recv.at[k], peer_c)

    def pass_on(k):
        return remote(peer_half.at[k], y.at[k, theirs, :], f_send.at[k], f_recv.at[k], peer_c)

    @pl.when(s == 0)
    def _():
        for k in range(n_micro):
            give_own(k).wait_recv()
            pass_on(k).wait_recv()

    @pl.when(s == 1)
    def _():
        act[:, mine, :] = from_core[...]
        act[:, theirs, :] = from_diag[...]

        for k in range(n_micro):
            @pl.loop(0, n_chunk)
            def _(j):
                if k == 0:
                    w1[j] = jnp.concatenate([new1[2 * j].astype(BF16), new1[2 * j + 1].astype(BF16)], axis=1)
                hid[:, span(j)] = gelu_parts(dot(act[k], w1[j]))[1].astype(BF16)

            @pl.loop(0, n_block)
            def _(c):
                if k == 0:
                    w2[:, span(c)] = new2[:, :, span(c)].reshape(-1, width).astype(BF16)
                part[k, :, span(c)] = dot(hid[...], w2[:, span(c)])
                send_part(k, c).start()

        for k in range(n_micro):
            @pl.loop(0, n_block)
            def _(c):
                send_part(k, c).wait_recv()
                out = act[k, mine, span(c)].astype(F32) + (part[k, mine, span(c)] + part_in[k, :, span(c)])
                own_half[k, :, span(c)] = out.astype(BF16)
                swap_y(k, c).start()

        pl.semaphore_wait(ready, 1)
        for k in range(n_micro):
            give_own(k).start()
            y[k, mine, :] = own_half[k]
        for k in range(n_micro):
            @pl.loop(0, n_block)
            def _(c):
                swap_y(k, c).wait_recv()

            pass_on(k).start()
            y[k, theirs, :] = peer_half[k]
        for k in range(n_micro):
            @pl.loop(0, n_block)
            def _(c):
                send_part(k, c).wait_send()
                swap_y(k, c).wait_send()

            give_own(k).wait_send()
            pass_on(k).wait_send()


def solution(mesh):
    up_spec = P('stage', None, 'model')
    down_spec = P('stage', 'model', None)
    row_spec = P(None, 'data', None)
    in_specs = (up_spec, down_spec, up_spec, down_spec, up_spec, down_spec, P('data', 'stage', None, 'model'), P('data', 'stage', 'model', None), P('stage', 'data', None), P('data', None), row_spec, P(None), P(None))
    out_specs = (up_spec, down_spec, up_spec, down_spec, up_spec, down_spec, row_spec)

    def device_step(w_up, w_down, m_up, m_down, v_up, v_down, g_up, g_down, acts_last, grad_out, x_next, learn_rate, max_norm):
        d_model, ff = w_up.shape[1:]
        rows = grad_out.shape[0]
        n_micro = x_next.shape[0]
        width = CHUNK
        n_chunk = ff // width
        half = rows // 2
        hbm = pl.BlockSpec(memory_space=pl.ANY)
        vmem = pl.BlockSpec(memory_space=pltpu.VMEM)
        smem = pl.BlockSpec(memory_space=pltpu.SMEM)
        dma = pltpu.SemaphoreType.DMA
        resident = 4 * 2 * d_model * ff
        n_block = d_model // (2 * width)

        mean_up, mean_down, clip, act_half = pl.pallas_call(
            functools.partial(grad_kernel, n_chunk, width),
            out_shape=(pltpu.VMEM((n_chunk, d_model, width), F32),
                       pltpu.VMEM((n_chunk, width, d_model), F32),
                       jax.ShapeDtypeStruct((8, 128), F32),
                       jax.ShapeDtypeStruct((n_micro, half, d_model), BF16)),
            in_specs=[hbm] * 11 + [smem, smem],
            out_specs=(vmem, vmem, vmem, hbm),
            scratch_shapes=[
                pltpu.VMEM((n_chunk, d_model, width), F32),
                pltpu.VMEM((n_chunk, width, d_model), F32),
                pltpu.VMEM((2, d_model, width), F32),
                pltpu.VMEM((2, width, d_model), F32),
                pltpu.VMEM((2, half, d_model), F32),
                pltpu.VMEM((n_micro, half, d_model), F32),
                pltpu.VMEM((2 * n_micro, half, d_model), BF16),
                pltpu.VMEM((8, width), F32),
                pltpu.VMEM((8, d_model), F32),
                pltpu.VMEM((8, 128), F32),
                pltpu.VMEM((4, 8, 128), F32),
                dma((2, 2)), dma((2, 2)),
                dma((n_chunk,)), dma((n_chunk,)), dma((n_chunk,)), dma((n_chunk,)),
                dma((2,)), dma((2,)), dma((3,)), dma((4,)),
                dma(()), dma(()), dma((18,)), dma((n_block,)), dma((n_block,)),
            ],
            compiler_params=pltpu.CompilerParams(collective_id=0, has_side_effects=True, vmem_limit_bytes=VMEM_MAX - resident - SPARE),
            name="grad_exchange",
        )(w_up[0], w_down[0], g_up[0, 0], g_down[0, 0], m_up[0], v_up[0], m_down[0], v_down[0], acts_last.reshape(2, half, d_model), grad_out.reshape(2, half, d_model), x_next.reshape(2 * n_micro, half, d_model), max_norm, learn_rate)

        from_diag = lax.ppermute(act_half, ('model', 'stage'), [(0, 3), (2, 1)])
        from_core = lax.ppermute(act_half, ('model', 'stage'), [(0, 1), (2, 3)])

        def stay(array):
            return pltpu.with_memory_space_constraint(array, pltpu.VMEM)

        up_out = jax.ShapeDtypeStruct(w_up.shape, F32)
        down_out = jax.ShapeDtypeStruct(w_down.shape, F32)
        nw1, nm1, nv1, nw2, nm2, nv2, new1, new2 = pl.pallas_call(
            update_kernel,
            out_shape=(up_out, up_out, up_out, down_out, down_out, down_out,
                       pltpu.VMEM(mean_up.shape, F32), pltpu.VMEM(mean_down.shape, F32)),
            in_specs=[smem, smem, hbm, hbm, hbm, vmem, hbm, hbm, hbm, vmem],
            out_specs=(hbm,) * 6 + (vmem, vmem),
            input_output_aliases={5: 6, 9: 7},
            scratch_shapes=[pltpu.VMEM((3, SLOTS, d_model, width), F32), dma((3, SLOTS)), dma((3, SLOTS))],
            compiler_params=pltpu.CompilerParams(vmem_limit_bytes=VMEM_MAX - resident - SPARE),
            cost_estimate=pl.CostEstimate(flops=2000 * d_model * ff, bytes_accessed=48 * d_model * ff, transcendentals=4 * d_model * ff),
            name="update",
        )(clip, learn_rate, w_up, m_up, v_up, stay(mean_up), w_down, m_down, v_down, stay(mean_down))

        f_width = 2 * width
        f_chunk = ff // f_width
        y_next = pl.pallas_call(
            forward_kernel,
            out_shape=pltpu.VMEM(x_next.shape, BF16),
            in_specs=[vmem, vmem, vmem, vmem],
            out_specs=vmem,
            scratch_shapes=[
                pltpu.VMEM((f_chunk, d_model, f_width), BF16),
                pltpu.VMEM((ff, d_model), BF16),
                pltpu.VMEM((rows, ff), BF16),
                pltpu.VMEM((n_micro, rows, d_model), BF16),
                pltpu.VMEM((n_micro, half, d_model), BF16),
                pltpu.VMEM((n_micro, half, d_model), BF16),
                pltpu.VMEM((n_micro, rows, d_model), F32),
                pltpu.VMEM((n_micro, half, d_model), F32),
                dma((n_micro, n_block)), dma((n_micro, n_block)), dma((n_micro, n_block)), dma((n_micro, n_block)),
                dma((n_micro,)), dma((n_micro,)), dma((n_micro,)), dma((n_micro,)),
                pltpu.SemaphoreType.REGULAR,
            ],
            compiler_params=pltpu.CompilerParams(collective_id=1, has_side_effects=True, vmem_limit_bytes=VMEM_MAX - resident - SPARE),
            name="forward_exchange",
        )(from_core, from_diag, stay(new1), stay(new2))
        return nw1, nw2, nm1, nm2, nv1, nv2, y_next

    return jax.shard_map(device_step, mesh=mesh, in_specs=in_specs, out_specs=out_specs, check_vma=False)
```

```python
import functools

import jax
import jax.numpy as jnp
from jax import lax
from jax.experimental import pallas as pl
from jax.experimental.pallas import tpu as pltpu
from jax.sharding import PartitionSpec as P

ADAM_STEP = 10
BETA_ONE = 0.9
BETA_TWO = 0.95
ADAM_EPS = 1e-8
WEIGHT_DECAY = 0.1
NORM_EPS = 1e-6
ONE_CORR = 1.0 - BETA_ONE ** ADAM_STEP
TWO_CORR = 1.0 - BETA_TWO ** ADAM_STEP
ROOT_EPS = ADAM_EPS * TWO_CORR ** 0.5
ROOT_GAIN = TWO_CORR ** 0.5 / ONE_CORR
TINY = 1.1754944e-38
HUGE = 3.4028235e38
GELU_A = 0.7978845608028654
GELU_B = 0.044715
NT = (((1,), (1,)), ((), ()))
TN = (((0,), (0,)), ((), ()))
MESH = pl.DeviceIdType.MESH
VMEM_MAX = 67_043_328
CHUNK = 128
SLOTS = 8
AHEAD = 5
SPARE = 5 << 19
F32 = jnp.float32
BF16 = jnp.bfloat16


def gelu_parts(z):
    t = jnp.tanh(GELU_A * (z + GELU_B * (z * z * z)))
    return t, z * (0.5 * (1.0 + t))


def gelu_slope(z, t):
    return 0.5 * (1.0 + t) + 0.5 * z * (1.0 - t * t) * (GELU_A * (1.0 + 3.0 * GELU_B * z * z))


def dot(a, b, dims=(((1,), (0,)), ((), ()))):
    return lax.dot_general(a, b, dims, preferred_element_type=F32)


def positions():
    return lax.axis_index("model"), lax.axis_index("data"), lax.axis_index("stage")


def entry_barrier(peers):
    barrier = pltpu.get_barrier_semaphore()
    for peer in peers:
        pl.semaphore_signal(barrier, inc=1, device_id=peer, device_id_type=MESH)
    pl.semaphore_wait(barrier, len(peers))


def remote(src, dst, send, recv, peer):
    return pltpu.make_async_remote_copy(src_ref=src, dst_ref=dst, send_sem=send, recv_sem=recv, device_id=peer, device_id_type=MESH)


def adamw(scale, rate, w, mom, sec, mean):
    grad = scale * mean
    mom_new = BETA_ONE * mom + (1.0 - BETA_ONE) * grad
    sec_new = BETA_TWO * sec + ((1.0 - BETA_TWO) * grad) * grad
    root = sec_new * lax.rsqrt(jnp.minimum(sec_new + TINY, HUGE))
    w_new = w * (1.0 - rate * WEIGHT_DECAY) - (rate * ROOT_GAIN) * (mom_new / (root + ROOT_EPS))
    return w_new, mom_new, sec_new


def grad_kernel(n_chunk, width, w1, w2, g1, g2, m1, v1, m2, v2, acts, dy, x, max_norm, rate,
                gr1, gr2, gs1, clip, act_half,
                gs2, w1b, w2b, part, got, x_buf, sq1, sq2, sq_out, sq_in,
                w_sem, g_sem, send1, send2, recv1, recv2, part_sem, gvec_sem, sq_send, sq_recv,
                row_sem, act_sem, f_sem, rs_send, rs_recv):
    m, d, s = positions()
    peer_x = (m, 1 - d, s)
    peer_y = (1 - m, d, s)
    peer_c = (m, d, 1 - s)
    peer_d = (1 - m, d, 1 - s)
    d_model = w1.shape[0]
    is_last = s == 1
    is_first = s == 0

    def loads(j):
        slot = lax.rem(j, 2)
        cols = pl.ds(pl.multiple_of(j * width, width), width)
        return (pltpu.make_async_copy(w1.at[:, cols], w1b.at[slot], w_sem.at[0, slot]),
                pltpu.make_async_copy(w2.at[cols, :], w2b.at[slot], w_sem.at[1, slot]),
                pltpu.make_async_copy(g2.at[cols, :], gs2.at[j], g_sem.at[0, slot]),
                pltpu.make_async_copy(g1.at[:, cols], gs1.at[j], g_sem.at[1, slot]))

    acts_buf, gvec = x_buf.at[2:4], x_buf.at[4:6]
    load_acts = pltpu.make_async_copy(acts, acts_buf, act_sem)
    load_dy = pltpu.make_async_copy(dy, gvec, row_sem)
    load_x = pltpu.make_async_copy(x, x_buf, row_sem)

    load_acts.start()

    @pl.when(is_last)
    def _():
        load_dy.start()

    for copy in loads(0):
        copy.start()
    entry_barrier((peer_x, peer_y, peer_c, peer_d))
    for copy in loads(1):
        copy.start()

    hand_over = remote(x_buf.at[:2], gvec, gvec_sem.at[0], gvec_sem.at[1], peer_c)
    swap_part = remote(part, got.at[:2], part_sem.at[0], part_sem.at[1], peer_y)

    @pl.when(is_last)
    def _():
        part[...] = jnp.zeros_like(part)
        load_dy.wait()

    @pl.when(is_first)
    def _():
        hand_over.wait_recv()

    load_acts.wait()

    def send_two(j):
        return remote(gs2.at[j], gr2.at[j], send2.at[j], recv2.at[j], peer_x)

    def send_one(j):
        return remote(gs1.at[j], gr1.at[j], send1.at[j], recv1.at[j], peer_x)

    @pl.loop(0, n_chunk)
    def _(j):
        slot = lax.rem(j, 2)
        copies = loads(j)
        copies[0].wait()
        up = w1b[slot].astype(BF16)
        rows = acts_buf[...].reshape(-1, d_model)
        grad = gvec[...].reshape(-1, d_model)
        z = dot(rows, up)
        t, act = gelu_parts(z)
        hid = act.astype(BF16)
        copies[2].wait()
        gs2[j] += dot(hid, grad, TN)
        send_two(j).start()
        copies[1].wait()
        grad_hid = dot(grad, w2b[slot].astype(BF16), NT)
        grad_pre = (gelu_slope(z, t) * grad_hid).astype(BF16)
        copies[3].wait()
        gs1[j] += dot(rows, grad_pre, TN)
        send_one(j).start()

        @pl.when(is_last)
        def _():
            part[...] += dot(grad_pre, up, NT).reshape(part.shape)

        @pl.when(j + 2 < n_chunk)
        def _():
            for copy in loads(j + 2):
                copy.start()

    @pl.when(is_last)
    def _():
        swap_part.start()
        swap_part.wait()
        x_buf[:2] = (gvec[...].astype(F32) + (part[...] + got[:2])).astype(BF16)
        hand_over.start()

    @pl.when(is_first)
    def _():
        load_x.start()

    n_up = n_chunk // 2
    n_pair = 2 * n_up

    def fetch(p):
        base = lax.rem(p, 3) * 6

        @pl.when(p < n_up)
        def _():
            for q, ref in enumerate((w1, m1, v1)):
                for h in (0, 1):
                    cols = pl.ds(pl.multiple_of((2 * p + h) * width, width), width)
                    pltpu.make_async_copy(ref.at[:, cols], gs1.at[base + 2 * q + h], f_sem.at[base + 2 * q + h]).start()

        @pl.when(p >= n_up)
        def _():
            rows = pl.ds(pl.multiple_of(lax.rem(p - n_up, 2) * d_model, d_model), d_model)
            for q, ref in enumerate((w2, m2, v2)):
                for h in (0, 1):
                    cols = pl.ds(pl.multiple_of((2 * ((p - n_up) // 2) + h) * width, width), width)
                    pltpu.make_async_copy(ref.at[rows, cols], gs1.at[base + 2 * q + h], f_sem.at[base + 2 * q + h]).start()

    def arrive(p):
        base = lax.rem(p, 3) * 6
        for i in range(6):
            pltpu.make_async_copy(w1.at[:, :width], gs1.at[base + i], f_sem.at[base + i]).wait()

    def free_and_fetch(lo, hi, p):
        for i in range(lo, hi):
            send_one(i).wait_send()

        fetch(p)

    sq1[...] = jnp.zeros_like(sq1)
    sq2[...] = jnp.zeros_like(sq2)

    @pl.loop(0, n_chunk)
    def _(j):
        send_two(j).wait_recv()
        mean = (gs2[j] + gr2[j]) * 0.5
        gr2[j] = mean
        sq2[...] += jnp.sum((mean * mean).reshape(-1, 8, mean.shape[1]), axis=0)
        send_one(j).wait_recv()
        mean = (gs1[j] + gr1[j]) * 0.5
        gr1[j] = mean
        sq1[...] += jnp.sum((mean * mean).reshape(-1, 8, mean.shape[1]), axis=0)

        @pl.when(j == 10)
        def _():
            free_and_fetch(0, 6, 18 * s)

        @pl.when(j == 15)
        def _():
            free_and_fetch(6, 12, 1 + 18 * s)

    sq_out[...] = jnp.full(sq_out.shape, jnp.sum(sq1[...]) + jnp.sum(sq2[...]), F32)
    mine = 2 * m + s
    others = ((peer_y, 2 * (1 - m) + s), (peer_c, 2 * m + 1 - s), (peer_d, 2 * (1 - m) + 1 - s))
    shares = [remote(sq_out, sq_in.at[mine], sq_send.at[k], sq_recv.at[mine], peer) for k, (peer, _) in enumerate(others)]
    for copy in shares:
        copy.start()
    free_and_fetch(12, n_chunk, 2 + 15 * s)
    sq_in[mine] = sq_out[...]
    for peer, index in others:
        remote(sq_out, sq_in.at[index], sq_send.at[0], sq_recv.at[index], peer).wait_recv()
    total = (sq_in[0] + sq_in[1]) + (sq_in[2] + sq_in[3])
    clip[...] = jnp.minimum(1.0, max_norm[0] / (jnp.sqrt(total) + NORM_EPS))

    for j in range(n_chunk):
        send_two(j).wait_send()
    for copy in shares:
        copy.wait_send()

    @pl.when(is_last)
    def _():
        hand_over.wait_send()
        for p in (18, 19, 17):
            arrive(jnp.int32(p))

    @pl.when(is_first)
    def _():
        scale = clip[0, 0]
        step_rate = rate[0]
        group, half = x_buf.shape[:2]
        n_micro = group // 2
        third = group // 2
        wide = 2 * width
        n_block = d_model // wide

        def new_weights(p, means):
            base = lax.rem(p, 3) * 6
            parts = [adamw(scale, step_rate, gs1[base + h], gs1[base + 2 + h], gs1[base + 4 + h], means[h])[0].astype(BF16) for h in (0, 1)]
            return jnp.concatenate(parts, axis=1)

        def up_pair(p):
            new = new_weights(p, [gr1[2 * p], gr1[2 * p + 1]])
            act = gelu_parts(dot(x_buf[...].reshape(-1, d_model), new))[1].astype(BF16).astype(F32)
            cols = pl.ds(pl.multiple_of(lax.rem(p, n_block) * wide, wide), wide)
            gs2[pl.ds((p // n_block) * group, group), :, cols] = act.reshape(group, half, wide)

        def down_pair(p, upper):
            means = []
            for h in (0, 1):
                cols = pl.ds(pl.multiple_of((2 * ((p - n_up) // 2) + h) * width, width), width)
                means.append(gr2[upper * n_up:(upper + 1) * n_up, :, cols].reshape(d_model, width))
            new = new_weights(p, means)
            for lo in range(0, group, third):
                rows = gs2[upper * group + lo:upper * group + lo + third].reshape(-1, d_model).astype(BF16)
                res = dot(rows, new).reshape(third, half, wide)
                for g in range(third):
                    spot = slice(g * wide, (g + 1) * wide)
                    if upper:
                        part[lo // third, :, spot] += res[g]
                    else:
                        part[lo // third, :, spot] = res[g]

        def give_block(c):
            cols = pl.ds(pl.multiple_of(c * wide, wide), wide)
            for k in range(n_micro):
                even, odd = [part[g // third, :, g % third * wide:(g % third + 1) * wide] for g in (2 * k, 2 * k + 1)]
                gs2[2 * group + k, :, cols] = jnp.where(m == 0, even, odd)
                gs2[2 * group + n_micro + k, :, cols] = jnp.where(m == 0, odd, even)
            block_copy(c).start()

        def block_copy(c):
            cols = pl.ds(pl.multiple_of(c * wide, wide), wide)
            return remote(gs2.at[2 * group + n_micro:2 * group + 2 * n_micro, :, cols], got.at[:, :, cols], rs_send.at[c], rs_recv.at[c], peer_y)

        def ahead(p):
            @pl.when(p < n_pair)
            def _():
                fetch(p)

        load_x.wait()

        @pl.loop(0, n_up)
        def _(p):
            arrive(p)
            up_pair(p)
            ahead(p + 3)

        @pl.loop(0, n_block)
        def _(c):
            for upper in (0, 1):
                p = n_up + 2 * c + upper
                arrive(p)
                down_pair(p, upper)
                ahead(p + 3)
            give_block(c)

        for c in range(n_block):
            block_copy(c).wait_recv()
            cols = slice(c * wide, (c + 1) * wide)
            for k in range(n_micro):
                rows = x_buf[2 * k + m, :, cols].astype(F32)
                x_buf[k, :, cols] = (rows + (gs2[2 * group + k, :, cols] + got[k, :, cols])).astype(BF16)
        store = pltpu.make_async_copy(x_buf.at[:n_micro], act_half, row_sem)
        store.start()
        for c in range(n_block):
            block_copy(c).wait_send()
        store.wait()


def update_kernel(clip, rate, w1, m1, v1, gb1, w2, m2, v2, gb2, held, nw1, nm1, nv1, nw2, nm2, nv2, keep1, keep2, held_out, ring, in_sem, out_sem, held_sem):
    n_up, deep, wide = gb1.shape
    n_slot = ring.shape[1]
    near = [(place, h) for place in range(3) for h in (0, 1)]
    last = 2 * n_up - len(near)
    block = deep // gb2.shape[1]
    scale = clip[0, 0]
    step_rate = rate[0]

    def place(i):
        i = i + i // (last - 1)
        col = pl.multiple_of(((i - n_up) // 2) * wide, wide)
        row = pl.multiple_of(lax.rem(i - n_up, 2) * deep, deep)
        return pl.ds(row, deep), pl.ds(col, wide)

    def start(i, fetch):
        slot = lax.rem(i, n_slot)
        sem = in_sem if fetch else out_sem

        def go(k, far):
            here = ring.at[k, slot]
            pair = (far, here) if fetch else (here, far)
            pltpu.make_async_copy(*pair, sem.at[k, slot]).start()

        @pl.when(i < n_up)
        def _():
            cols = pl.ds(pl.multiple_of(i * wide, wide), wide)
            for k, ref in enumerate((w1, m1, v1) if fetch else (nw1, nm1, nv1)):
                go(k, ref.at[0, :, cols])

        @pl.when(i >= n_up)
        def _():
            rows, cols = place(i)
            for k, ref in enumerate((w2, m2, v2) if fetch else (nw2, nm2, nv2)):
                go(k, ref.at[0, rows, cols])

    def finish(i, fetch):
        slot = lax.rem(i, n_slot)
        for k, ref in enumerate((w2, m2, v2) if fetch else (nw2, nm2, nv2)):
            far, here = ref.at[0, :deep, :wide], ring.at[k, slot]
            sem = (in_sem if fetch else out_sem).at[k, slot]
            (pltpu.make_async_copy(far, here, sem) if fetch else pltpu.make_async_copy(here, far, sem)).wait()

    for i in range(AHEAD):
        start(jnp.int32(i), True)

    def step(slot, mean):
        new, mom, sec = adamw(scale, step_rate, ring[0, slot], ring[1, slot], ring[2, slot], mean)
        ring[0, slot] = new
        ring[1, slot] = mom
        ring[2, slot] = sec
        return new

    def held_copies(place, h):
        col, upper = {2: (6, 1), 0: (8, 0), 1: (8, 1)}[place]
        rows, cols = slice(upper * deep, (upper + 1) * deep), slice((col + h) * wide, (col + h + 1) * wide)
        return upper, cols, [pltpu.make_async_copy(held_out.at[6 * place + 2 * k + h], ref.at[0, rows, cols], held_sem.at[6 * place + 2 * k + h])
                             for k, ref in enumerate((nw2, nm2, nv2))]

    for spot, h in near:
        upper, cols, copies = held_copies(spot, h)
        rows = slice(upper * block, (upper + 1) * block)
        base = 6 * spot + h
        new, mom, sec = adamw(scale, step_rate, held[base], held[base + 2], held[base + 4], gb2[rows, :, cols].reshape(deep, wide))
        held_out[base] = new
        held_out[base + 2] = mom
        held_out[base + 4] = sec
        keep2[rows, :, cols] = new.reshape(block, -1, wide)
        for copy in copies:
            copy.start()

    @pl.loop(0, last)
    def _(i):
        slot = lax.rem(i, n_slot)
        finish(i, True)

        @pl.when(i < n_up)
        def _():
            keep1[i] = step(slot, gb1[i])

        @pl.when(i >= n_up)
        def _():
            cols = place(i)[1]
            rows = pl.ds(lax.rem(i + i // (last - 1) - n_up, 2) * block, block)
            new = step(slot, gb2[rows, :, cols].reshape(deep, wide))
            keep2[rows, :, cols] = new.reshape(block, -1, wide)

        start(i, False)

        @pl.when(i + AHEAD < last)
        def _():
            @pl.when(i + AHEAD - n_slot >= 0)
            def _():
                finish(i + AHEAD - n_slot, False)
            start(i + AHEAD, True)

    for i in range(last - n_slot, last):
        finish(jnp.int32(i), False)
    for spot, h in near:
        for copy in held_copies(spot, h)[2]:
            copy.wait()


def forward_kernel(from_core, from_diag, new1, new2, y,
                   hid, act, own_half, peer_half, part, part_in,
                   in_sem, p_send, p_recv, y_send, y_recv, g_send, g_recv, f_send, f_recv, ready):
    m, d, s = positions()
    n_micro, half, d_model = own_half.shape
    width = 2 * new1.shape[2]
    n_chunk, n_block = new1.shape[0] // 2, d_model // width
    peer_y = (1 - m, d, s)
    peer_c = (m, d, 1 - s)
    barrier = pltpu.get_barrier_semaphore()
    mine = pl.ds(pl.multiple_of(m * half, half), half)
    theirs = pl.ds(pl.multiple_of((1 - m) * half, half), half)
    rows_in = (pltpu.make_async_copy(from_core, act.at[:, mine, :], in_sem.at[0]),
               pltpu.make_async_copy(from_diag, act.at[:, theirs, :], in_sem.at[1]))

    @pl.when(s == 1)
    def _():
        for copy in rows_in:
            copy.start()
        pl.semaphore_signal(barrier, inc=1, device_id=peer_y, device_id_type=MESH)
        pl.semaphore_signal(barrier, inc=1, device_id=peer_c, device_id_type=MESH)

    pl.semaphore_wait(barrier, 1)

    @pl.when(s == 0)
    def _():
        pl.semaphore_signal(ready, inc=1, device_id=peer_c, device_id_type=MESH)

    def span(c):
        return pl.ds(pl.multiple_of(c * width, width), width)

    def send_part(k, c):
        return remote(part.at[k, theirs, span(c)], part_in.at[k, :, span(c)], p_send.at[k, c], p_recv.at[k, c], peer_y)

    def swap_y(k, c):
        return remote(own_half.at[k, :, span(c)], peer_half.at[k, :, span(c)], y_send.at[k, c], y_recv.at[k, c], peer_y)

    def give_own(k):
        return remote(own_half.at[k], y.at[k, mine, :], g_send.at[k], g_recv.at[k], peer_c)

    def pass_on(k):
        return remote(peer_half.at[k], y.at[k, theirs, :], f_send.at[k], f_recv.at[k], peer_c)

    @pl.when(s == 0)
    def _():
        for k in range(n_micro):
            give_own(k).wait_recv()
            pass_on(k).wait_recv()

    @pl.when(s == 1)
    def _():
        for copy in rows_in:
            copy.wait()

        for k in range(n_micro):
            @pl.loop(0, n_chunk)
            def _(j):
                up = jnp.concatenate([new1[2 * j].astype(BF16), new1[2 * j + 1].astype(BF16)], axis=1)
                hid[:, span(j)] = gelu_parts(dot(act[k], up))[1].astype(BF16)

            @pl.loop(0, n_block)
            def _(c):
                down = new2[:, :, span(c)].reshape(-1, width).astype(BF16)
                part[k, :, span(c)] = dot(hid[...], down)
                send_part(k, c).start()

        for k in range(n_micro):
            @pl.loop(0, n_block)
            def _(c):
                send_part(k, c).wait_recv()
                out = act[k, mine, span(c)].astype(F32) + (part[k, mine, span(c)] + part_in[k, :, span(c)])
                own_half[k, :, span(c)] = out.astype(BF16)
                swap_y(k, c).start()

        pl.semaphore_wait(ready, 1)
        for k in range(n_micro):
            give_own(k).start()
            y[k, mine, :] = own_half[k]
        for k in range(n_micro):
            @pl.loop(0, n_block)
            def _(c):
                swap_y(k, c).wait_recv()

            pass_on(k).start()
            y[k, theirs, :] = peer_half[k]
        for k in range(n_micro):
            @pl.loop(0, n_block)
            def _(c):
                send_part(k, c).wait_send()
                swap_y(k, c).wait_send()

            give_own(k).wait_send()
            pass_on(k).wait_send()


def solution(mesh):
    up_spec = P('stage', None, 'model')
    down_spec = P('stage', 'model', None)
    row_spec = P(None, 'data', None)
    in_specs = (up_spec, down_spec, up_spec, down_spec, up_spec, down_spec, P('data', 'stage', None, 'model'), P('data', 'stage', 'model', None), P('stage', 'data', None), P('data', None), row_spec, P(None), P(None))
    out_specs = (up_spec, down_spec, up_spec, down_spec, up_spec, down_spec, row_spec)

    def device_step(w_up, w_down, m_up, m_down, v_up, v_down, g_up, g_down, acts_last, grad_out, x_next, learn_rate, max_norm):
        d_model, ff = w_up.shape[1:]
        rows = grad_out.shape[0]
        n_micro = x_next.shape[0]
        width = CHUNK
        n_chunk = ff // width
        half = rows // 2
        hbm = pl.BlockSpec(memory_space=pl.ANY)
        vmem = pl.BlockSpec(memory_space=pltpu.VMEM)
        smem = pl.BlockSpec(memory_space=pltpu.SMEM)
        dma = pltpu.SemaphoreType.DMA
        resident = 4 * 3 * d_model * ff
        n_block = d_model // (2 * width)

        mean_up, mean_down, held, clip, act_half = pl.pallas_call(
            functools.partial(grad_kernel, n_chunk, width),
            out_shape=(pltpu.VMEM((n_chunk, d_model, width), F32),
                       pltpu.VMEM((n_chunk, width, d_model), F32),
                       pltpu.VMEM((n_chunk, d_model, width), F32),
                       jax.ShapeDtypeStruct((8, 128), F32),
                       jax.ShapeDtypeStruct((n_micro, half, d_model), BF16)),
            in_specs=[hbm] * 11 + [smem, smem],
            out_specs=(vmem, vmem, vmem, vmem, hbm),
            scratch_shapes=[
                pltpu.VMEM((n_chunk, width, d_model), F32),
                pltpu.VMEM((2, d_model, width), F32),
                pltpu.VMEM((2, width, d_model), F32),
                pltpu.VMEM((2, half, d_model), F32),
                pltpu.VMEM((n_micro, half, d_model), F32),
                pltpu.VMEM((2 * n_micro, half, d_model), BF16),
                pltpu.VMEM((8, width), F32),
                pltpu.VMEM((8, d_model), F32),
                pltpu.VMEM((8, 128), F32),
                pltpu.VMEM((4, 8, 128), F32),
                dma((2, 2)), dma((2, 2)),
                dma((n_chunk,)), dma((n_chunk,)), dma((n_chunk,)), dma((n_chunk,)),
                dma((2,)), dma((2,)), dma((3,)), dma((4,)),
                dma(()), dma(()), dma((18,)), dma((n_block,)), dma((n_block,)),
            ],
            compiler_params=pltpu.CompilerParams(collective_id=0, has_side_effects=True, vmem_limit_bytes=VMEM_MAX - resident - SPARE),
            name="grad_exchange",
        )(w_up[0], w_down[0], g_up[0, 0], g_down[0, 0], m_up[0], v_up[0], m_down[0], v_down[0], acts_last.reshape(2, half, d_model), grad_out.reshape(2, half, d_model), x_next.reshape(2 * n_micro, half, d_model), max_norm, learn_rate)

        from_diag = lax.ppermute(act_half, ('model', 'stage'), [(0, 3), (2, 1)])
        from_core = lax.ppermute(act_half, ('model', 'stage'), [(0, 1), (2, 3)])

        def stay(array):
            return pltpu.with_memory_space_constraint(array, pltpu.VMEM)

        up_out = jax.ShapeDtypeStruct(w_up.shape, F32)
        down_out = jax.ShapeDtypeStruct(w_down.shape, F32)
        nw1, nm1, nv1, nw2, nm2, nv2, new1, new2, _ = pl.pallas_call(
            update_kernel,
            out_shape=(up_out, up_out, up_out, down_out, down_out, down_out,
                       pltpu.VMEM(mean_up.shape, F32), pltpu.VMEM(mean_down.shape, F32), pltpu.VMEM(held.shape, F32)),
            in_specs=[smem, smem, hbm, hbm, hbm, vmem, hbm, hbm, hbm, vmem, vmem],
            out_specs=(hbm,) * 6 + (vmem, vmem, vmem),
            input_output_aliases={5: 6, 9: 7, 10: 8},
            scratch_shapes=[pltpu.VMEM((3, SLOTS, d_model, width), F32), dma((3, SLOTS)), dma((3, SLOTS)), dma((18,))],
            compiler_params=pltpu.CompilerParams(vmem_limit_bytes=VMEM_MAX - resident - SPARE),
            cost_estimate=pl.CostEstimate(flops=2000 * d_model * ff, bytes_accessed=48 * d_model * ff, transcendentals=4 * d_model * ff),
            name="update",
        )(clip, learn_rate, w_up, m_up, v_up, stay(mean_up), w_down, m_down, v_down, stay(mean_down), stay(held))

        y_next = pl.pallas_call(
            forward_kernel,
            out_shape=pltpu.VMEM(x_next.shape, BF16),
            in_specs=[hbm, hbm, vmem, vmem],
            out_specs=vmem,
            scratch_shapes=[
                pltpu.VMEM((rows, ff), BF16),
                pltpu.VMEM((n_micro, rows, d_model), BF16),
                pltpu.VMEM((n_micro, half, d_model), BF16),
                pltpu.VMEM((n_micro, half, d_model), BF16),
                pltpu.VMEM((n_micro, rows, d_model), F32),
                pltpu.VMEM((n_micro, half, d_model), F32),
                dma((2,)), dma((n_micro, n_block)), dma((n_micro, n_block)), dma((n_micro, n_block)), dma((n_micro, n_block)),
                dma((n_micro,)), dma((n_micro,)), dma((n_micro,)), dma((n_micro,)),
                pltpu.SemaphoreType.REGULAR,
            ],
            compiler_params=pltpu.CompilerParams(collective_id=1, has_side_effects=True, vmem_limit_bytes=VMEM_MAX - resident - SPARE),
            name="forward_exchange",
        )(from_core, from_diag, stay(new1), stay(new2))
        return nw1, nw2, nm1, nm2, nv1, nv2, y_next

    return jax.shard_map(device_step, mesh=mesh, in_specs=in_specs, out_specs=out_specs, check_vma=False)
```

```python
import functools

import jax
import jax.numpy as jnp
from jax import lax
from jax.experimental import pallas as pl
from jax.experimental.pallas import tpu as pltpu
from jax.sharding import PartitionSpec as P


ADAM_STEP = 10
BETA_ONE = 0.9
BETA_TWO = 0.95
ADAM_EPS = 1e-8
WEIGHT_DECAY = 0.1
NORM_EPS = 1e-6
ONE_CORR = 1.0 - BETA_ONE ** ADAM_STEP
TWO_CORR = 1.0 - BETA_TWO ** ADAM_STEP
ROOT_EPS = ADAM_EPS * TWO_CORR ** 0.5
ROOT_GAIN = TWO_CORR ** 0.5 / ONE_CORR
TINY = 1.1754944e-38
HUGE = 3.4028235e38
GELU_A = 0.7978845608028654
GELU_B = 0.044715
NT = (((1,), (1,)), ((), ()))
TN = (((0,), (0,)), ((), ()))
MESH = pl.DeviceIdType.MESH
VMEM_MAX = 67_043_328
CHUNK = 128
SLOTS = 8
AHEAD = 5
SPARE = 5 << 19
F32 = jnp.float32
BF16 = jnp.bfloat16


def gelu_parts(z):
    t = jnp.tanh(GELU_A * (z + GELU_B * (z * z * z)))
    return t, z * (0.5 * (1.0 + t))


def gelu_slope(z, t):
    return 0.5 * (1.0 + t) + 0.5 * z * (1.0 - t * t) * (GELU_A * (1.0 + 3.0 * GELU_B * z * z))


def dot(a, b, dims=(((1,), (0,)), ((), ()))):
    return lax.dot_general(a, b, dims, preferred_element_type=F32)


def positions():
    return lax.axis_index("model"), lax.axis_index("data"), lax.axis_index("stage")


def entry_barrier(peers):
    barrier = pltpu.get_barrier_semaphore()
    for peer in peers:
        pl.semaphore_signal(barrier, inc=1, device_id=peer, device_id_type=MESH)
    pl.semaphore_wait(barrier, len(peers))


def remote(src, dst, send, recv, peer):
    return pltpu.make_async_remote_copy(src_ref=src, dst_ref=dst, send_sem=send, recv_sem=recv, device_id=peer, device_id_type=MESH)


def adamw(scale, rate, w, mom, sec, mean):
    grad = scale * mean
    mom_new = BETA_ONE * mom + (1.0 - BETA_ONE) * grad
    sec_new = BETA_TWO * sec + ((1.0 - BETA_TWO) * grad) * grad
    root = sec_new * lax.rsqrt(jnp.minimum(sec_new + TINY, HUGE))
    w_new = w * (1.0 - rate * WEIGHT_DECAY) - (rate * ROOT_GAIN) * (mom_new / (root + ROOT_EPS))
    return w_new, mom_new, sec_new


def grad_kernel(n_chunk, width, w1, w2, g1, g2, m1, v1, m2, v2, acts, dy, x, max_norm, rate,
                gr1, gr2, gs1, clip, act_half,
                gs2, w1b, w2b, part, got, x_buf, sq1, sq2, sq_out, sq_in,
                w_sem, g_sem, send1, send2, recv1, recv2, part_sem, gvec_sem, sq_send, sq_recv,
                row_sem, act_sem, f_sem, rs_send, rs_recv):
    m, d, s = positions()
    peer_x = (m, 1 - d, s)
    peer_y = (1 - m, d, s)
    peer_c = (m, d, 1 - s)
    peer_d = (1 - m, d, 1 - s)
    d_model = w1.shape[0]
    is_last = s == 1
    is_first = s == 0

    def loads(j):
        slot = lax.rem(j, 2)
        cols = pl.ds(pl.multiple_of(j * width, width), width)
        return (pltpu.make_async_copy(w1.at[:, cols], w1b.at[slot], w_sem.at[0, slot]),
                pltpu.make_async_copy(w2.at[cols, :], w2b.at[slot], w_sem.at[1, slot]),
                pltpu.make_async_copy(g2.at[cols, :], gs2.at[j], g_sem.at[0, slot]),
                pltpu.make_async_copy(g1.at[:, cols], gs1.at[j], g_sem.at[1, slot]))

    acts_buf, gvec = x_buf.at[2:4], x_buf.at[4:6]
    load_acts = pltpu.make_async_copy(acts, acts_buf, act_sem)
    load_dy = pltpu.make_async_copy(dy, gvec, row_sem)
    load_x = pltpu.make_async_copy(x, x_buf, row_sem)

    load_acts.start()

    @pl.when(is_last)
    def _():
        load_dy.start()

    for copy in loads(0):
        copy.start()
    entry_barrier((peer_x, peer_y, peer_c, peer_d))
    for copy in loads(1):
        copy.start()

    hand_over = remote(x_buf.at[:2], gvec, gvec_sem.at[0], gvec_sem.at[1], peer_c)
    swap_part = remote(part, got.at[:2], part_sem.at[0], part_sem.at[1], peer_y)

    @pl.when(is_last)
    def _():
        part[...] = jnp.zeros_like(part)
        load_dy.wait()

    @pl.when(is_first)
    def _():
        hand_over.wait_recv()

    load_acts.wait()

    def send_two(j):
        return remote(gs2.at[j], gr2.at[j], send2.at[j], recv2.at[j], peer_x)

    def send_one(j):
        return remote(gs1.at[j], gr1.at[j], send1.at[j], recv1.at[j], peer_x)

    @pl.loop(0, n_chunk)
    def _(j):
        slot = lax.rem(j, 2)
        copies = loads(j)
        copies[0].wait()
        up = w1b[slot].astype(BF16)
        rows = acts_buf[...].reshape(-1, d_model)
        grad = gvec[...].reshape(-1, d_model)
        z = dot(rows, up)
        t, act = gelu_parts(z)
        hid = act.astype(BF16)
        copies[2].wait()
        gs2[j] += dot(hid, grad, TN)
        send_two(j).start()
        copies[1].wait()
        grad_hid = dot(grad, w2b[slot].astype(BF16), NT)
        grad_pre = (gelu_slope(z, t) * grad_hid).astype(BF16)
        copies[3].wait()
        gs1[j] += dot(rows, grad_pre, TN)
        send_one(j).start()

        @pl.when(is_last)
        def _():
            part[...] += dot(grad_pre, up, NT).reshape(part.shape)

        @pl.when(j + 2 < n_chunk)
        def _():
            for copy in loads(j + 2):
                copy.start()

    @pl.when(is_last)
    def _():
        swap_part.start()
        swap_part.wait()
        x_buf[:2] = (gvec[...].astype(F32) + (part[...] + got[:2])).astype(BF16)
        hand_over.start()

    @pl.when(is_first)
    def _():
        load_x.start()

    n_up = n_chunk // 2
    n_pair = 2 * n_up

    def fetch(p):
        base = lax.rem(p, 3) * 6

        @pl.when(p < n_up)
        def _():
            for q, ref in enumerate((w1, m1, v1)):
                for h in (0, 1):
                    cols = pl.ds(pl.multiple_of((2 * p + h) * width, width), width)
                    pltpu.make_async_copy(ref.at[:, cols], gs1.at[base + 2 * q + h], f_sem.at[base + 2 * q + h]).start()

        @pl.when(p >= n_up)
        def _():
            rows = pl.ds(pl.multiple_of(lax.rem(p - n_up, 2) * d_model, d_model), d_model)
            for q, ref in enumerate((w2, m2, v2)):
                for h in (0, 1):
                    cols = pl.ds(pl.multiple_of((2 * ((p - n_up) // 2) + h) * width, width), width)
                    pltpu.make_async_copy(ref.at[rows, cols], gs1.at[base + 2 * q + h], f_sem.at[base + 2 * q + h]).start()

    def arrive(p):
        base = lax.rem(p, 3) * 6
        for i in range(6):
            pltpu.make_async_copy(w1.at[:, :width], gs1.at[base + i], f_sem.at[base + i]).wait()

    def free_and_fetch(lo, hi, p):
        for i in range(lo, hi):
            send_one(i).wait_send()

        fetch(p)

    sq1[...] = jnp.zeros_like(sq1)
    sq2[...] = jnp.zeros_like(sq2)

    @pl.loop(0, n_chunk)
    def _(j):
        send_two(j).wait_recv()
        mean = (gs2[j] + gr2[j]) * 0.5
        gr2[j] = mean
        sq2[...] += jnp.sum((mean * mean).reshape(-1, 8, mean.shape[1]), axis=0)
        send_one(j).wait_recv()
        mean = (gs1[j] + gr1[j]) * 0.5
        gr1[j] = mean
        sq1[...] += jnp.sum((mean * mean).reshape(-1, 8, mean.shape[1]), axis=0)

        @pl.when(j == 10)
        def _():
            free_and_fetch(0, 6, 18 * s)

        @pl.when(j == 15)
        def _():
            free_and_fetch(6, 12, 1 + 18 * s)

    sq_out[...] = jnp.full(sq_out.shape, jnp.sum(sq1[...]) + jnp.sum(sq2[...]), F32)
    mine = 2 * m + s
    others = ((peer_y, 2 * (1 - m) + s), (peer_c, 2 * m + 1 - s), (peer_d, 2 * (1 - m) + 1 - s))
    shares = [remote(sq_out, sq_in.at[mine], sq_send.at[k], sq_recv.at[mine], peer) for k, (peer, _) in enumerate(others)]
    for copy in shares:
        copy.start()
    free_and_fetch(12, n_chunk, 2 + 15 * s)
    sq_in[mine] = sq_out[...]
    for peer, index in others:
        remote(sq_out, sq_in.at[index], sq_send.at[0], sq_recv.at[index], peer).wait_recv()
    total = (sq_in[0] + sq_in[1]) + (sq_in[2] + sq_in[3])
    clip[...] = jnp.minimum(1.0, max_norm[0] / (jnp.sqrt(total) + NORM_EPS))

    for j in range(n_chunk):
        send_two(j).wait_send()
    for copy in shares:
        copy.wait_send()

    @pl.when(is_last)
    def _():
        hand_over.wait_send()
        for p in (18, 19, 17):
            arrive(jnp.int32(p))

    @pl.when(is_first)
    def _():
        scale = clip[0, 0]
        step_rate = rate[0]
        group, half = x_buf.shape[:2]
        n_micro = group // 2
        third = group // 2
        wide = 2 * width
        n_block = d_model // wide

        def new_weights(p, means):
            base = lax.rem(p, 3) * 6
            parts = [adamw(scale, step_rate, gs1[base + h], gs1[base + 2 + h], gs1[base + 4 + h], means[h])[0].astype(BF16) for h in (0, 1)]
            return jnp.concatenate(parts, axis=1)

        def up_pair(p):
            new = new_weights(p, [gr1[2 * p], gr1[2 * p + 1]])
            act = gelu_parts(dot(x_buf[...].reshape(-1, d_model), new))[1].astype(BF16).astype(F32)
            cols = pl.ds(pl.multiple_of(lax.rem(p, n_block) * wide, wide), wide)
            gs2[pl.ds((p // n_block) * group, group), :, cols] = act.reshape(group, half, wide)

        def down_pair(p, upper):
            means = []
            for h in (0, 1):
                cols = pl.ds(pl.multiple_of((2 * ((p - n_up) // 2) + h) * width, width), width)
                means.append(gr2[upper * n_up:(upper + 1) * n_up, :, cols].reshape(d_model, width))
            new = new_weights(p, means)
            for lo in range(0, group, third):
                rows = gs2[upper * group + lo:upper * group + lo + third].reshape(-1, d_model).astype(BF16)
                res = dot(rows, new).reshape(third, half, wide)
                for g in range(third):
                    spot = slice(g * wide, (g + 1) * wide)
                    if upper:
                        part[lo // third, :, spot] += res[g]
                    else:
                        part[lo // third, :, spot] = res[g]

        def give_block(c):
            cols = pl.ds(pl.multiple_of(c * wide, wide), wide)
            for k in range(n_micro):
                even, odd = [part[g // third, :, g % third * wide:(g % third + 1) * wide] for g in (2 * k, 2 * k + 1)]
                gs2[2 * group + k, :, cols] = jnp.where(m == 0, even, odd)
                gs2[2 * group + n_micro + k, :, cols] = jnp.where(m == 0, odd, even)
            block_copy(c).start()

        def block_copy(c):
            cols = pl.ds(pl.multiple_of(c * wide, wide), wide)
            return remote(gs2.at[2 * group + n_micro:2 * group + 2 * n_micro, :, cols], got.at[:, :, cols], rs_send.at[c], rs_recv.at[c], peer_y)

        def ahead(p):
            @pl.when(p < n_pair)
            def _():
                fetch(p)

        load_x.wait()

        @pl.loop(0, n_up)
        def _(p):
            arrive(p)
            up_pair(p)
            ahead(p + 3)

        @pl.loop(0, n_block)
        def _(c):
            for upper in (0, 1):
                p = n_up + 2 * c + upper
                arrive(p)
                down_pair(p, upper)
                ahead(p + 3)
            give_block(c)

        for c in range(n_block):
            block_copy(c).wait_recv()
            cols = slice(c * wide, (c + 1) * wide)
            for k in range(n_micro):
                rows = x_buf[2 * k + m, :, cols].astype(F32)
                x_buf[k, :, cols] = (rows + (gs2[2 * group + k, :, cols] + got[k, :, cols])).astype(BF16)
        store = pltpu.make_async_copy(x_buf.at[:n_micro], act_half, row_sem)
        store.start()
        for c in range(n_block):
            block_copy(c).wait_send()
        store.wait()


def update_kernel(clip, rate, w1, m1, v1, gb1, w2, m2, v2, gb2, held, nw1, nm1, nv1, nw2, nm2, nv2, keep1, keep2, held_out,
                  ring, in_sem, out_sem, held_sem):
    _, deep, wide = gb1.shape
    n_slot, tall, span = ring.shape[1:]
    block = deep // tall
    per_row = w1.shape[2] // span
    n_up = per_row * (deep // tall)
    n_down = w2.shape[1] // tall
    last = n_up + n_down
    scale = clip[0, 0]
    step_rate = rate[0]
    kinds = ((0, n_up, span), (n_up, n_up + n_down // 2, 8 * wide), (n_up + n_down // 2, last, 6 * wide))

    def copies(i, kind, fetch):
        slot = lax.rem(i, n_slot)
        sem = in_sem if fetch else out_sem
        cols = kinds[kind][2]
        if kind == 0:
            refs = (w1, m1, v1) if fetch else (nw1, nm1, nv1)
            where = (0, pl.ds(pl.multiple_of(i // per_row * tall, tall), tall), pl.ds(pl.multiple_of(lax.rem(i, per_row) * span, span), span))
        else:
            refs = (w2, m2, v2) if fetch else (nw2, nm2, nv2)
            where = (0, pl.ds(pl.multiple_of((i - n_up) * tall, tall), tall), slice(0, cols))
        out = []
        for k, ref in enumerate(refs):
            pair = (ref.at[where], ring.at[k, slot, :, :cols])
            out.append(pltpu.make_async_copy(*(pair if fetch else pair[::-1]), sem.at[k, slot]))
        return out

    def each(i, act):
        if isinstance(i, int):
            kind = [n for n, (lo, hi, _) in enumerate(kinds) if lo <= i < hi][0]
            act(jnp.int32(i), kind)
            return
        for kind, (lo, hi, _) in enumerate(kinds):
            @pl.when((i >= lo) & (i < hi))
            def _():
                act(i, kind)

    def start(i, fetch):
        def act(i, kind):
            for copy in copies(i, kind, fetch):
                copy.start()

        each(i, act)

    def finish(i, fetch):
        def act(i, kind):
            for copy in copies(i, kind, fetch):
                copy.wait()

        each(i, act)

    for i in range(AHEAD):
        start(i, True)

    near = [(place, h) for place in range(3) for h in (0, 1)]

    def held_copies(place, h):
        col, upper = {2: (6, 1), 0: (8, 0), 1: (8, 1)}[place]
        rows, cols = slice(upper * deep, (upper + 1) * deep), slice((col + h) * wide, (col + h + 1) * wide)
        return upper, cols, [pltpu.make_async_copy(held_out.at[6 * place + 2 * k + h], ref.at[0, rows, cols], held_sem.at[6 * place + 2 * k + h])
                             for k, ref in enumerate((nw2, nm2, nv2))]

    for spot, h in near:
        upper, cols, moves = held_copies(spot, h)
        rows = slice(upper * block, (upper + 1) * block)
        base = 6 * spot + h
        new, mom, sec = adamw(scale, step_rate, held[base], held[base + 2], held[base + 4], gb2[rows, :, cols].reshape(deep, wide))
        held_out[base] = new
        held_out[base + 2] = mom
        held_out[base + 4] = sec
        keep2[rows, :, cols] = new.reshape(block, -1, wide)
        for copy in moves:
            copy.start()

    def step(slot, cols, mean):
        new, mom, sec = adamw(scale, step_rate, ring[0, slot, :, cols], ring[1, slot, :, cols], ring[2, slot, :, cols], mean)
        ring[0, slot, :, cols] = new
        ring[1, slot, :, cols] = mom
        ring[2, slot, :, cols] = sec
        return new

    def compute(i, kind):
        slot = lax.rem(i, n_slot)
        if kind == 0:
            rows = pl.ds(pl.multiple_of(i // per_row * tall, tall), tall)
            for t in range(span // wide):
                col = lax.rem(i, per_row) * (span // wide) + t
                keep1[col, rows] = step(slot, slice(t * wide, (t + 1) * wide), gb1[col, rows])
        else:
            cols = slice(0, kinds[kind][2])
            keep2[i - n_up, :, cols] = step(slot, cols, gb2[i - n_up, :, cols])

    @pl.loop(0, last)
    def _(i):
        finish(i, True)
        each(i, compute)
        start(i, False)

        @pl.when(i + AHEAD < last)
        def _():
            @pl.when(i + AHEAD - n_slot >= 0)
            def _():
                finish(i + AHEAD - n_slot, False)

            start(i + AHEAD, True)

    for i in range(last - n_slot, last):
        finish(i, False)
    for spot, h in near:
        for copy in held_copies(spot, h)[2]:
            copy.wait()


def forward_kernel(from_core, from_diag, new1, new2, y,
                   hid, act, own_half, peer_half, part, part_in,
                   in_sem, p_send, p_recv, y_send, y_recv, g_send, g_recv, f_send, f_recv, ready):
    m, d, s = positions()
    n_micro, half, d_model = own_half.shape
    width = 2 * new1.shape[2]
    n_chunk, n_block = new1.shape[0] // 2, d_model // width
    peer_y = (1 - m, d, s)
    peer_c = (m, d, 1 - s)
    barrier = pltpu.get_barrier_semaphore()
    mine = pl.ds(pl.multiple_of(m * half, half), half)
    theirs = pl.ds(pl.multiple_of((1 - m) * half, half), half)
    rows_in = (pltpu.make_async_copy(from_core, act.at[:, mine, :], in_sem.at[0]),
               pltpu.make_async_copy(from_diag, act.at[:, theirs, :], in_sem.at[1]))

    @pl.when(s == 1)
    def _():
        for copy in rows_in:
            copy.start()
        pl.semaphore_signal(barrier, inc=1, device_id=peer_y, device_id_type=MESH)
        pl.semaphore_signal(barrier, inc=1, device_id=peer_c, device_id_type=MESH)

    pl.semaphore_wait(barrier, 1)

    @pl.when(s == 0)
    def _():
        pl.semaphore_signal(ready, inc=1, device_id=peer_c, device_id_type=MESH)

    def span(c):
        return pl.ds(pl.multiple_of(c * width, width), width)

    def send_part(k, c):
        return remote(part.at[k, theirs, span(c)], part_in.at[k, :, span(c)], p_send.at[k, c], p_recv.at[k, c], peer_y)

    def swap_y(k, c):
        return remote(own_half.at[k, :, span(c)], peer_half.at[k, :, span(c)], y_send.at[k, c], y_recv.at[k, c], peer_y)

    def give_own(k):
        return remote(own_half.at[k], y.at[k, mine, :], g_send.at[k], g_recv.at[k], peer_c)

    def pass_on(k):
        return remote(peer_half.at[k], y.at[k, theirs, :], f_send.at[k], f_recv.at[k], peer_c)

    @pl.when(s == 0)
    def _():
        for k in range(n_micro):
            give_own(k).wait_recv()
            pass_on(k).wait_recv()

    @pl.when(s == 1)
    def _():
        for copy in rows_in:
            copy.wait()

        for k in range(n_micro):
            @pl.loop(0, n_chunk)
            def _(j):
                up = jnp.concatenate([new1[2 * j].astype(BF16), new1[2 * j + 1].astype(BF16)], axis=1)
                hid[:, span(j)] = gelu_parts(dot(act[k], up))[1].astype(BF16)

            @pl.loop(0, n_block)
            def _(c):
                down = new2[:, :, span(c)].reshape(-1, width).astype(BF16)
                part[k, :, span(c)] = dot(hid[...], down)
                send_part(k, c).start()

        for k in range(n_micro):
            @pl.loop(0, n_block)
            def _(c):
                send_part(k, c).wait_recv()
                out = act[k, mine, span(c)].astype(F32) + (part[k, mine, span(c)] + part_in[k, :, span(c)])
                own_half[k, :, span(c)] = out.astype(BF16)
                swap_y(k, c).start()

        pl.semaphore_wait(ready, 1)
        for k in range(n_micro):
            give_own(k).start()
            y[k, mine, :] = own_half[k]
        for k in range(n_micro):
            @pl.loop(0, n_block)
            def _(c):
                swap_y(k, c).wait_recv()

            pass_on(k).start()
            y[k, theirs, :] = peer_half[k]
        for k in range(n_micro):
            @pl.loop(0, n_block)
            def _(c):
                send_part(k, c).wait_send()
                swap_y(k, c).wait_send()

            give_own(k).wait_send()
            pass_on(k).wait_send()


def solution(mesh):
    up_spec = P('stage', None, 'model')
    down_spec = P('stage', 'model', None)
    row_spec = P(None, 'data', None)
    in_specs = (up_spec, down_spec, up_spec, down_spec, up_spec, down_spec, P('data', 'stage', None, 'model'), P('data', 'stage', 'model', None), P('stage', 'data', None), P('data', None), row_spec, P(None), P(None))
    out_specs = (up_spec, down_spec, up_spec, down_spec, up_spec, down_spec, row_spec)

    def device_step(w_up, w_down, m_up, m_down, v_up, v_down, g_up, g_down, acts_last, grad_out, x_next, learn_rate, max_norm):
        d_model, ff = w_up.shape[1:]
        rows = grad_out.shape[0]
        n_micro = x_next.shape[0]
        width = CHUNK
        n_chunk = ff // width
        half = rows // 2
        hbm = pl.BlockSpec(memory_space=pl.ANY)
        vmem = pl.BlockSpec(memory_space=pltpu.VMEM)
        smem = pl.BlockSpec(memory_space=pltpu.SMEM)
        dma = pltpu.SemaphoreType.DMA
        resident = 4 * 3 * d_model * ff
        n_block = d_model // (2 * width)

        mean_up, mean_down, held, clip, act_half = pl.pallas_call(
            functools.partial(grad_kernel, n_chunk, width),
            out_shape=(pltpu.VMEM((n_chunk, d_model, width), F32),
                       pltpu.VMEM((n_chunk, width, d_model), F32),
                       pltpu.VMEM((n_chunk, d_model, width), F32),
                       jax.ShapeDtypeStruct((8, 128), F32),
                       jax.ShapeDtypeStruct((n_micro, half, d_model), BF16)),
            in_specs=[hbm] * 11 + [smem, smem],
            out_specs=(vmem, vmem, vmem, vmem, hbm),
            scratch_shapes=[
                pltpu.VMEM((n_chunk, width, d_model), F32),
                pltpu.VMEM((2, d_model, width), F32),
                pltpu.VMEM((2, width, d_model), F32),
                pltpu.VMEM((2, half, d_model), F32),
                pltpu.VMEM((n_micro, half, d_model), F32),
                pltpu.VMEM((2 * n_micro, half, d_model), BF16),
                pltpu.VMEM((8, width), F32),
                pltpu.VMEM((8, d_model), F32),
                pltpu.VMEM((8, 128), F32),
                pltpu.VMEM((4, 8, 128), F32),
                dma((2, 2)), dma((2, 2)),
                dma((n_chunk,)), dma((n_chunk,)), dma((n_chunk,)), dma((n_chunk,)),
                dma((2,)), dma((2,)), dma((3,)), dma((4,)),
                dma(()), dma(()), dma((18,)), dma((n_block,)), dma((n_block,)),
            ],
            compiler_params=pltpu.CompilerParams(collective_id=0, has_side_effects=True, vmem_limit_bytes=VMEM_MAX - resident - SPARE),
            name="grad_exchange",
        )(w_up[0], w_down[0], g_up[0, 0], g_down[0, 0], m_up[0], v_up[0], m_down[0], v_down[0], acts_last.reshape(2, half, d_model), grad_out.reshape(2, half, d_model), x_next.reshape(2 * n_micro, half, d_model), max_norm, learn_rate)

        from_diag = lax.ppermute(act_half, ('model', 'stage'), [(0, 3), (2, 1)])
        from_core = lax.ppermute(act_half, ('model', 'stage'), [(0, 1), (2, 3)])

        def stay(array):
            return pltpu.with_memory_space_constraint(array, pltpu.VMEM)

        up_out = jax.ShapeDtypeStruct(w_up.shape, F32)
        down_out = jax.ShapeDtypeStruct(w_down.shape, F32)
        nw1, nm1, nv1, nw2, nm2, nv2, new1, new2, _ = pl.pallas_call(
            update_kernel,
            out_shape=(up_out, up_out, up_out, down_out, down_out, down_out,
                       pltpu.VMEM(mean_up.shape, F32), pltpu.VMEM(mean_down.shape, F32), pltpu.VMEM(held.shape, F32)),
            in_specs=[smem, smem, hbm, hbm, hbm, vmem, hbm, hbm, hbm, vmem, vmem],
            out_specs=(hbm,) * 6 + (vmem, vmem, vmem),
            input_output_aliases={5: 6, 9: 7, 10: 8},
            scratch_shapes=[pltpu.VMEM((3, SLOTS, width, d_model), F32), dma((3, SLOTS)), dma((3, SLOTS)), dma((18,))],
            compiler_params=pltpu.CompilerParams(vmem_limit_bytes=VMEM_MAX - resident - SPARE),
            cost_estimate=pl.CostEstimate(flops=2000 * d_model * ff, bytes_accessed=48 * d_model * ff, transcendentals=4 * d_model * ff),
            name="update",
        )(clip, learn_rate, w_up, m_up, v_up, stay(mean_up), w_down, m_down, v_down, stay(mean_down), stay(held))

        y_next = pl.pallas_call(
            forward_kernel,
            out_shape=pltpu.VMEM(x_next.shape, BF16),
            in_specs=[hbm, hbm, vmem, vmem],
            out_specs=vmem,
            scratch_shapes=[
                pltpu.VMEM((rows, ff), BF16),
                pltpu.VMEM((n_micro, rows, d_model), BF16),
                pltpu.VMEM((n_micro, half, d_model), BF16),
                pltpu.VMEM((n_micro, half, d_model), BF16),
                pltpu.VMEM((n_micro, rows, d_model), F32),
                pltpu.VMEM((n_micro, half, d_model), F32),
                dma((2,)), dma((n_micro, n_block)), dma((n_micro, n_block)), dma((n_micro, n_block)), dma((n_micro, n_block)),
                dma((n_micro,)), dma((n_micro,)), dma((n_micro,)), dma((n_micro,)),
                pltpu.SemaphoreType.REGULAR,
            ],
            compiler_params=pltpu.CompilerParams(collective_id=1, has_side_effects=True, vmem_limit_bytes=VMEM_MAX - resident - SPARE),
            name="forward_exchange",
        )(from_core, from_diag, stay(new1), stay(new2))
        return nw1, nw2, nm1, nm2, nv1, nv2, y_next

    return jax.shard_map(device_step, mesh=mesh, in_specs=in_specs, out_specs=out_specs, check_vma=False)
```

```python
import functools

import jax
import jax.numpy as jnp
from jax import lax
from jax.experimental import pallas as pl
from jax.experimental.pallas import tpu as pltpu
from jax.sharding import PartitionSpec as P


ADAM_STEP = 10
BETA_ONE = 0.9
BETA_TWO = 0.95
ADAM_EPS = 1e-8
WEIGHT_DECAY = 0.1
NORM_EPS = 1e-6
ONE_CORR = 1.0 - BETA_ONE ** ADAM_STEP
TWO_CORR = 1.0 - BETA_TWO ** ADAM_STEP
ROOT_EPS = ADAM_EPS * TWO_CORR ** 0.5
ROOT_GAIN = TWO_CORR ** 0.5 / ONE_CORR
TINY = 1.1754944e-38
HUGE = 3.4028235e38
GELU_A = 0.7978845608028654
GELU_B = 0.044715
NT = (((1,), (1,)), ((), ()))
TN = (((0,), (0,)), ((), ()))
MESH = pl.DeviceIdType.MESH
VMEM_MAX = 67_043_328
CHUNK = 128
SLOTS = 8
AHEAD = 5
SPARE = 5 << 19
F32 = jnp.float32
BF16 = jnp.bfloat16


def gelu_parts(z):
    t = jnp.tanh(GELU_A * (z + GELU_B * (z * z * z)))
    return t, z * (0.5 * (1.0 + t))


def gelu_slope(z, t):
    return 0.5 * (1.0 + t) + 0.5 * z * (1.0 - t * t) * (GELU_A * (1.0 + 3.0 * GELU_B * z * z))


def dot(a, b, dims=(((1,), (0,)), ((), ()))):
    return lax.dot_general(a, b, dims, preferred_element_type=F32)


def positions():
    return lax.axis_index("model"), lax.axis_index("data"), lax.axis_index("stage")


def entry_barrier(peers):
    barrier = pltpu.get_barrier_semaphore()
    for peer in peers:
        pl.semaphore_signal(barrier, inc=1, device_id=peer, device_id_type=MESH)
    pl.semaphore_wait(barrier, len(peers))


def remote(src, dst, send, recv, peer):
    return pltpu.make_async_remote_copy(src_ref=src, dst_ref=dst, send_sem=send, recv_sem=recv, device_id=peer, device_id_type=MESH)


def adamw(scale, rate, w, mom, sec, mean):
    grad = scale * mean
    mom_new = BETA_ONE * mom + (1.0 - BETA_ONE) * grad
    sec_new = BETA_TWO * sec + ((1.0 - BETA_TWO) * grad) * grad
    root = sec_new * lax.rsqrt(jnp.minimum(sec_new + TINY, HUGE))
    w_new = w * (1.0 - rate * WEIGHT_DECAY) - (rate * ROOT_GAIN) * (mom_new / (root + ROOT_EPS))
    return w_new, mom_new, sec_new


def grad_kernel(n_chunk, width, w1, w2, g1, g2, m1, v1, m2, v2, acts, dy, x, max_norm, rate,
                gr1, gr2, gs1, clip, act_half,
                gs2, w1b, w2b, part, got, x_buf, sq1, sq2, sq_out, sq_in,
                w_sem, g_sem, send1, send2, recv1, recv2, part_sem, gvec_sem, sq_send, sq_recv,
                row_sem, act_sem, f_sem, rs_send, rs_recv, out_sem):
    m, d, s = positions()
    peer_x = (m, 1 - d, s)
    peer_y = (1 - m, d, s)
    peer_c = (m, d, 1 - s)
    peer_d = (1 - m, d, 1 - s)
    d_model = w1.shape[0]
    is_last = s == 1
    is_first = s == 0

    def loads(j):
        slot = lax.rem(j, 2)
        cols = pl.ds(pl.multiple_of(j * width, width), width)
        return (pltpu.make_async_copy(w1.at[:, cols], w1b.at[slot], w_sem.at[0, slot]),
                pltpu.make_async_copy(w2.at[cols, :], w2b.at[slot], w_sem.at[1, slot]),
                pltpu.make_async_copy(g2.at[cols, :], gs2.at[j], g_sem.at[0, slot]),
                pltpu.make_async_copy(g1.at[:, cols], gs1.at[j], g_sem.at[1, slot]))

    acts_buf, gvec = x_buf.at[2:4], x_buf.at[4:6]
    load_acts = pltpu.make_async_copy(acts, acts_buf, act_sem)
    load_dy = pltpu.make_async_copy(dy, gvec, row_sem)
    load_x = pltpu.make_async_copy(x, x_buf, row_sem)

    load_acts.start()

    @pl.when(is_last)
    def _():
        load_dy.start()

    for copy in loads(0):
        copy.start()
    entry_barrier((peer_x, peer_y, peer_c, peer_d))
    for copy in loads(1):
        copy.start()

    hand_over = remote(x_buf.at[:2], gvec, gvec_sem.at[0], gvec_sem.at[1], peer_c)
    swap_part = remote(part, got.at[:2], part_sem.at[0], part_sem.at[1], peer_y)

    @pl.when(is_last)
    def _():
        part[...] = jnp.zeros_like(part)
        load_dy.wait()

    @pl.when(is_first)
    def _():
        hand_over.wait_recv()

    load_acts.wait()

    def send_two(j):
        return remote(gs2.at[j], gr2.at[j], send2.at[j], recv2.at[j], peer_x)

    def send_one(j):
        return remote(gs1.at[j], gr1.at[j], send1.at[j], recv1.at[j], peer_x)

    @pl.loop(0, n_chunk)
    def _(j):
        slot = lax.rem(j, 2)
        copies = loads(j)
        copies[0].wait()
        up = w1b[slot].astype(BF16)
        rows = acts_buf[...].reshape(-1, d_model)
        grad = gvec[...].reshape(-1, d_model)
        z = dot(rows, up)
        t, act = gelu_parts(z)
        hid = act.astype(BF16)
        copies[2].wait()
        gs2[j] += dot(hid, grad, TN)
        send_two(j).start()
        copies[1].wait()
        grad_hid = dot(grad, w2b[slot].astype(BF16), NT)
        grad_pre = (gelu_slope(z, t) * grad_hid).astype(BF16)
        copies[3].wait()
        gs1[j] += dot(rows, grad_pre, TN)
        send_one(j).start()

        @pl.when(is_last)
        def _():
            part[...] += dot(grad_pre, up, NT).reshape(part.shape)

        @pl.when(j + 2 < n_chunk)
        def _():
            for copy in loads(j + 2):
                copy.start()

    @pl.when(is_last)
    def _():
        swap_part.start()
        swap_part.wait()
        x_buf[:2] = (gvec[...].astype(F32) + (part[...] + got[:2])).astype(BF16)
        hand_over.start()

    @pl.when(is_first)
    def _():
        load_x.start()

    n_up = n_chunk // 2
    n_pair = 2 * n_up

    def fetch(p):
        base = lax.rem(p, 3) * 6

        @pl.when(p < n_up)
        def _():
            for q, ref in enumerate((w1, m1, v1)):
                for h in (0, 1):
                    cols = pl.ds(pl.multiple_of((2 * p + h) * width, width), width)
                    pltpu.make_async_copy(ref.at[:, cols], gs1.at[base + 2 * q + h], f_sem.at[base + 2 * q + h]).start()

        @pl.when(p >= n_up)
        def _():
            cols = pl.ds(pl.multiple_of((p - n_up) * width, width), width)
            for q, ref in enumerate((w2, m2, v2)):
                for h in (0, 1):
                    rows = pl.ds(h * d_model, d_model)
                    pltpu.make_async_copy(ref.at[rows, cols], gs1.at[base + 2 * q + h], f_sem.at[base + 2 * q + h]).start()

    def arrive(p):
        base = lax.rem(p, 3) * 6
        for i in range(6):
            pltpu.make_async_copy(w1.at[:, :width], gs1.at[base + i], f_sem.at[base + i]).wait()

    def free_and_fetch(lo, hi, p):
        for i in range(lo, hi):
            send_one(i).wait_send()

        fetch(p)

    sq1[...] = jnp.zeros_like(sq1)
    sq2[...] = jnp.zeros_like(sq2)

    @pl.loop(0, n_chunk)
    def _(j):
        send_two(j).wait_recv()
        mean = (gs2[j] + gr2[j]) * 0.5
        gr2[j] = mean
        sq2[...] += jnp.sum((mean * mean).reshape(-1, 8, mean.shape[1]), axis=0)
        send_one(j).wait_recv()
        mean = (gs1[j] + gr1[j]) * 0.5
        gr1[j] = mean
        sq1[...] += jnp.sum((mean * mean).reshape(-1, 8, mean.shape[1]), axis=0)

        @pl.when(j == 10)
        def _():
            free_and_fetch(0, 6, 18 * s)

        @pl.when(j == 15)
        def _():
            free_and_fetch(6, 12, 1 + 18 * s)

    sq_out[...] = jnp.full(sq_out.shape, jnp.sum(sq1[...]) + jnp.sum(sq2[...]), F32)
    mine = 2 * m + s
    others = ((peer_y, 2 * (1 - m) + s), (peer_c, 2 * m + 1 - s), (peer_d, 2 * (1 - m) + 1 - s))
    shares = [remote(sq_out, sq_in.at[mine], sq_send.at[k], sq_recv.at[mine], peer) for k, (peer, _) in enumerate(others)]
    for copy in shares:
        copy.start()
    free_and_fetch(12, n_chunk, 2 + 15 * s)
    sq_in[mine] = sq_out[...]
    for peer, index in others:
        remote(sq_out, sq_in.at[index], sq_send.at[0], sq_recv.at[index], peer).wait_recv()
    total = (sq_in[0] + sq_in[1]) + (sq_in[2] + sq_in[3])
    clip[...] = jnp.minimum(1.0, max_norm[0] / (jnp.sqrt(total) + NORM_EPS))

    for j in range(n_chunk):
        send_two(j).wait_send()
    for copy in shares:
        copy.wait_send()

    @pl.when(is_last)
    def _():
        hand_over.wait_send()
        for p in (18, 19, 17):
            arrive(jnp.int32(p))

    @pl.when(is_first)
    def _():
        scale = clip[0, 0]
        step_rate = rate[0]
        group, half = x_buf.shape[:2]
        n_micro = group // 2
        third = group // 2
        wide = 2 * width
        n_block = d_model // width

        def new_weights(p, means):
            base = lax.rem(p, 3) * 6
            return [adamw(scale, step_rate, gs1[base + h], gs1[base + 2 + h], gs1[base + 4 + h], means[h])[0].astype(BF16) for h in (0, 1)]

        def up_pair(p):
            new = jnp.concatenate(new_weights(p, [gr1[2 * p], gr1[2 * p + 1]]), axis=1)
            act = gelu_parts(dot(x_buf[...].reshape(-1, d_model), new))[1].astype(BF16).astype(F32)
            cols = pl.ds(pl.multiple_of(lax.rem(p, n_up // 2) * wide, wide), wide)
            gs2[pl.ds((p // (n_up // 2)) * group, group), :, cols] = act.reshape(group, half, wide)

        def block(c):
            return pl.ds(pl.multiple_of(c * width, width), width)

        def down_pair(c):
            new = new_weights(n_up + c, [gr2[h * n_up:(h + 1) * n_up, :, block(c)].reshape(d_model, width) for h in (0, 1)])
            for lo in range(0, group, third):
                low, high = [dot(gs2[h * group + lo:h * group + lo + third].reshape(-1, d_model).astype(BF16), new[h]) for h in (0, 1)]
                res = (low + high).reshape(third, half, width)
                for g in range(lo, lo + third):
                    other = m if g % 2 == 0 else 1 - m
                    gs2[2 * group + g // 2 + n_micro * other, :, block(c)] = res[g - lo]
            block_copy(c).start()

        def block_copy(c):
            return remote(gs2.at[2 * group + n_micro:2 * group + 2 * n_micro, :, block(c)], got.at[:, :, block(c)], rs_send.at[c], rs_recv.at[c], peer_y)

        def ahead(p):
            @pl.when(p < n_pair)
            def _():
                fetch(p)

        load_x.wait()

        @pl.loop(0, n_up)
        def _(p):
            arrive(p)
            up_pair(p)
            ahead(p + 3)

        @pl.loop(0, n_block)
        def _(c):
            arrive(n_up + c)
            down_pair(c)
            ahead(n_up + c + 3)

        def store(c):
            return pltpu.make_async_copy(x_buf.at[:n_micro, :, block(c)], act_half.at[:, :, block(c)], out_sem.at[c])

        @pl.loop(0, n_block)
        def _(c):
            block_copy(c).wait_recv()
            for k in range(n_micro):
                rows = x_buf[2 * k + m, :, block(c)].astype(F32)
                x_buf[k, :, block(c)] = (rows + (gs2[2 * group + k, :, block(c)] + got[k, :, block(c)])).astype(BF16)
            store(c).start()

        @pl.loop(0, n_block)
        def _(c):
            block_copy(c).wait_send()
            store(c).wait()


def update_kernel(clip, rate, w1, m1, v1, gb1, w2, m2, v2, gb2, held, nw1, nm1, nv1, nw2, nm2, nv2, keep1, keep2, held_out,
                  ring, in_sem, out_sem, held_sem):
    _, deep, wide = gb1.shape
    n_slot, tall, span = ring.shape[1:]
    block = deep // tall
    per_row = w1.shape[2] // span
    n_up = per_row * (deep // tall)
    n_down = w2.shape[1] // tall
    last = n_up + n_down
    scale = clip[0, 0]
    step_rate = rate[0]
    n_held = 3
    first_held = span // wide - n_held
    kinds = ((0, n_up, span), (n_up, last, first_held * wide))

    def copies(i, kind, fetch):
        slot = lax.rem(i, n_slot)
        sem = in_sem if fetch else out_sem
        cols = kinds[kind][2]
        if kind == 0:
            refs = (w1, m1, v1) if fetch else (nw1, nm1, nv1)
            where = (0, pl.ds(pl.multiple_of(i // per_row * tall, tall), tall), pl.ds(pl.multiple_of(lax.rem(i, per_row) * span, span), span))
        else:
            refs = (w2, m2, v2) if fetch else (nw2, nm2, nv2)
            where = (0, pl.ds(pl.multiple_of((i - n_up) * tall, tall), tall), slice(0, cols))
        out = []
        for k, ref in enumerate(refs):
            pair = (ref.at[where], ring.at[k, slot, :, :cols])
            out.append(pltpu.make_async_copy(*(pair if fetch else pair[::-1]), sem.at[k, slot]))
        return out

    def each(i, act):
        if isinstance(i, int):
            kind = [n for n, (lo, hi, _) in enumerate(kinds) if lo <= i < hi][0]
            act(jnp.int32(i), kind)
            return
        for kind, (lo, hi, _) in enumerate(kinds):
            @pl.when((i >= lo) & (i < hi))
            def _():
                act(i, kind)

    def start(i, fetch):
        def act(i, kind):
            for copy in copies(i, kind, fetch):
                copy.start()

        each(i, act)

    def finish(i, fetch):
        def act(i, kind):
            for copy in copies(i, kind, fetch):
                copy.wait()

        each(i, act)

    for i in range(AHEAD):
        start(i, True)

    near = [(spot, h) for spot in range(n_held) for h in (0, 1)]

    def held_copies(spot, h):
        col = first_held + (spot + 1) % n_held
        rows, cols = slice(h * deep, (h + 1) * deep), slice(col * wide, (col + 1) * wide)
        return cols, [pltpu.make_async_copy(held_out.at[6 * spot + 2 * k + h], ref.at[0, rows, cols], held_sem.at[6 * spot + 2 * k + h])
                      for k, ref in enumerate((nw2, nm2, nv2))]

    for spot, h in near:
        cols, moves = held_copies(spot, h)
        rows = slice(h * block, (h + 1) * block)
        base = 6 * spot + h
        new, mom, sec = adamw(scale, step_rate, held[base], held[base + 2], held[base + 4], gb2[rows, :, cols].reshape(deep, wide))
        held_out[base] = new
        held_out[base + 2] = mom
        held_out[base + 4] = sec
        keep2[rows, :, cols] = new.reshape(block, -1, wide)
        for copy in moves:
            copy.start()

    def step(slot, cols, mean):
        new, mom, sec = adamw(scale, step_rate, ring[0, slot, :, cols], ring[1, slot, :, cols], ring[2, slot, :, cols], mean)
        ring[0, slot, :, cols] = new
        ring[1, slot, :, cols] = mom
        ring[2, slot, :, cols] = sec
        return new

    def compute(i, kind):
        slot = lax.rem(i, n_slot)
        if kind == 0:
            rows = pl.ds(pl.multiple_of(i // per_row * tall, tall), tall)
            for t in range(span // wide):
                col = lax.rem(i, per_row) * (span // wide) + t
                keep1[col, rows] = step(slot, slice(t * wide, (t + 1) * wide), gb1[col, rows])
        else:
            cols = slice(0, kinds[kind][2])
            keep2[i - n_up, :, cols] = step(slot, cols, gb2[i - n_up, :, cols])

    @pl.loop(0, last)
    def _(i):
        finish(i, True)
        each(i, compute)
        start(i, False)

        @pl.when(i + AHEAD < last)
        def _():
            @pl.when(i + AHEAD - n_slot >= 0)
            def _():
                finish(i + AHEAD - n_slot, False)

            start(i + AHEAD, True)

    for i in range(last - n_slot, last):
        finish(i, False)
    for spot, h in near:
        for copy in held_copies(spot, h)[1]:
            copy.wait()


def forward_kernel(from_core, from_diag, new1, new2, y,
                   hid, act, own_half, peer_half, part, part_in,
                   in_sem, p_send, p_recv, y_send, y_recv, g_send, g_recv, f_send, f_recv, ready):
    m, d, s = positions()
    n_micro, half, d_model = own_half.shape
    width = 2 * new1.shape[2]
    n_chunk, n_block = new1.shape[0] // 2, d_model // width
    peer_y = (1 - m, d, s)
    peer_c = (m, d, 1 - s)
    barrier = pltpu.get_barrier_semaphore()
    mine = pl.ds(pl.multiple_of(m * half, half), half)
    theirs = pl.ds(pl.multiple_of((1 - m) * half, half), half)
    rows_in = (pltpu.make_async_copy(from_core, act.at[:, mine, :], in_sem.at[0]),
               pltpu.make_async_copy(from_diag, act.at[:, theirs, :], in_sem.at[1]))

    @pl.when(s == 1)
    def _():
        for copy in rows_in:
            copy.start()
        pl.semaphore_signal(barrier, inc=1, device_id=peer_y, device_id_type=MESH)
        pl.semaphore_signal(barrier, inc=1, device_id=peer_c, device_id_type=MESH)

    pl.semaphore_wait(barrier, 1)

    @pl.when(s == 0)
    def _():
        pl.semaphore_signal(ready, inc=1, device_id=peer_c, device_id_type=MESH)

    def span(c):
        return pl.ds(pl.multiple_of(c * width, width), width)

    def send_part(k, c):
        return remote(part.at[k, theirs, span(c)], part_in.at[k, :, span(c)], p_send.at[k, c], p_recv.at[k, c], peer_y)

    def swap_y(k, c):
        return remote(own_half.at[k, :, span(c)], peer_half.at[k, :, span(c)], y_send.at[k, c], y_recv.at[k, c], peer_y)

    def give_own(k):
        return remote(own_half.at[k], y.at[k, mine, :], g_send.at[k], g_recv.at[k], peer_c)

    def pass_on(k):
        return remote(peer_half.at[k], y.at[k, theirs, :], f_send.at[k], f_recv.at[k], peer_c)

    @pl.when(s == 0)
    def _():
        for k in range(n_micro):
            give_own(k).wait_recv()
            pass_on(k).wait_recv()

    @pl.when(s == 1)
    def _():
        for copy in rows_in:
            copy.wait()

        for k in range(n_micro):
            @pl.loop(0, n_chunk)
            def _(j):
                up = jnp.concatenate([new1[2 * j].astype(BF16), new1[2 * j + 1].astype(BF16)], axis=1)
                hid[:, span(j)] = gelu_parts(dot(act[k], up))[1].astype(BF16)

            @pl.loop(0, n_block)
            def _(c):
                down = new2[:, :, span(c)].reshape(-1, width).astype(BF16)
                part[k, :, span(c)] = dot(hid[...], down)
                send_part(k, c).start()

        for k in range(n_micro):
            @pl.loop(0, n_block)
            def _(c):
                send_part(k, c).wait_recv()
                out = act[k, mine, span(c)].astype(F32) + (part[k, mine, span(c)] + part_in[k, :, span(c)])
                own_half[k, :, span(c)] = out.astype(BF16)
                swap_y(k, c).start()

        pl.semaphore_wait(ready, 1)
        for k in range(n_micro):
            give_own(k).start()
            y[k, mine, :] = own_half[k]
        for k in range(n_micro):
            @pl.loop(0, n_block)
            def _(c):
                swap_y(k, c).wait_recv()

            pass_on(k).start()
            y[k, theirs, :] = peer_half[k]
        for k in range(n_micro):
            @pl.loop(0, n_block)
            def _(c):
                send_part(k, c).wait_send()
                swap_y(k, c).wait_send()

            give_own(k).wait_send()
            pass_on(k).wait_send()


def solution(mesh):
    up_spec = P('stage', None, 'model')
    down_spec = P('stage', 'model', None)
    row_spec = P(None, 'data', None)
    in_specs = (up_spec, down_spec, up_spec, down_spec, up_spec, down_spec, P('data', 'stage', None, 'model'), P('data', 'stage', 'model', None), P('stage', 'data', None), P('data', None), row_spec, P(None), P(None))
    out_specs = (up_spec, down_spec, up_spec, down_spec, up_spec, down_spec, row_spec)

    def device_step(w_up, w_down, m_up, m_down, v_up, v_down, g_up, g_down, acts_last, grad_out, x_next, learn_rate, max_norm):
        d_model, ff = w_up.shape[1:]
        rows = grad_out.shape[0]
        n_micro = x_next.shape[0]
        width = CHUNK
        n_chunk = ff // width
        half = rows // 2
        hbm = pl.BlockSpec(memory_space=pl.ANY)
        vmem = pl.BlockSpec(memory_space=pltpu.VMEM)
        smem = pl.BlockSpec(memory_space=pltpu.SMEM)
        dma = pltpu.SemaphoreType.DMA
        resident = 4 * 3 * d_model * ff
        n_block = d_model // (2 * width)

        mean_up, mean_down, held, clip, act_half = pl.pallas_call(
            functools.partial(grad_kernel, n_chunk, width),
            out_shape=(pltpu.VMEM((n_chunk, d_model, width), F32),
                       pltpu.VMEM((n_chunk, width, d_model), F32),
                       pltpu.VMEM((n_chunk, d_model, width), F32),
                       jax.ShapeDtypeStruct((8, 128), F32),
                       jax.ShapeDtypeStruct((n_micro, half, d_model), BF16)),
            in_specs=[hbm] * 11 + [smem, smem],
            out_specs=(vmem, vmem, vmem, vmem, hbm),
            scratch_shapes=[
                pltpu.VMEM((n_chunk, width, d_model), F32),
                pltpu.VMEM((2, d_model, width), F32),
                pltpu.VMEM((2, width, d_model), F32),
                pltpu.VMEM((2, half, d_model), F32),
                pltpu.VMEM((n_micro, half, d_model), F32),
                pltpu.VMEM((2 * n_micro, half, d_model), BF16),
                pltpu.VMEM((8, width), F32),
                pltpu.VMEM((8, d_model), F32),
                pltpu.VMEM((8, 128), F32),
                pltpu.VMEM((4, 8, 128), F32),
                dma((2, 2)), dma((2, 2)),
                dma((n_chunk,)), dma((n_chunk,)), dma((n_chunk,)), dma((n_chunk,)),
                dma((2,)), dma((2,)), dma((3,)), dma((4,)),
                dma(()), dma(()), dma((18,)), dma((2 * n_block,)), dma((2 * n_block,)), dma((2 * n_block,)),
            ],
            compiler_params=pltpu.CompilerParams(collective_id=0, has_side_effects=True, vmem_limit_bytes=VMEM_MAX - resident - SPARE),
            name="grad_exchange",
        )(w_up[0], w_down[0], g_up[0, 0], g_down[0, 0], m_up[0], v_up[0], m_down[0], v_down[0], acts_last.reshape(2, half, d_model), grad_out.reshape(2, half, d_model), x_next.reshape(2 * n_micro, half, d_model), max_norm, learn_rate)

        from_diag = lax.ppermute(act_half, ('model', 'stage'), [(0, 3), (2, 1)])
        from_core = lax.ppermute(act_half, ('model', 'stage'), [(0, 1), (2, 3)])

        def stay(array):
            return pltpu.with_memory_space_constraint(array, pltpu.VMEM)

        up_out = jax.ShapeDtypeStruct(w_up.shape, F32)
        down_out = jax.ShapeDtypeStruct(w_down.shape, F32)
        nw1, nm1, nv1, nw2, nm2, nv2, new1, new2, _ = pl.pallas_call(
            update_kernel,
            out_shape=(up_out, up_out, up_out, down_out, down_out, down_out,
                       pltpu.VMEM(mean_up.shape, F32), pltpu.VMEM(mean_down.shape, F32), pltpu.VMEM(held.shape, F32)),
            in_specs=[smem, smem, hbm, hbm, hbm, vmem, hbm, hbm, hbm, vmem, vmem],
            out_specs=(hbm,) * 6 + (vmem, vmem, vmem),
            input_output_aliases={5: 6, 9: 7, 10: 8},
            scratch_shapes=[pltpu.VMEM((3, SLOTS, width, d_model), F32), dma((3, SLOTS)), dma((3, SLOTS)), dma((18,))],
            compiler_params=pltpu.CompilerParams(vmem_limit_bytes=VMEM_MAX - resident - SPARE),
            cost_estimate=pl.CostEstimate(flops=2000 * d_model * ff, bytes_accessed=48 * d_model * ff, transcendentals=4 * d_model * ff),
            name="update",
        )(clip, learn_rate, w_up, m_up, v_up, stay(mean_up), w_down, m_down, v_down, stay(mean_down), stay(held))

        y_next = pl.pallas_call(
            forward_kernel,
            out_shape=pltpu.VMEM(x_next.shape, BF16),
            in_specs=[hbm, hbm, vmem, vmem],
            out_specs=vmem,
            scratch_shapes=[
                pltpu.VMEM((rows, ff), BF16),
                pltpu.VMEM((n_micro, rows, d_model), BF16),
                pltpu.VMEM((n_micro, half, d_model), BF16),
                pltpu.VMEM((n_micro, half, d_model), BF16),
                pltpu.VMEM((n_micro, rows, d_model), F32),
                pltpu.VMEM((n_micro, half, d_model), F32),
                dma((2,)), dma((n_micro, n_block)), dma((n_micro, n_block)), dma((n_micro, n_block)), dma((n_micro, n_block)),
                dma((n_micro,)), dma((n_micro,)), dma((n_micro,)), dma((n_micro,)),
                pltpu.SemaphoreType.REGULAR,
            ],
            compiler_params=pltpu.CompilerParams(collective_id=1, has_side_effects=True, vmem_limit_bytes=VMEM_MAX - resident - SPARE),
            name="forward_exchange",
        )(from_core, from_diag, stay(new1), stay(new2))
        return nw1, nw2, nm1, nm2, nv1, nv2, y_next

    return jax.shard_map(device_step, mesh=mesh, in_specs=in_specs, out_specs=out_specs, check_vma=False)
```

```python
import functools

import jax
import jax.numpy as jnp
from jax import lax
from jax.experimental import pallas as pl
from jax.experimental.pallas import tpu as pltpu
from jax.sharding import PartitionSpec as P


ADAM_STEP = 10
BETA_ONE = 0.9
BETA_TWO = 0.95
ADAM_EPS = 1e-8
WEIGHT_DECAY = 0.1
NORM_EPS = 1e-6
ONE_CORR = 1.0 - BETA_ONE ** ADAM_STEP
TWO_CORR = 1.0 - BETA_TWO ** ADAM_STEP
ROOT_EPS = ADAM_EPS * TWO_CORR ** 0.5
ROOT_GAIN = TWO_CORR ** 0.5 / ONE_CORR
TINY = 1.1754944e-38
HUGE = 3.4028235e38
GELU_A = 0.7978845608028654
GELU_B = 0.044715
NT = (((1,), (1,)), ((), ()))
TN = (((0,), (0,)), ((), ()))
MESH = pl.DeviceIdType.MESH
VMEM_MAX = 67_043_328
CHUNK = 128
SLOTS = 11
AHEAD = 7
SPARE = 5 << 19
F32 = jnp.float32
BF16 = jnp.bfloat16


def gelu_parts(z):
    t = jnp.tanh(GELU_A * (z + GELU_B * (z * z * z)))
    return t, z * (0.5 * (1.0 + t))


def gelu_slope(z, t):
    return 0.5 * (1.0 + t) + 0.5 * z * (1.0 - t * t) * (GELU_A * (1.0 + 3.0 * GELU_B * z * z))


def dot(a, b, dims=(((1,), (0,)), ((), ()))):
    return lax.dot_general(a, b, dims, preferred_element_type=F32)


def positions():
    return lax.axis_index("model"), lax.axis_index("data"), lax.axis_index("stage")


def entry_barrier(peers):
    barrier = pltpu.get_barrier_semaphore()
    for peer in peers:
        pl.semaphore_signal(barrier, inc=1, device_id=peer, device_id_type=MESH)
    pl.semaphore_wait(barrier, len(peers))


def remote(src, dst, send, recv, peer):
    return pltpu.make_async_remote_copy(src_ref=src, dst_ref=dst, send_sem=send, recv_sem=recv, device_id=peer, device_id_type=MESH)


def adamw(scale, rate, w, mom, sec, mean):
    grad = scale * mean
    mom_new = BETA_ONE * mom + (1.0 - BETA_ONE) * grad
    sec_new = BETA_TWO * sec + ((1.0 - BETA_TWO) * grad) * grad
    root = sec_new * lax.rsqrt(jnp.minimum(sec_new + TINY, HUGE))
    w_new = w * (1.0 - rate * WEIGHT_DECAY) - (rate * ROOT_GAIN) * (mom_new / (root + ROOT_EPS))
    return w_new, mom_new, sec_new


def grad_kernel(n_chunk, width, w1, w2, g1, g2, m1, v1, m2, v2, acts, dy, x, max_norm, rate,
                gr1, gr2, gs1, clip, act_half,
                gs2, w1b, w2b, part, got, x_buf, sq1, sq2, sq_out, sq_in,
                w_sem, g_sem, send1, send2, recv1, recv2, part_sem, gvec_sem, sq_send, sq_recv,
                row_sem, act_sem, f_sem, rs_send, rs_recv, out_sem):
    m, d, s = positions()
    peer_x = (m, 1 - d, s)
    peer_y = (1 - m, d, s)
    peer_c = (m, d, 1 - s)
    peer_d = (1 - m, d, 1 - s)
    d_model = w1.shape[0]
    is_last = s == 1
    is_first = s == 0

    def loads(j):
        slot = lax.rem(j, 2)
        cols = pl.ds(pl.multiple_of(j * width, width), width)
        return (pltpu.make_async_copy(w1.at[:, cols], w1b.at[slot], w_sem.at[0, slot]),
                pltpu.make_async_copy(w2.at[cols, :], w2b.at[slot], w_sem.at[1, slot]),
                pltpu.make_async_copy(g2.at[cols, :], gs2.at[j], g_sem.at[0, slot]),
                pltpu.make_async_copy(g1.at[:, cols], gs1.at[j], g_sem.at[1, slot]))

    acts_buf, gvec = x_buf.at[2:4], x_buf.at[4:6]
    load_acts = pltpu.make_async_copy(acts, acts_buf, act_sem)
    load_dy = pltpu.make_async_copy(dy, gvec, row_sem)
    load_x = pltpu.make_async_copy(x, x_buf, row_sem)

    load_acts.start()

    @pl.when(is_last)
    def _():
        load_dy.start()

    for copy in loads(0):
        copy.start()
    entry_barrier((peer_x, peer_y, peer_c, peer_d))
    for copy in loads(1):
        copy.start()

    hand_over = remote(x_buf.at[:2], gvec, gvec_sem.at[0], gvec_sem.at[1], peer_c)
    swap_part = remote(part, got.at[:2], part_sem.at[0], part_sem.at[1], peer_y)

    @pl.when(is_last)
    def _():
        part[...] = jnp.zeros_like(part)
        load_dy.wait()

    @pl.when(is_first)
    def _():
        hand_over.wait_recv()

    load_acts.wait()

    def send_two(j):
        return remote(gs2.at[j], gr2.at[j], send2.at[j], recv2.at[j], peer_x)

    def send_one(j):
        return remote(gs1.at[j], gr1.at[j], send1.at[j], recv1.at[j], peer_x)

    @pl.loop(0, n_chunk)
    def _(j):
        slot = lax.rem(j, 2)
        copies = loads(j)
        copies[0].wait()
        up = w1b[slot].astype(BF16)
        rows = acts_buf[...].reshape(-1, d_model)
        grad = gvec[...].reshape(-1, d_model)
        z = dot(rows, up)
        t, act = gelu_parts(z)
        hid = act.astype(BF16)
        copies[2].wait()
        gs2[j] += dot(hid, grad, TN)
        send_two(j).start()
        copies[1].wait()
        grad_hid = dot(grad, w2b[slot].astype(BF16), NT)
        grad_pre = (gelu_slope(z, t) * grad_hid).astype(BF16)
        copies[3].wait()
        gs1[j] += dot(rows, grad_pre, TN)
        send_one(j).start()

        @pl.when(is_last)
        def _():
            part[...] += dot(grad_pre, up, NT).reshape(part.shape)

        @pl.when(j + 2 < n_chunk)
        def _():
            for copy in loads(j + 2):
                copy.start()

    @pl.when(is_last)
    def _():
        swap_part.start()
        swap_part.wait()
        x_buf[:2] = (gvec[...].astype(F32) + (part[...] + got[:2])).astype(BF16)
        hand_over.start()

    @pl.when(is_first)
    def _():
        load_x.start()

    n_up = n_chunk // 2
    n_pair = 2 * n_up

    def fetch(p):
        base = lax.rem(p, 3) * 6

        @pl.when(p < n_up)
        def _():
            for q, ref in enumerate((w1, m1, v1)):
                for h in (0, 1):
                    cols = pl.ds(pl.multiple_of((2 * p + h) * width, width), width)
                    pltpu.make_async_copy(ref.at[:, cols], gs1.at[base + 2 * q + h], f_sem.at[base + 2 * q + h]).start()

        @pl.when(p >= n_up)
        def _():
            cols = pl.ds(pl.multiple_of((p - n_up) * width, width), width)
            for q, ref in enumerate((w2, m2, v2)):
                for h in (0, 1):
                    rows = pl.ds(h * d_model, d_model)
                    pltpu.make_async_copy(ref.at[rows, cols], gs1.at[base + 2 * q + h], f_sem.at[base + 2 * q + h]).start()

    def arrive(p):
        base = lax.rem(p, 3) * 6
        for i in range(6):
            pltpu.make_async_copy(w1.at[:, :width], gs1.at[base + i], f_sem.at[base + i]).wait()

    def free_and_fetch(lo, hi, p):
        for i in range(lo, hi):
            send_one(i).wait_send()

        fetch(p)

    sq1[...] = jnp.zeros_like(sq1)
    sq2[...] = jnp.zeros_like(sq2)

    @pl.loop(0, n_chunk)
    def _(j):
        send_two(j).wait_recv()
        mean = (gs2[j] + gr2[j]) * 0.5
        gr2[j] = mean
        sq2[...] += jnp.sum((mean * mean).reshape(-1, 8, mean.shape[1]), axis=0)
        send_one(j).wait_recv()
        mean = (gs1[j] + gr1[j]) * 0.5
        gr1[j] = mean
        sq1[...] += jnp.sum((mean * mean).reshape(-1, 8, mean.shape[1]), axis=0)

        @pl.when(j == 10)
        def _():
            free_and_fetch(0, 6, 18 * s)

        @pl.when(j == 15)
        def _():
            free_and_fetch(6, 12, 1 + 18 * s)

    sq_out[...] = jnp.full(sq_out.shape, jnp.sum(sq1[...]) + jnp.sum(sq2[...]), F32)
    mine = 2 * m + s
    others = ((peer_y, 2 * (1 - m) + s), (peer_c, 2 * m + 1 - s), (peer_d, 2 * (1 - m) + 1 - s))
    shares = [remote(sq_out, sq_in.at[mine], sq_send.at[k], sq_recv.at[mine], peer) for k, (peer, _) in enumerate(others)]
    for copy in shares:
        copy.start()
    free_and_fetch(12, n_chunk, 2 + 15 * s)
    sq_in[mine] = sq_out[...]
    for peer, index in others:
        remote(sq_out, sq_in.at[index], sq_send.at[0], sq_recv.at[index], peer).wait_recv()
    total = (sq_in[0] + sq_in[1]) + (sq_in[2] + sq_in[3])
    clip[...] = jnp.minimum(1.0, max_norm[0] / (jnp.sqrt(total) + NORM_EPS))

    for j in range(n_chunk):
        send_two(j).wait_send()
    for copy in shares:
        copy.wait_send()

    @pl.when(is_last)
    def _():
        hand_over.wait_send()
        for p in (18, 19, 17):
            arrive(jnp.int32(p))

    @pl.when(is_first)
    def _():
        scale = clip[0, 0]
        step_rate = rate[0]
        group, half = x_buf.shape[:2]
        n_micro = group // 2
        wide = 2 * width
        n_block = d_model // width

        def new_weights(p, means):
            base = lax.rem(p, 3) * 6
            return [adamw(scale, step_rate, gs1[base + h], gs1[base + 2 + h], gs1[base + 4 + h], means[h])[0].astype(BF16) for h in (0, 1)]

        def up_pair(p):
            new = jnp.concatenate(new_weights(p, [gr1[2 * p], gr1[2 * p + 1]]), axis=1)
            act = gelu_parts(dot(x_buf[...].reshape(-1, d_model), new))[1].astype(BF16).astype(F32)
            cols = pl.ds(pl.multiple_of(lax.rem(p, n_up // 2) * wide, wide), wide)
            gs2[pl.ds((p // (n_up // 2)) * group, group), :, cols] = act.reshape(group, half, wide)

        def block(c):
            return pl.ds(pl.multiple_of(c * width, width), width)

        def down_pair(c):
            new = new_weights(n_up + c, [gr2[h * n_up:(h + 1) * n_up, :, block(c)].reshape(d_model, width) for h in (0, 1)])
            low, high = [dot(gs2[h * group:(h + 1) * group].reshape(-1, d_model).astype(BF16), new[h]) for h in (0, 1)]
            res = (low + high).reshape(group, half, width)
            for g in range(group):
                other = m if g % 2 == 0 else 1 - m
                gs2[2 * group + g // 2 + n_micro * other, :, block(c)] = res[g]
            block_copy(c).start()

        def block_copy(c):
            return remote(gs2.at[2 * group + n_micro:2 * group + 2 * n_micro, :, block(c)], got.at[:, :, block(c)], rs_send.at[c], rs_recv.at[c], peer_y)

        def ahead(p):
            @pl.when(p < n_pair)
            def _():
                fetch(p)

        load_x.wait()

        @pl.loop(0, n_up)
        def _(p):
            arrive(p)
            up_pair(p)
            ahead(p + 3)

        @pl.loop(0, n_block)
        def _(c):
            arrive(n_up + c)
            down_pair(c)
            ahead(n_up + c + 3)

        def store(c):
            return pltpu.make_async_copy(x_buf.at[:n_micro, :, block(c)], act_half.at[:, :, block(c)], out_sem.at[c])

        @pl.loop(0, n_block)
        def _(c):
            block_copy(c).wait_recv()
            for k in range(n_micro):
                rows = x_buf[2 * k + m, :, block(c)].astype(F32)
                x_buf[k, :, block(c)] = (rows + (gs2[2 * group + k, :, block(c)] + got[k, :, block(c)])).astype(BF16)
            store(c).start()

        @pl.loop(0, n_block)
        def _(c):
            block_copy(c).wait_send()
            store(c).wait()


def update_kernel(clip, rate, w1, m1, v1, gb1, w2, m2, v2, gb2, held, nw1, nm1, nv1, nw2, nm2, nv2, keep1, keep2, held_out,
                  ring, in_sem, out_sem, held_sem):
    _, deep, wide = gb1.shape
    n_slot, tall, span = ring.shape[1:]
    block = deep // tall
    per_row = w1.shape[2] // span
    n_up = per_row * (deep // tall)
    n_down = w2.shape[1] // tall
    last = n_up + n_down
    scale = clip[0, 0]
    step_rate = rate[0]
    n_held = 3
    first_held = span // wide - n_held
    kinds = ((0, n_up, span), (n_up, last, first_held * wide))

    def copies(i, kind, fetch):
        slot = lax.rem(i, n_slot)
        sem = in_sem if fetch else out_sem
        cols = kinds[kind][2]
        if kind == 0:
            refs = (w1, m1, v1) if fetch else (nw1, nm1, nv1)
            where = (0, pl.ds(pl.multiple_of(i // per_row * tall, tall), tall), pl.ds(pl.multiple_of(lax.rem(i, per_row) * span, span), span))
        else:
            refs = (w2, m2, v2) if fetch else (nw2, nm2, nv2)
            where = (0, pl.ds(pl.multiple_of((i - n_up) * tall, tall), tall), slice(0, cols))
        out = []
        for k, ref in enumerate(refs):
            pair = (ref.at[where], ring.at[k, slot, :, :cols])
            out.append(pltpu.make_async_copy(*(pair if fetch else pair[::-1]), sem.at[k, slot]))
        return out

    def each(i, act):
        if isinstance(i, int):
            kind = [n for n, (lo, hi, _) in enumerate(kinds) if lo <= i < hi][0]
            act(jnp.int32(i), kind)
            return
        for kind, (lo, hi, _) in enumerate(kinds):
            @pl.when((i >= lo) & (i < hi))
            def _():
                act(i, kind)

    def start(i, fetch):
        def act(i, kind):
            for copy in copies(i, kind, fetch):
                copy.start()

        each(i, act)

    def finish(i, fetch):
        def act(i, kind):
            for copy in copies(i, kind, fetch):
                copy.wait()

        each(i, act)

    for i in range(AHEAD):
        start(i, True)

    near = [(spot, h) for spot in range(n_held) for h in (0, 1)]

    def held_copies(spot, h):
        col = first_held + (spot + 1) % n_held
        rows, cols = slice(h * deep, (h + 1) * deep), slice(col * wide, (col + 1) * wide)
        return cols, [pltpu.make_async_copy(held_out.at[6 * spot + 2 * k + h], ref.at[0, rows, cols], held_sem.at[6 * spot + 2 * k + h])
                      for k, ref in enumerate((nw2, nm2, nv2))]

    for spot, h in near:
        cols, moves = held_copies(spot, h)
        rows = slice(h * block, (h + 1) * block)
        base = 6 * spot + h
        new, mom, sec = adamw(scale, step_rate, held[base], held[base + 2], held[base + 4], gb2[rows, :, cols].reshape(deep, wide))
        held_out[base] = new
        held_out[base + 2] = mom
        held_out[base + 4] = sec
        keep2[rows, :, cols] = new.reshape(block, -1, wide)
        for copy in moves:
            copy.start()

    def step(slot, cols, mean):
        new, mom, sec = adamw(scale, step_rate, ring[0, slot, :, cols], ring[1, slot, :, cols], ring[2, slot, :, cols], mean)
        ring[0, slot, :, cols] = new
        ring[1, slot, :, cols] = mom
        ring[2, slot, :, cols] = sec
        return new

    def compute(i, kind):
        slot = lax.rem(i, n_slot)
        if kind == 0:
            rows = pl.ds(pl.multiple_of(i // per_row * tall, tall), tall)
            for t in range(span // wide):
                col = lax.rem(i, per_row) * (span // wide) + t
                keep1[col, rows] = step(slot, slice(t * wide, (t + 1) * wide), gb1[col, rows])
        else:
            cols = slice(0, kinds[kind][2])
            keep2[i - n_up, :, cols] = step(slot, cols, gb2[i - n_up, :, cols])

    @pl.loop(0, last)
    def _(i):
        finish(i, True)
        each(i, compute)
        start(i, False)

        @pl.when(i + AHEAD < last)
        def _():
            @pl.when(i + AHEAD - n_slot >= 0)
            def _():
                finish(i + AHEAD - n_slot, False)

            start(i + AHEAD, True)

    for i in range(last - n_slot, last):
        finish(i, False)
    for spot, h in near:
        for copy in held_copies(spot, h)[1]:
            copy.wait()


def forward_kernel(from_core, from_diag, new1, new2, y,
                   hid, act, own_half, peer_half, part, part_in,
                   in_sem, p_send, p_recv, y_send, y_recv, g_send, g_recv, f_send, f_recv, ready):
    m, d, s = positions()
    n_micro, half, d_model = own_half.shape
    width = 2 * new1.shape[2]
    n_chunk, n_block = new1.shape[0] // 2, d_model // width
    peer_y = (1 - m, d, s)
    peer_c = (m, d, 1 - s)
    barrier = pltpu.get_barrier_semaphore()
    mine = pl.ds(pl.multiple_of(m * half, half), half)
    theirs = pl.ds(pl.multiple_of((1 - m) * half, half), half)
    rows_in = (pltpu.make_async_copy(from_core, act.at[:, mine, :], in_sem.at[0]),
               pltpu.make_async_copy(from_diag, act.at[:, theirs, :], in_sem.at[1]))

    @pl.when(s == 1)
    def _():
        for copy in rows_in:
            copy.start()
        pl.semaphore_signal(barrier, inc=1, device_id=peer_y, device_id_type=MESH)
        pl.semaphore_signal(barrier, inc=1, device_id=peer_c, device_id_type=MESH)

    pl.semaphore_wait(barrier, 1)

    @pl.when(s == 0)
    def _():
        pl.semaphore_signal(ready, inc=1, device_id=peer_c, device_id_type=MESH)

    def span(c):
        return pl.ds(pl.multiple_of(c * width, width), width)

    def send_part(k, c):
        return remote(part.at[k, theirs, span(c)], part_in.at[k, :, span(c)], p_send.at[k, c], p_recv.at[k, c], peer_y)

    def swap_y(k, c):
        return remote(own_half.at[k, :, span(c)], peer_half.at[k, :, span(c)], y_send.at[k, c], y_recv.at[k, c], peer_y)

    def give_own(k):
        return remote(own_half.at[k], y.at[k, mine, :], g_send.at[k], g_recv.at[k], peer_c)

    def pass_on(k):
        return remote(peer_half.at[k], y.at[k, theirs, :], f_send.at[k], f_recv.at[k], peer_c)

    @pl.when(s == 0)
    def _():
        for k in range(n_micro):
            give_own(k).wait_recv()
            pass_on(k).wait_recv()

    @pl.when(s == 1)
    def _():
        for copy in rows_in:
            copy.wait()

        for k in range(n_micro):
            @pl.loop(0, n_chunk)
            def _(j):
                up = jnp.concatenate([new1[2 * j].astype(BF16), new1[2 * j + 1].astype(BF16)], axis=1)
                hid[:, span(j)] = gelu_parts(dot(act[k], up))[1].astype(BF16)

            @pl.loop(0, n_block)
            def _(c):
                down = new2[:, :, span(c)].reshape(-1, width).astype(BF16)
                part[k, :, span(c)] = dot(hid[...], down)
                send_part(k, c).start()

        for k in range(n_micro):
            @pl.loop(0, n_block)
            def _(c):
                send_part(k, c).wait_recv()
                out = act[k, mine, span(c)].astype(F32) + (part[k, mine, span(c)] + part_in[k, :, span(c)])
                own_half[k, :, span(c)] = out.astype(BF16)
                swap_y(k, c).start()

            y[k, mine, :] = own_half[k]

        pl.semaphore_wait(ready, 1)
        for k in range(n_micro):
            give_own(k).start()
        for k in range(n_micro):
            @pl.loop(0, n_block)
            def _(c):
                swap_y(k, c).wait_recv()

            pass_on(k).start()
            y[k, theirs, :] = peer_half[k]
        for k in range(n_micro):
            @pl.loop(0, n_block)
            def _(c):
                send_part(k, c).wait_send()
                swap_y(k, c).wait_send()

            give_own(k).wait_send()
            pass_on(k).wait_send()


def solution(mesh):
    up_spec = P('stage', None, 'model')
    down_spec = P('stage', 'model', None)
    row_spec = P(None, 'data', None)
    in_specs = (up_spec, down_spec, up_spec, down_spec, up_spec, down_spec, P('data', 'stage', None, 'model'), P('data', 'stage', 'model', None), P('stage', 'data', None), P('data', None), row_spec, P(None), P(None))
    out_specs = (up_spec, down_spec, up_spec, down_spec, up_spec, down_spec, row_spec)

    def device_step(w_up, w_down, m_up, m_down, v_up, v_down, g_up, g_down, acts_last, grad_out, x_next, learn_rate, max_norm):
        d_model, ff = w_up.shape[1:]
        rows = grad_out.shape[0]
        n_micro = x_next.shape[0]
        width = CHUNK
        n_chunk = ff // width
        half = rows // 2
        hbm = pl.BlockSpec(memory_space=pl.ANY)
        vmem = pl.BlockSpec(memory_space=pltpu.VMEM)
        smem = pl.BlockSpec(memory_space=pltpu.SMEM)
        dma = pltpu.SemaphoreType.DMA
        resident = 4 * 3 * d_model * ff
        n_block = d_model // (2 * width)

        mean_up, mean_down, held, clip, act_half = pl.pallas_call(
            functools.partial(grad_kernel, n_chunk, width),
            out_shape=(pltpu.VMEM((n_chunk, d_model, width), F32),
                       pltpu.VMEM((n_chunk, width, d_model), F32),
                       pltpu.VMEM((n_chunk, d_model, width), F32),
                       jax.ShapeDtypeStruct((8, 128), F32),
                       jax.ShapeDtypeStruct((n_micro, half, d_model), BF16)),
            in_specs=[hbm] * 11 + [smem, smem],
            out_specs=(vmem, vmem, vmem, vmem, hbm),
            scratch_shapes=[
                pltpu.VMEM((n_chunk, width, d_model), F32),
                pltpu.VMEM((2, d_model, width), F32),
                pltpu.VMEM((2, width, d_model), F32),
                pltpu.VMEM((2, half, d_model), F32),
                pltpu.VMEM((n_micro, half, d_model), F32),
                pltpu.VMEM((2 * n_micro, half, d_model), BF16),
                pltpu.VMEM((8, width), F32),
                pltpu.VMEM((8, d_model), F32),
                pltpu.VMEM((8, 128), F32),
                pltpu.VMEM((4, 8, 128), F32),
                dma((2, 2)), dma((2, 2)),
                dma((n_chunk,)), dma((n_chunk,)), dma((n_chunk,)), dma((n_chunk,)),
                dma((2,)), dma((2,)), dma((3,)), dma((4,)),
                dma(()), dma(()), dma((18,)), dma((2 * n_block,)), dma((2 * n_block,)), dma((2 * n_block,)),
            ],
            compiler_params=pltpu.CompilerParams(collective_id=0, has_side_effects=True, vmem_limit_bytes=VMEM_MAX - resident - SPARE),
            name="grad_exchange",
        )(w_up[0], w_down[0], g_up[0, 0], g_down[0, 0], m_up[0], v_up[0], m_down[0], v_down[0], acts_last.reshape(2, half, d_model), grad_out.reshape(2, half, d_model), x_next.reshape(2 * n_micro, half, d_model), max_norm, learn_rate)

        from_diag = lax.ppermute(act_half, ('model', 'stage'), [(0, 3), (2, 1)])
        from_core = lax.ppermute(act_half, ('model', 'stage'), [(0, 1), (2, 3)])

        def stay(array):
            return pltpu.with_memory_space_constraint(array, pltpu.VMEM)

        up_out = jax.ShapeDtypeStruct(w_up.shape, F32)
        down_out = jax.ShapeDtypeStruct(w_down.shape, F32)
        nw1, nm1, nv1, nw2, nm2, nv2, new1, new2, _ = pl.pallas_call(
            update_kernel,
            out_shape=(up_out, up_out, up_out, down_out, down_out, down_out,
                       pltpu.VMEM(mean_up.shape, F32), pltpu.VMEM(mean_down.shape, F32), pltpu.VMEM(held.shape, F32)),
            in_specs=[smem, smem, hbm, hbm, hbm, vmem, hbm, hbm, hbm, vmem, vmem],
            out_specs=(hbm,) * 6 + (vmem, vmem, vmem),
            input_output_aliases={5: 6, 9: 7, 10: 8},
            scratch_shapes=[pltpu.VMEM((3, SLOTS, width, d_model), F32), dma((3, SLOTS)), dma((3, SLOTS)), dma((18,))],
            compiler_params=pltpu.CompilerParams(vmem_limit_bytes=VMEM_MAX - resident - SPARE),
            cost_estimate=pl.CostEstimate(flops=2000 * d_model * ff, bytes_accessed=48 * d_model * ff, transcendentals=4 * d_model * ff),
            name="update",
        )(clip, learn_rate, w_up, m_up, v_up, stay(mean_up), w_down, m_down, v_down, stay(mean_down), stay(held))

        y_next = pl.pallas_call(
            forward_kernel,
            out_shape=pltpu.VMEM(x_next.shape, BF16),
            in_specs=[hbm, hbm, vmem, vmem],
            out_specs=vmem,
            scratch_shapes=[
                pltpu.VMEM((rows, ff), BF16),
                pltpu.VMEM((n_micro, rows, d_model), BF16),
                pltpu.VMEM((n_micro, half, d_model), BF16),
                pltpu.VMEM((n_micro, half, d_model), BF16),
                pltpu.VMEM((n_micro, rows, d_model), F32),
                pltpu.VMEM((n_micro, half, d_model), F32),
                dma((2,)), dma((n_micro, n_block)), dma((n_micro, n_block)), dma((n_micro, n_block)), dma((n_micro, n_block)),
                dma((n_micro,)), dma((n_micro,)), dma((n_micro,)), dma((n_micro,)),
                pltpu.SemaphoreType.REGULAR,
            ],
            compiler_params=pltpu.CompilerParams(collective_id=1, has_side_effects=True, vmem_limit_bytes=VMEM_MAX - resident - SPARE),
            name="forward_exchange",
        )(from_core, from_diag, stay(new1), stay(new2))
        return nw1, nw2, nm1, nm2, nv1, nv2, y_next

    return jax.shard_map(device_step, mesh=mesh, in_specs=in_specs, out_specs=out_specs, check_vma=False)
```

```python
import functools

import jax
import jax.numpy as jnp
from jax import lax
from jax.experimental import pallas as pl
from jax.experimental.pallas import tpu as pltpu
from jax.sharding import PartitionSpec as P


ADAM_STEP = 10
BETA_ONE = 0.9
BETA_TWO = 0.95
ADAM_EPS = 1e-8
WEIGHT_DECAY = 0.1
NORM_EPS = 1e-6
ONE_CORR = 1.0 - BETA_ONE ** ADAM_STEP
TWO_CORR = 1.0 - BETA_TWO ** ADAM_STEP
ROOT_EPS = ADAM_EPS * TWO_CORR ** 0.5
ROOT_GAIN = TWO_CORR ** 0.5 / ONE_CORR
TINY = 1.1754944e-38
HUGE = 3.4028235e38
GELU_A = 0.7978845608028654
GELU_B = 0.044715
NT = (((1,), (1,)), ((), ()))
TN = (((0,), (0,)), ((), ()))
MESH = pl.DeviceIdType.MESH
VMEM_MAX = 67_043_328
CHUNK = 128
SLOTS = 11
AHEAD = 8
SPARE = 5 << 19
F32 = jnp.float32
BF16 = jnp.bfloat16


def gelu_parts(z):
    t = jnp.tanh(GELU_A * (z + GELU_B * (z * z * z)))
    return t, z * (0.5 * (1.0 + t))


def gelu_slope(z, t):
    return 0.5 * (1.0 + t) + 0.5 * z * (1.0 - t * t) * (GELU_A * (1.0 + 3.0 * GELU_B * z * z))


def dot(a, b, dims=(((1,), (0,)), ((), ()))):
    return lax.dot_general(a, b, dims, preferred_element_type=F32)


def positions():
    return lax.axis_index("model"), lax.axis_index("data"), lax.axis_index("stage")


def entry_barrier(peers):
    barrier = pltpu.get_barrier_semaphore()
    for peer in peers:
        pl.semaphore_signal(barrier, inc=1, device_id=peer, device_id_type=MESH)
    pl.semaphore_wait(barrier, len(peers))


def remote(src, dst, send, recv, peer):
    return pltpu.make_async_remote_copy(src_ref=src, dst_ref=dst, send_sem=send, recv_sem=recv, device_id=peer, device_id_type=MESH)


def adamw(scale, rate, w, mom, sec, mean):
    grad = scale * mean
    mom_new = BETA_ONE * mom + (1.0 - BETA_ONE) * grad
    sec_new = BETA_TWO * sec + ((1.0 - BETA_TWO) * grad) * grad
    root = sec_new * lax.rsqrt(jnp.minimum(sec_new + TINY, HUGE))
    w_new = w * (1.0 - rate * WEIGHT_DECAY) - (rate * ROOT_GAIN) * (mom_new / (root + ROOT_EPS))
    return w_new, mom_new, sec_new


def grad_kernel(n_chunk, width, w1, w2, g1, g2, m1, v1, m2, v2, acts, dy, x, max_norm, rate,
                gr1, gr2, gs1, clip, act_half,
                gs2, w1b, w2b, part, got, x_buf, sq1, sq2, sq_out, sq_in,
                w_sem, g_sem, send1, send2, recv1, recv2, part_sem, gvec_sem, sq_send, sq_recv,
                row_sem, act_sem, f_sem, rs_send, rs_recv, out_sem):
    m, d, s = positions()
    peer_x = (m, 1 - d, s)
    peer_y = (1 - m, d, s)
    peer_c = (m, d, 1 - s)
    peer_d = (1 - m, d, 1 - s)
    d_model = w1.shape[0]
    is_last = s == 1
    is_first = s == 0

    def loads(j):
        slot = lax.rem(j, 2)
        cols = pl.ds(pl.multiple_of(j * width, width), width)
        return (pltpu.make_async_copy(w1.at[:, cols], w1b.at[slot], w_sem.at[0, slot]),
                pltpu.make_async_copy(w2.at[cols, :], w2b.at[slot], w_sem.at[1, slot]),
                pltpu.make_async_copy(g2.at[cols, :], gs2.at[j], g_sem.at[0, slot]),
                pltpu.make_async_copy(g1.at[:, cols], gs1.at[j], g_sem.at[1, slot]))

    acts_buf, gvec = x_buf.at[2:4], x_buf.at[4:6]
    load_acts = pltpu.make_async_copy(acts, acts_buf, act_sem)
    load_dy = pltpu.make_async_copy(dy, gvec, row_sem)
    load_x = pltpu.make_async_copy(x, x_buf, row_sem)

    load_acts.start()
    urgent = loads(0)
    urgent[0].start()

    @pl.when(is_last)
    def _():
        load_dy.start()

    urgent[2].start()
    entry_barrier((peer_x, peer_y, peer_c, peer_d))
    for copy in (urgent[1], urgent[3], *loads(1)):
        copy.start()

    hand_over = remote(x_buf.at[:2], gvec, gvec_sem.at[0], gvec_sem.at[1], peer_c)
    swap_part = remote(part, got.at[:2], part_sem.at[0], part_sem.at[1], peer_y)

    @pl.when(is_last)
    def _():
        part[...] = jnp.zeros_like(part)
        load_dy.wait()

    @pl.when(is_first)
    def _():
        hand_over.wait_recv()

    load_acts.wait()

    def send_two(j):
        return remote(gs2.at[j], gr2.at[j], send2.at[j], recv2.at[j], peer_x)

    def send_one(j):
        return remote(gs1.at[j], gr1.at[j], send1.at[j], recv1.at[j], peer_x)

    @pl.loop(0, n_chunk)
    def _(j):
        slot = lax.rem(j, 2)
        copies = loads(j)
        copies[0].wait()
        up = w1b[slot].astype(BF16)
        rows = acts_buf[...].reshape(-1, d_model)
        grad = gvec[...].reshape(-1, d_model)
        z = dot(rows, up)
        t, act = gelu_parts(z)
        hid = act.astype(BF16)
        copies[2].wait()
        gs2[j] += dot(hid, grad, TN)
        send_two(j).start()
        copies[1].wait()
        grad_hid = dot(grad, w2b[slot].astype(BF16), NT)
        grad_pre = (gelu_slope(z, t) * grad_hid).astype(BF16)
        copies[3].wait()
        gs1[j] += dot(rows, grad_pre, TN)
        send_one(j).start()

        @pl.when(is_last)
        def _():
            part[...] += dot(grad_pre, up, NT).reshape(part.shape)

        @pl.when(j + 2 < n_chunk)
        def _():
            for copy in loads(j + 2):
                copy.start()

    @pl.when(is_last)
    def _():
        swap_part.start()
        swap_part.wait()
        x_buf[:2] = (gvec[...].astype(F32) + (part[...] + got[:2])).astype(BF16)
        hand_over.start()

    @pl.when(is_first)
    def _():
        load_x.start()

    n_up = n_chunk // 2
    n_pair = 2 * n_up

    def fetch(p):
        base = lax.rem(p, 3) * 6

        @pl.when(p < n_up)
        def _():
            for q, ref in enumerate((w1, m1, v1)):
                for h in (0, 1):
                    cols = pl.ds(pl.multiple_of((2 * p + h) * width, width), width)
                    pltpu.make_async_copy(ref.at[:, cols], gs1.at[base + 2 * q + h], f_sem.at[base + 2 * q + h]).start()

        @pl.when(p >= n_up)
        def _():
            cols = pl.ds(pl.multiple_of((p - n_up) * width, width), width)
            for q, ref in enumerate((w2, m2, v2)):
                for h in (0, 1):
                    rows = pl.ds(h * d_model, d_model)
                    pltpu.make_async_copy(ref.at[rows, cols], gs1.at[base + 2 * q + h], f_sem.at[base + 2 * q + h]).start()

    def arrive(p):
        base = lax.rem(p, 3) * 6
        for i in range(6):
            pltpu.make_async_copy(w1.at[:, :width], gs1.at[base + i], f_sem.at[base + i]).wait()

    def free_and_fetch(lo, hi, p):
        for i in range(lo, hi):
            send_one(i).wait_send()

        fetch(p)

    sq1[...] = jnp.zeros_like(sq1)
    sq2[...] = jnp.zeros_like(sq2)

    @pl.loop(0, n_chunk)
    def _(j):
        send_two(j).wait_recv()
        mean = (gs2[j] + gr2[j]) * 0.5
        gr2[j] = mean
        sq2[...] += jnp.sum((mean * mean).reshape(-1, 8, mean.shape[1]), axis=0)
        send_one(j).wait_recv()
        mean = (gs1[j] + gr1[j]) * 0.5
        gr1[j] = mean
        sq1[...] += jnp.sum((mean * mean).reshape(-1, 8, mean.shape[1]), axis=0)

        @pl.when(j == 10)
        def _():
            free_and_fetch(0, 6, 18 * s)

        @pl.when(j == 15)
        def _():
            free_and_fetch(6, 12, 1 + 18 * s)

    sq_out[...] = jnp.full(sq_out.shape, jnp.sum(sq1[...]) + jnp.sum(sq2[...]), F32)
    mine = 2 * m + s
    others = ((peer_y, 2 * (1 - m) + s), (peer_c, 2 * m + 1 - s), (peer_d, 2 * (1 - m) + 1 - s))
    shares = [remote(sq_out, sq_in.at[mine], sq_send.at[k], sq_recv.at[mine], peer) for k, (peer, _) in enumerate(others)]
    for copy in shares:
        copy.start()
    free_and_fetch(12, n_chunk, 2 + 15 * s)
    sq_in[mine] = sq_out[...]
    for peer, index in others:
        remote(sq_out, sq_in.at[index], sq_send.at[0], sq_recv.at[index], peer).wait_recv()
    total = (sq_in[0] + sq_in[1]) + (sq_in[2] + sq_in[3])
    clip[...] = jnp.minimum(1.0, max_norm[0] / (jnp.sqrt(total) + NORM_EPS))

    for j in range(n_chunk):
        send_two(j).wait_send()
    for copy in shares:
        copy.wait_send()

    @pl.when(is_last)
    def _():
        hand_over.wait_send()
        for p in (18, 19, 17):
            arrive(jnp.int32(p))

    @pl.when(is_first)
    def _():
        scale = clip[0, 0]
        step_rate = rate[0]
        group, half = x_buf.shape[:2]
        n_micro = group // 2
        wide = 2 * width
        n_block = d_model // width

        def new_weights(p, means):
            base = lax.rem(p, 3) * 6
            return [adamw(scale, step_rate, gs1[base + h], gs1[base + 2 + h], gs1[base + 4 + h], means[h])[0].astype(BF16) for h in (0, 1)]

        def up_pair(p):
            new = jnp.concatenate(new_weights(p, [gr1[2 * p], gr1[2 * p + 1]]), axis=1)
            act = gelu_parts(dot(x_buf[...].reshape(-1, d_model), new))[1].astype(BF16).astype(F32)
            cols = pl.ds(pl.multiple_of(lax.rem(p, n_up // 2) * wide, wide), wide)
            gs2[pl.ds((p // (n_up // 2)) * group, group), :, cols] = act.reshape(group, half, wide)

        def block(c):
            return pl.ds(pl.multiple_of(c * width, width), width)

        def down_pair(c):
            new = new_weights(n_up + c, [gr2[h * n_up:(h + 1) * n_up, :, block(c)].reshape(d_model, width) for h in (0, 1)])
            low, high = [dot(gs2[h * group:(h + 1) * group].reshape(-1, d_model).astype(BF16), new[h]) for h in (0, 1)]
            res = (low + high).reshape(group, half, width)
            for g in range(group):
                other = m if g % 2 == 0 else 1 - m
                gs2[2 * group + g // 2 + n_micro * other, :, block(c)] = res[g]
            block_copy(c).start()

        def block_copy(c):
            return remote(gs2.at[2 * group + n_micro:2 * group + 2 * n_micro, :, block(c)], got.at[:, :, block(c)], rs_send.at[c], rs_recv.at[c], peer_y)

        def ahead(p):
            @pl.when(p < n_pair)
            def _():
                fetch(p)

        load_x.wait()

        @pl.loop(0, n_up)
        def _(p):
            arrive(p)
            up_pair(p)
            ahead(p + 3)

        @pl.loop(0, n_block)
        def _(c):
            arrive(n_up + c)
            down_pair(c)
            ahead(n_up + c + 3)

        def store(c):
            return pltpu.make_async_copy(x_buf.at[:n_micro, :, block(c)], act_half.at[:, :, block(c)], out_sem.at[c])

        @pl.loop(0, n_block)
        def _(c):
            block_copy(c).wait_recv()
            for k in range(n_micro):
                rows = x_buf[2 * k + m, :, block(c)].astype(F32)
                x_buf[k, :, block(c)] = (rows + (gs2[2 * group + k, :, block(c)] + got[k, :, block(c)])).astype(BF16)
            store(c).start()

        @pl.loop(0, n_block)
        def _(c):
            block_copy(c).wait_send()
            store(c).wait()


def update_kernel(clip, rate, w1, m1, v1, gb1, w2, m2, v2, gb2, held, nw1, nm1, nv1, nw2, nm2, nv2, keep1, keep2, held_out,
                  ring, in_sem, out_sem, held_sem):
    _, deep, wide = gb1.shape
    n_slot, tall, span = ring.shape[1:]
    block = deep // tall
    per_row = w1.shape[2] // span
    n_up = per_row * (deep // tall)
    n_down = w2.shape[1] // tall
    last = n_up + n_down
    scale = clip[0, 0]
    step_rate = rate[0]
    n_held = 3
    first_held = span // wide - n_held
    kinds = ((0, n_up, span), (n_up, last, first_held * wide))

    def copies(i, kind, fetch):
        slot = lax.rem(i, n_slot)
        sem = in_sem if fetch else out_sem
        cols = kinds[kind][2]
        if kind == 0:
            refs = (w1, m1, v1) if fetch else (nw1, nm1, nv1)
            where = (0, pl.ds(pl.multiple_of(i // per_row * tall, tall), tall), pl.ds(pl.multiple_of(lax.rem(i, per_row) * span, span), span))
        else:
            refs = (w2, m2, v2) if fetch else (nw2, nm2, nv2)
            where = (0, pl.ds(pl.multiple_of((i - n_up) * tall, tall), tall), slice(0, cols))
        out = []
        for k, ref in enumerate(refs):
            pair = (ref.at[where], ring.at[k, slot, :, :cols])
            out.append(pltpu.make_async_copy(*(pair if fetch else pair[::-1]), sem.at[k, slot]))
        return out

    def each(i, act):
        if isinstance(i, int):
            kind = [n for n, (lo, hi, _) in enumerate(kinds) if lo <= i < hi][0]
            act(jnp.int32(i), kind)
            return
        for kind, (lo, hi, _) in enumerate(kinds):
            @pl.when((i >= lo) & (i < hi))
            def _():
                act(i, kind)

    def start(i, fetch):
        def act(i, kind):
            for copy in copies(i, kind, fetch):
                copy.start()

        each(i, act)

    def finish(i, fetch):
        def act(i, kind):
            for copy in copies(i, kind, fetch):
                copy.wait()

        each(i, act)

    for i in range(AHEAD):
        start(i, True)

    near = [(spot, h) for spot in range(n_held) for h in (0, 1)]

    def held_copies(spot, h):
        col = first_held + (spot + 1) % n_held
        rows, cols = slice(h * deep, (h + 1) * deep), slice(col * wide, (col + 1) * wide)
        return cols, [pltpu.make_async_copy(held_out.at[6 * spot + 2 * k + h], ref.at[0, rows, cols], held_sem.at[6 * spot + 2 * k + h])
                      for k, ref in enumerate((nw2, nm2, nv2))]

    for spot, h in near:
        cols, moves = held_copies(spot, h)
        rows = slice(h * block, (h + 1) * block)
        base = 6 * spot + h
        new, mom, sec = adamw(scale, step_rate, held[base], held[base + 2], held[base + 4], gb2[rows, :, cols].reshape(deep, wide))
        held_out[base] = new
        held_out[base + 2] = mom
        held_out[base + 4] = sec
        keep2[rows, :, cols] = new.reshape(block, -1, wide)
        for copy in moves:
            copy.start()

    def step(slot, cols, mean):
        new, mom, sec = adamw(scale, step_rate, ring[0, slot, :, cols], ring[1, slot, :, cols], ring[2, slot, :, cols], mean)
        ring[0, slot, :, cols] = new
        ring[1, slot, :, cols] = mom
        ring[2, slot, :, cols] = sec
        return new

    def compute(i, kind):
        slot = lax.rem(i, n_slot)
        if kind == 0:
            rows = pl.ds(pl.multiple_of(i // per_row * tall, tall), tall)
            for t in range(span // wide):
                col = lax.rem(i, per_row) * (span // wide) + t
                keep1[col, rows] = step(slot, slice(t * wide, (t + 1) * wide), gb1[col, rows])
        else:
            cols = slice(0, kinds[kind][2])
            keep2[i - n_up, :, cols] = step(slot, cols, gb2[i - n_up, :, cols])

    @pl.loop(0, last)
    def _(i):
        finish(i, True)
        each(i, compute)
        start(i, False)

        @pl.when(i + AHEAD < last)
        def _():
            @pl.when(i + AHEAD - n_slot >= 0)
            def _():
                finish(i + AHEAD - n_slot, False)

            start(i + AHEAD, True)

    for i in range(last - n_slot, last):
        finish(i, False)
    for spot, h in near:
        for copy in held_copies(spot, h)[1]:
            copy.wait()


def forward_kernel(from_core, from_diag, new1, new2, y,
                   hid, act, own_half, peer_half, part, part_in,
                   in_sem, p_send, p_recv, y_send, y_recv, g_send, g_recv, f_send, f_recv, ready):
    m, d, s = positions()
    n_micro, half, d_model = own_half.shape
    width = 2 * new1.shape[2]
    n_chunk, n_block = new1.shape[0] // 2, d_model // width
    peer_y = (1 - m, d, s)
    peer_c = (m, d, 1 - s)
    barrier = pltpu.get_barrier_semaphore()
    mine = pl.ds(pl.multiple_of(m * half, half), half)
    theirs = pl.ds(pl.multiple_of((1 - m) * half, half), half)
    rows_in = (pltpu.make_async_copy(from_core, act.at[:, mine, :], in_sem.at[0]),
               pltpu.make_async_copy(from_diag, act.at[:, theirs, :], in_sem.at[1]))

    @pl.when(s == 1)
    def _():
        for copy in rows_in:
            copy.start()
        pl.semaphore_signal(barrier, inc=1, device_id=peer_y, device_id_type=MESH)
        pl.semaphore_signal(barrier, inc=1, device_id=peer_c, device_id_type=MESH)

    pl.semaphore_wait(barrier, 1)

    @pl.when(s == 0)
    def _():
        pl.semaphore_signal(ready, inc=1, device_id=peer_c, device_id_type=MESH)

    def span(c):
        return pl.ds(pl.multiple_of(c * width, width), width)

    def send_part(k, c):
        return remote(part.at[k, theirs, span(c)], part_in.at[k, :, span(c)], p_send.at[k, c], p_recv.at[k, c], peer_y)

    def swap_y(k, c):
        return remote(own_half.at[k, :, span(c)], peer_half.at[k, :, span(c)], y_send.at[k, c], y_recv.at[k, c], peer_y)

    def give_own(k):
        return remote(own_half.at[k], y.at[k, mine, :], g_send.at[k], g_recv.at[k], peer_c)

    def pass_on(k):
        return remote(peer_half.at[k], y.at[k, theirs, :], f_send.at[k], f_recv.at[k], peer_c)

    @pl.when(s == 0)
    def _():
        for k in range(n_micro):
            give_own(k).wait_recv()
            pass_on(k).wait_recv()

    @pl.when(s == 1)
    def _():
        for copy in rows_in:
            copy.wait()

        for k in range(n_micro):
            @pl.loop(0, n_chunk)
            def _(j):
                up = jnp.concatenate([new1[2 * j].astype(BF16), new1[2 * j + 1].astype(BF16)], axis=1)
                hid[:, span(j)] = gelu_parts(dot(act[k], up))[1].astype(BF16)

            @pl.loop(0, n_block)
            def _(c):
                down = new2[:, :, span(c)].reshape(-1, width).astype(BF16)
                part[k, :, span(c)] = dot(hid[...], down)
                send_part(k, c).start()

        for k in range(n_micro):
            @pl.loop(0, n_block)
            def _(c):
                send_part(k, c).wait_recv()
                out = act[k, mine, span(c)].astype(F32) + (part[k, mine, span(c)] + part_in[k, :, span(c)])
                own_half[k, :, span(c)] = out.astype(BF16)
                swap_y(k, c).start()

            y[k, mine, :] = own_half[k]

        pl.semaphore_wait(ready, 1)
        for k in range(n_micro):
            give_own(k).start()
        for k in range(n_micro):
            @pl.loop(0, n_block)
            def _(c):
                swap_y(k, c).wait_recv()

            pass_on(k).start()
            y[k, theirs, :] = peer_half[k]
        for k in range(n_micro):
            @pl.loop(0, n_block)
            def _(c):
                send_part(k, c).wait_send()
                swap_y(k, c).wait_send()

            give_own(k).wait_send()
            pass_on(k).wait_send()


def solution(mesh):
    up_spec = P('stage', None, 'model')
    down_spec = P('stage', 'model', None)
    row_spec = P(None, 'data', None)
    in_specs = (up_spec, down_spec, up_spec, down_spec, up_spec, down_spec, P('data', 'stage', None, 'model'), P('data', 'stage', 'model', None), P('stage', 'data', None), P('data', None), row_spec, P(None), P(None))
    out_specs = (up_spec, down_spec, up_spec, down_spec, up_spec, down_spec, row_spec)

    def device_step(w_up, w_down, m_up, m_down, v_up, v_down, g_up, g_down, acts_last, grad_out, x_next, learn_rate, max_norm):
        d_model, ff = w_up.shape[1:]
        rows = grad_out.shape[0]
        n_micro = x_next.shape[0]
        width = CHUNK
        n_chunk = ff // width
        half = rows // 2
        hbm = pl.BlockSpec(memory_space=pl.ANY)
        vmem = pl.BlockSpec(memory_space=pltpu.VMEM)
        smem = pl.BlockSpec(memory_space=pltpu.SMEM)
        dma = pltpu.SemaphoreType.DMA
        resident = 4 * 3 * d_model * ff
        n_block = d_model // (2 * width)

        mean_up, mean_down, held, clip, act_half = pl.pallas_call(
            functools.partial(grad_kernel, n_chunk, width),
            out_shape=(pltpu.VMEM((n_chunk, d_model, width), F32),
                       pltpu.VMEM((n_chunk, width, d_model), F32),
                       pltpu.VMEM((n_chunk, d_model, width), F32),
                       jax.ShapeDtypeStruct((8, 128), F32),
                       jax.ShapeDtypeStruct((n_micro, half, d_model), BF16)),
            in_specs=[hbm] * 11 + [smem, smem],
            out_specs=(vmem, vmem, vmem, vmem, hbm),
            scratch_shapes=[
                pltpu.VMEM((n_chunk, width, d_model), F32),
                pltpu.VMEM((2, d_model, width), F32),
                pltpu.VMEM((2, width, d_model), F32),
                pltpu.VMEM((2, half, d_model), F32),
                pltpu.VMEM((n_micro, half, d_model), F32),
                pltpu.VMEM((2 * n_micro, half, d_model), BF16),
                pltpu.VMEM((8, width), F32),
                pltpu.VMEM((8, d_model), F32),
                pltpu.VMEM((8, 128), F32),
                pltpu.VMEM((4, 8, 128), F32),
                dma((2, 2)), dma((2, 2)),
                dma((n_chunk,)), dma((n_chunk,)), dma((n_chunk,)), dma((n_chunk,)),
                dma((2,)), dma((2,)), dma((3,)), dma((4,)),
                dma(()), dma(()), dma((18,)), dma((2 * n_block,)), dma((2 * n_block,)), dma((2 * n_block,)),
            ],
            compiler_params=pltpu.CompilerParams(collective_id=0, has_side_effects=True, vmem_limit_bytes=VMEM_MAX - resident - SPARE),
            name="grad_exchange",
        )(w_up[0], w_down[0], g_up[0, 0], g_down[0, 0], m_up[0], v_up[0], m_down[0], v_down[0], acts_last.reshape(2, half, d_model), grad_out.reshape(2, half, d_model), x_next.reshape(2 * n_micro, half, d_model), max_norm, learn_rate)

        from_diag = lax.ppermute(act_half, ('model', 'stage'), [(0, 3), (2, 1)])
        from_core = lax.ppermute(act_half, ('model', 'stage'), [(0, 1), (2, 3)])

        def stay(array):
            return pltpu.with_memory_space_constraint(array, pltpu.VMEM)

        up_out = jax.ShapeDtypeStruct(w_up.shape, F32)
        down_out = jax.ShapeDtypeStruct(w_down.shape, F32)
        nw1, nm1, nv1, nw2, nm2, nv2, new1, new2, _ = pl.pallas_call(
            update_kernel,
            out_shape=(up_out, up_out, up_out, down_out, down_out, down_out,
                       pltpu.VMEM(mean_up.shape, F32), pltpu.VMEM(mean_down.shape, F32), pltpu.VMEM(held.shape, F32)),
            in_specs=[smem, smem, hbm, hbm, hbm, vmem, hbm, hbm, hbm, vmem, vmem],
            out_specs=(hbm,) * 6 + (vmem, vmem, vmem),
            input_output_aliases={5: 6, 9: 7, 10: 8},
            scratch_shapes=[pltpu.VMEM((3, SLOTS, width, d_model), F32), dma((3, SLOTS)), dma((3, SLOTS)), dma((18,))],
            compiler_params=pltpu.CompilerParams(vmem_limit_bytes=VMEM_MAX - resident - SPARE),
            cost_estimate=pl.CostEstimate(flops=2000 * d_model * ff, bytes_accessed=48 * d_model * ff, transcendentals=4 * d_model * ff),
            name="update",
        )(clip, learn_rate, w_up, m_up, v_up, stay(mean_up), w_down, m_down, v_down, stay(mean_down), stay(held))

        y_next = pl.pallas_call(
            forward_kernel,
            out_shape=pltpu.VMEM(x_next.shape, BF16),
            in_specs=[hbm, hbm, vmem, vmem],
            out_specs=vmem,
            scratch_shapes=[
                pltpu.VMEM((rows, ff), BF16),
                pltpu.VMEM((n_micro, rows, d_model), BF16),
                pltpu.VMEM((n_micro, half, d_model), BF16),
                pltpu.VMEM((n_micro, half, d_model), BF16),
                pltpu.VMEM((n_micro, rows, d_model), F32),
                pltpu.VMEM((n_micro, half, d_model), F32),
                dma((2,)), dma((n_micro, n_block)), dma((n_micro, n_block)), dma((n_micro, n_block)), dma((n_micro, n_block)),
                dma((n_micro,)), dma((n_micro,)), dma((n_micro,)), dma((n_micro,)),
                pltpu.SemaphoreType.REGULAR,
            ],
            compiler_params=pltpu.CompilerParams(collective_id=1, has_side_effects=True, vmem_limit_bytes=VMEM_MAX - resident - SPARE),
            name="forward_exchange",
        )(from_core, from_diag, stay(new1), stay(new2))
        return nw1, nw2, nm1, nm2, nv1, nv2, y_next

    return jax.shard_map(device_step, mesh=mesh, in_specs=in_specs, out_specs=out_specs, check_vma=False)
```
